32 devices in a mesh: dp: 8 (over z, x), chan: 4 (over y, core).
Axes of the slice: x: 2, y: 2, z: 4, core: 2. Of those that a mesh axis runs over, the one named last changes fastest.
Arguments:
- inputs: bfloat16 [32768, 512], P('dp', 'chan'), may hold values from -6 to 6
- condition: float32 [2048, 1152], P('dp'), may hold values from -36 to 36
- lengths: int32 [2048], P('dp'), may hold values from 4 to 16
- cotangent: bfloat16 [16384, 512], P('dp', 'chan'), may hold values from -6 to 6
- conv1_w: float32 [512, 5, 512], P('dp', None, 'chan'), may hold values from -0.125 to 0.125
- conv1_m: float32 [512, 5, 512], P('dp', None, 'chan'), as said below
- conv1_v: float32 [512, 5, 512], P('dp', None, 'chan'), as said below
- conv2_w: float32 [512, 5, 512], P('dp', None, 'chan'), may hold values from -0.125 to 0.125
- conv2_m: float32 [512, 5, 512], P('dp', None, 'chan'), as said below
- conv2_v: float32 [512, 5, 512], P('dp', None, 'chan'), as said below
- res_w: float32 [512, 512], P('dp', 'chan'), may hold values from -0.25 to 0.25
- res_m: float32 [512, 512], P('dp', 'chan'), as said below
- res_v: float32 [512, 512], P('dp', 'chan'), as said below
- down_w: float32 [512, 3, 512], P('dp', None, 'chan'), may hold values from -0.15625 to 0.15625
- down_m: float32 [512, 3, 512], P('dp', None, 'chan'), as said below
- down_v: float32 [512, 3, 512], P('dp', None, 'chan'), as said below
- film_w: float32 [1152, 2, 512], P('dp', None, 'chan'), may hold values from -0.1875 to 0.1875
- film_m: float32 [1152, 2, 512], P('dp', None, 'chan'), as said below
- film_v: float32 [1152, 2, 512], P('dp', None, 'chan'), as said below
- small_w: float32 [10, 512], P(None, 'chan'), may hold values from -1 to 2, as said below
- small_m: float32 [10, 512], P(None, 'chan'), as said below
- small_v: float32 [10, 512], P(None, 'chan'), as said below
Outputs:
- output: bfloat16 [16384, 512], P('dp', 'chan')
- input_grad: bfloat16 [32768, 512], P('dp', 'chan')
- conv1_m_new: float32 [512, 5, 512], P('dp', None, 'chan')
- conv1_v_new: float32 [512, 5, 512], P('dp', None, 'chan')
- conv1_w_new: float32 [512, 5, 512], P('dp', None, 'chan')
- conv2_m_new: float32 [512, 5, 512], P('dp', None, 'chan')
- conv2_v_new: float32 [512, 5, 512], P('dp', None, 'chan')
- conv2_w_new: float32 [512, 5, 512], P('dp', None, 'chan')
- res_m_new: float32 [512, 512], P('dp', 'chan')
- res_v_new: float32 [512, 512], P('dp', 'chan')
- res_w_new: float32 [512, 512], P('dp', 'chan')
- down_m_new: float32 [512, 3, 512], P('dp', None, 'chan')
- down_v_new: float32 [512, 3, 512], P('dp', None, 'chan')
- down_w_new: float32 [512, 3, 512], P('dp', None, 'chan')
- film_m_new: float32 [1152, 2, 512], P('dp', None, 'chan')
- film_v_new: float32 [1152, 2, 512], P('dp', None, 'chan')
- film_w_new: float32 [1152, 2, 512], P('dp', None, 'chan')
- small_m_new: float32 [10, 512], P(None, 'chan')
- small_v_new: float32 [10, 512], P(None, 'chan')
- small_w_new: float32 [10, 512], P(None, 'chan')
The draws below stay inside these ranges and needn't reach their ends.
Inputs may be any that keep to these rules, and one draw needn't show every extreme that they name: `lengths`: frames from a sample's length on are padding. `conv1_m`: old first moments. `conv1_v`: old second moments, positive. `conv2_m`: old first moments. `conv2_v`: old second moments, positive. `res_m`: old first moments. `res_v`: old second moments, positive. `down_m`: old first moments. `down_v`: old second moments, positive. `film_m`: old first moments. `film_v`: old second moments, positive. `small_w`: biases and norm parameters. `small_m`: old first moments. `small_v`: old second moments, positive.
All inputs are finite; a program needn't handle non-finite values.
Results may differ from the reference program's by a relative error of at most 0.017.
Values may be sent and summed in bfloat16 or wider, within the bound.
A program may use at most 192 MiB of HBM per device.

```python
import jax
import jax.numpy as jnp
from jax import lax

C = 512
COND = 1152
GROUPS = 8
KERNEL = 5
HORIZON = 16
SMALL_ROWS = 10
S_DEV = 256
SAMPLES = 2048
FRAMES = 32768
N_DP = 8
N_CHAN = 4


def signed_state(key, shape, grad_size):
    values = jnp.clip(jax.random.normal(key, shape, jnp.float32), -4.0, 4.0)
    return values * (grad_size / 9.0)


def square_state(key, shape, grad_size):
    factor = jnp.exp(jax.random.uniform(key, shape, jnp.float32, 0.0, jnp.log(4.0)))
    return factor * (grad_size * grad_size / 999.0)


def frame_root():
    return jnp.sqrt(jnp.float32(FRAMES))


def draw_condition(key, part):
    row_key = jax.random.fold_in(key, 11)
    col_key = jax.random.fold_in(key, 12)
    rows = jnp.arange(SAMPLES).astype(jnp.float32)
    row_scale = 1.0 + 2.0 * rows / (SAMPLES - 1)
    col_scale = jnp.exp(jax.random.uniform(col_key, (COND,), jnp.float32, jnp.log(0.02), jnp.log(2.0)))
    values = jnp.clip(jax.random.normal(row_key, (SAMPLES, COND), jnp.float32), -6.0, 6.0)
    return row_scale[:, None] * col_scale[None, :] * values


def draw_conv1_m(key, part):
    return signed_state(key, (C, KERNEL, C), 0.3 * frame_root())


def draw_conv1_v(key, part):
    return square_state(key, (C, KERNEL, C), 0.3 * frame_root())


def draw_conv2_m(key, part):
    return signed_state(key, (C, KERNEL, C), 0.45 * frame_root())


def draw_conv2_v(key, part):
    return square_state(key, (C, KERNEL, C), 0.45 * frame_root())


def draw_res_m(key, part):
    return signed_state(key, (C, C), 0.55 * frame_root())


def draw_res_v(key, part):
    return square_state(key, (C, C), 0.55 * frame_root())


def draw_down_m(key, part):
    return signed_state(key, (C, 3, C), 0.56 * frame_root())


def draw_down_v(key, part):
    return square_state(key, (C, 3, C), 0.56 * frame_root())


def draw_film_m(key, part):
    return signed_state(key, (COND, 2, C), 0.8 * jnp.sqrt(jnp.float32(SAMPLES)))


def draw_film_v(key, part):
    return square_state(key, (COND, 2, C), 0.8 * jnp.sqrt(jnp.float32(SAMPLES)))


def draw_small_w(key, part):
    base = 0.2 * jnp.clip(jax.random.normal(key, (SMALL_ROWS, C), jnp.float32), -5.0, 5.0)
    row_ids = jnp.arange(SMALL_ROWS)[:, None]
    lifted = ((row_ids == 1) | (row_ids == 4) | (row_ids == 6)).astype(jnp.float32)
    return base + lifted


def draw_small_m(key, part):
    return signed_state(key, (SMALL_ROWS, C), 0.8 * frame_root())


def draw_small_v(key, part):
    return square_state(key, (SMALL_ROWS, C), 0.8 * frame_root())


def plant(values, key, low, high):
    longest = values.shape.index(max(values.shape))
    spots = []
    for shift in (0, 1):
        where = [jax.random.randint(jax.random.fold_in(key, axis), (), 0, length) for axis, length in enumerate(values.shape)]
        where[longest] = (where[longest] + shift) % values.shape[longest]
        spots.append(tuple(where))
    return values.at[spots[0]].set(low).at[spots[1]].set(high)


def with_spikes(result, own_key, source, target, blocks, factor):
    def block_of(position):
        return (jnp.arange(result.shape[position]) // (result.shape[position] // blocks)).reshape((-1,) + (1,) * (result.ndim - 1 - position))

    first = jax.random.permutation(own_key, blocks)[block_of(target)]
    other_side = (block_of(target) + blocks // 2) % blocks
    return jnp.where((block_of(source) == first) | (block_of(source) == other_side), factor * result, result)


def block_scale(own_key, shape, split, least, top_value):
    def one(dim, blocks):
        draws = jax.random.uniform(jax.random.fold_in(jax.random.fold_in(own_key, 6), dim), (blocks,), jnp.float32, least / len(split), top_value / len(split))
        return jnp.repeat(jnp.exp(draws), shape[dim] // blocks).reshape((-1,) + (1,) * (len(shape) - dim - 1))

    gain = one(*split[0])
    for cut in split[1:]:
        gain = gain * one(*cut)
    return gain


def bell_draw(key, extent, deviation, limit, pieces=(), kind=jnp.bfloat16):
    drawn = deviation * jax.random.normal(key, extent, jnp.float32)
    if pieces:
        drawn = drawn * block_scale(key, extent, pieces, -0.22, 0.18)
    return jnp.clip(drawn, -limit, limit).astype(kind)


def gaussian_with(key, dims, spread, limit, cuts, heavy, kind=jnp.bfloat16):
    values = spread * jax.random.normal(key, dims, jnp.float32)
    if cuts:
        values = values * block_scale(key, dims, cuts, -0.22, 0.18)
    return jnp.clip(with_spikes(values, jax.random.fold_in(key, 3), *heavy), -limit, limit).astype(kind)


def setup_inputs(seed: int = 0) -> dict:
    arg_keys = jax.random.split(jax.random.key(seed), 23)
    inputs = gaussian_with(arg_keys[0], (FRAMES, C), 1.0, 6.0, ((0, 8), (1, 4)), (0, 1, 8, 2.0))
    condition = draw_condition(jax.random.fold_in(arg_keys[22], 71), 0)
    lengths = plant(jax.random.randint(arg_keys[2], (SAMPLES,), 4, HORIZON + 1), jax.random.fold_in(arg_keys[2], 1), 4, HORIZON).astype(jnp.int32)
    cotangent = bell_draw(arg_keys[3], (SAMPLES * HORIZON // 2, C), 1.0, 6.0, ((0, 8), (1, 4)))
    conv1_w = bell_draw(arg_keys[4], (C, KERNEL, C), (C * KERNEL) ** -0.5, 0.125, ((0, 8), (2, 4)), jnp.float32)
    conv1_m = draw_conv1_m(jax.random.fold_in(arg_keys[22], 71), 0)
    conv1_v = draw_conv1_v(jax.random.fold_in(arg_keys[22], 71), 0)
    conv2_w = bell_draw(arg_keys[7], (C, KERNEL, C), (C * KERNEL) ** -0.5, 0.125, ((0, 8), (2, 4)), jnp.float32)
    conv2_m = draw_conv2_m(jax.random.fold_in(arg_keys[22], 71), 0)
    conv2_v = draw_conv2_v(jax.random.fold_in(arg_keys[22], 71), 0)
    res_w = bell_draw(arg_keys[10], (C, C), C ** -0.5, 0.25, ((0, 8), (1, 4)), jnp.float32)
    res_m = draw_res_m(jax.random.fold_in(arg_keys[22], 71), 0)
    res_v = draw_res_v(jax.random.fold_in(arg_keys[22], 71), 0)
    down_w = bell_draw(arg_keys[13], (C, 3, C), (C * 3) ** -0.5, 0.15625, ((0, 8), (2, 4)), jnp.float32)
    down_m = draw_down_m(jax.random.fold_in(arg_keys[22], 71), 0)
    down_v = draw_down_v(jax.random.fold_in(arg_keys[22], 71), 0)
    film_w = bell_draw(arg_keys[16], (COND, 2, C), COND ** -0.5, 0.1875, ((0, 8), (2, 4)), jnp.float32)
    film_m = draw_film_m(jax.random.fold_in(arg_keys[22], 71), 0)
    film_v = draw_film_v(jax.random.fold_in(arg_keys[22], 71), 0)
    small_w = draw_small_w(jax.random.fold_in(arg_keys[22], 71), 0)
    small_m = draw_small_m(jax.random.fold_in(arg_keys[22], 71), 0)
    small_v = draw_small_v(jax.random.fold_in(arg_keys[22], 71), 0)
    return dict(inputs=inputs, condition=condition, lengths=lengths, cotangent=cotangent, conv1_w=conv1_w, conv1_m=conv1_m, conv1_v=conv1_v, conv2_w=conv2_w, conv2_m=conv2_m, conv2_v=conv2_v, res_w=res_w, res_m=res_m, res_v=res_v, down_w=down_w, down_m=down_m, down_v=down_v, film_w=film_w, film_m=film_m, film_v=film_v, small_w=small_w, small_m=small_m, small_v=small_v)


@jax.custom_vjp
def low(v):
    return lax.optimization_barrier(v.astype(jnp.bfloat16)).astype(jnp.float32)

@jax.custom_vjp
def low_back(v):
    return v

def low_keep(v):
    return (low(v), None)

def low_pass(kept, grad):
    return (grad,)

def back_keep(v):
    return (v, None)

def back_low(kept, grad):
    return (low(grad),)
low.defvjp(low_keep, low_pass)
low_back.defvjp(back_keep, back_low)
eps_norm = 1e-05
beta_one = 0.9
beta_two = 0.999
adam_eps = 1e-08
weight_decay = 0.01
rate_large = 0.05
rate_small = 0.3
adam_step = 10
highest = lax.Precision.HIGHEST

def mish(values):
    return values * jnp.tanh(jax.nn.softplus(values))

def group_norm(pre_norm, valid_mask, gain_row, shift_row):
    samples, frames, channels = pre_norm.shape
    group_size = C // GROUPS
    grouped = pre_norm.reshape(samples, frames, channels // group_size, group_size)
    weights_in = valid_mask[:, :, None, None]
    counted = (lax.optimization_barrier(jnp.sum(valid_mask, axis=1)) * group_size).reshape(samples, 1, 1, 1)
    centre = lax.optimization_barrier(jnp.sum(grouped * weights_in, axis=(1, 3), keepdims=True)) / counted
    shifted = grouped - centre
    spread_sq = lax.optimization_barrier(jnp.sum(jnp.square(shifted * weights_in), axis=(1, 3), keepdims=True)) / counted
    normed = (shifted * lax.rsqrt(spread_sq + eps_norm)).reshape(samples, frames, channels)
    return normed * gain_row + shift_row

def taps_sum(products, samples, kernel, local_width):
    frames = products.shape[0] // samples
    half_k = kernel // 2
    padded_grid = jnp.pad(products.reshape(samples, frames, kernel, local_width), ((0, 0), (half_k, half_k), (0, 0), (0, 0)))
    summed = padded_grid[:, 0:frames, 0, :]
    for offset in range(1, kernel):
        summed = summed + padded_grid[:, offset:offset + frames, offset, :]
    return summed

def stride_sum(products, samples, local_width):
    frames = products.shape[0] // samples
    padded_grid = jnp.pad(products.reshape(samples, frames, 3, local_width), ((0, 0), (1, 1), (0, 0), (0, 0)))
    return padded_grid[:, 0:frames:2, 0, :] + padded_grid[:, 1:frames + 1:2, 1, :] + padded_grid[:, 2:frames + 2:2, 2, :]

def first_section(valid_mask, conv_out, bias_row, gain_row, shift_row, film_scale, film_shift):
    normed = group_norm(conv_out + bias_row, valid_mask, gain_row, shift_row)
    return (film_scale[:, None, :] * mish(normed) + film_shift[:, None, :]) * valid_mask[:, :, None]

def second_section(valid_mask, conv_out, res_out, bias_row, gain_row, shift_row, res_bias):
    normed = group_norm(conv_out + bias_row, valid_mask, gain_row, shift_row)
    return (mish(normed) + res_out + res_bias) * valid_mask[:, :, None]

def adam_update(weight, gradient, old_first, old_second, learn_rate, decay_term):
    first_new = beta_one * old_first + (1.0 - beta_one) * gradient
    second_new = beta_two * old_second + (1.0 - beta_two) * gradient * gradient
    step_size = first_new / (1.0 - beta_one ** adam_step) / (jnp.sqrt(second_new / (1.0 - beta_two ** adam_step)) + adam_eps)
    return (first_new, second_new, weight - learn_rate * (step_size + decay_term * weight))

def forward(block_in, valid_mask, half_mask, cond_act, params):
    conv1_w, conv2_w, res_w, down_w, film_w, small_w = params
    samples = valid_mask.shape[0]
    local_width = C // N_CHAN
    weight_one = low(conv1_w)
    weight_two = low(conv2_w)
    weight_res = low(res_w)
    weight_down = low(down_w)
    weight_film = low(film_w)
    film_out = low_back(jnp.dot(cond_act, weight_film.reshape(COND, 2 * C), precision=highest))
    film_scale = film_out[:, :C] + small_w[6]
    film_shift = film_out[:, C:] + small_w[7]
    masked_in = block_in * valid_mask.reshape(samples * HORIZON, 1)
    conv_parts = []
    res_parts = []
    for group_index in range(N_CHAN):
        col_range = slice(group_index * local_width, (group_index + 1) * local_width)
        copied = low_back(masked_in)
        joint = jnp.concatenate([weight_one[:, :, col_range].reshape(C, KERNEL * local_width), weight_res[:, col_range]], axis=1)
        products = jnp.dot(copied, joint, precision=highest)
        conv_parts.append(low_back(taps_sum(products[:, :KERNEL * local_width], samples, KERNEL, local_width)))
        res_parts.append(low_back(products[:, KERNEL * local_width:]).reshape(samples, HORIZON, local_width))
    conv_one = jnp.concatenate(conv_parts, axis=2)
    res_out = jnp.concatenate(res_parts, axis=2)
    section_one = first_section(valid_mask, conv_one, small_w[0], small_w[1], small_w[2], film_scale, film_shift)
    hidden = low(section_one).reshape(samples * HORIZON, C)
    two_parts = []
    for group_index in range(N_CHAN):
        col_range = slice(group_index * local_width, (group_index + 1) * local_width)
        copied = low_back(hidden)
        products = jnp.dot(copied, weight_two[:, :, col_range].reshape(C, KERNEL * local_width), precision=highest)
        two_parts.append(low_back(taps_sum(products, samples, KERNEL, local_width)))
    conv_two = jnp.concatenate(two_parts, axis=2)
    section_two = second_section(valid_mask, conv_two, res_out, small_w[3], small_w[4], small_w[5], small_w[8])
    block_out = low(section_two).reshape(samples * HORIZON, C)
    down_parts = []
    for group_index in range(N_CHAN):
        col_range = slice(group_index * local_width, (group_index + 1) * local_width)
        copied = low_back(block_out)
        products = jnp.dot(copied, weight_down[:, :, col_range].reshape(C, 3 * local_width), precision=highest)
        down_parts.append(stride_sum(products, samples, local_width))
    return (jnp.concatenate(down_parts, axis=2) + small_w[9]) * half_mask[:, :, None]

def reference(inputs, condition, lengths, cotangent, conv1_w, conv1_m, conv1_v, conv2_w, conv2_m, conv2_v, res_w, res_m, res_v, down_w, down_m, down_v, film_w, film_m, film_v, small_w, small_m, small_v):
    high_end = lax.optimization_barrier(jnp.max(condition, axis=0))
    low_end = lax.optimization_barrier(jnp.min(condition, axis=0))
    normed_cond = 2.0 * (condition - low_end) / jnp.maximum(high_end - low_end, 1.0) - 1.0
    cond_act = low(mish(normed_cond))
    valid_all = (jnp.arange(HORIZON)[None, :] < lengths[:, None]).astype(jnp.float32)
    half_all = (2 * jnp.arange(HORIZON // 2)[None, :] < lengths[:, None]).astype(jnp.float32)
    params = (conv1_w, conv2_w, res_w, down_w, film_w, small_w)
    input_blocks = inputs.astype(jnp.float32).reshape(N_DP, S_DEV * HORIZON, C)
    grad_blocks = cotangent.astype(jnp.float32).reshape(N_DP, S_DEV, HORIZON // 2, C)
    valid_blocks = valid_all.reshape(N_DP, S_DEV, HORIZON)
    half_blocks = half_all.reshape(N_DP, S_DEV, HORIZON // 2)
    cond_blocks = cond_act.reshape(N_DP, S_DEV, COND)

    def block_step(totals, block):
        block_in, block_grad, block_valid, block_half, block_cond = block

        def run_block(first_arg, second_arg):
            return forward(first_arg, block_valid, block_half, block_cond, second_arg)
        block_out, pullback = jax.vjp(run_block, block_in, params)
        grad_in, grad_params = pullback(block_grad)

        def add_pair(left_sum, right_sum):
            return left_sum + right_sum
        totals = jax.tree.map(add_pair, totals, grad_params)
        return (totals, (block_out.astype(jnp.bfloat16), grad_in.astype(jnp.bfloat16)))
    zero_totals = jax.tree.map(jnp.zeros_like, params)
    totals, (outs_all, grads_all) = lax.scan(block_step, zero_totals, (input_blocks, grad_blocks, valid_blocks, half_blocks, cond_blocks))
    output = outs_all.reshape(SAMPLES * HORIZON // 2, C)
    input_grad = grads_all.reshape(FRAMES, C)
    grad_one, grad_two, grad_res, grad_down, grad_film, grad_small = totals
    one_m, one_v, one_w = adam_update(conv1_w, grad_one, conv1_m, conv1_v, rate_large, weight_decay)
    two_m, two_v, two_w = adam_update(conv2_w, grad_two, conv2_m, conv2_v, rate_large, weight_decay)
    res_m2, res_v2, res_w2 = adam_update(res_w, grad_res, res_m, res_v, rate_large, weight_decay)
    down_m2, down_v2, down_w2 = adam_update(down_w, grad_down, down_m, down_v, rate_large, weight_decay)
    film_m2, film_v2, film_w2 = adam_update(film_w, grad_film, film_m, film_v, rate_large, weight_decay)
    small_m2, small_v2, small_w2 = adam_update(small_w, grad_small, small_m, small_v, rate_small, 0.0)
    return (output, input_grad, one_m, one_v, one_w, two_m, two_v, two_w, res_m2, res_v2, res_w2, down_m2, down_v2, down_w2, film_m2, film_v2, film_w2, small_m2, small_v2, small_w2)
```

```python
from functools import partial

import jax
import jax.numpy as jnp
from jax import lax
from jax.experimental import pallas as pl
from jax.experimental.pallas import tpu as pltpu
from jax.sharding import PartitionSpec as P

f32, bf16 = jnp.float32, jnp.bfloat16
GROUP = 64
TAPS = 5
DOWN = 3
eps_norm = 1e-05


def dot_nn(a, b):
    return lax.dot_general(a, b, (((1,), (0,)), ((), ())), preferred_element_type=f32)


def dot_nt(a, b):
    return lax.dot_general(a, b, (((1,), (1,)), ((), ())), preferred_element_type=f32)


def dot_tn(a, b):
    return lax.dot_general(a, b, (((0,), (0,)), ((), ())), preferred_element_type=f32)


def mish_pair(v):
    u = jnp.exp(-jnp.abs(v))
    pos = v >= 0
    num = jnp.where(pos, 1.0 + 2.0 * u, u * (u + 2.0))
    q = jnp.where(pos, 2.0 * u * u, 2.0)
    r = 1.0 / (num + q)
    w = num * r
    sig = jnp.where(pos, 1.0, u) / (1.0 + u)
    return v * w, w + v * sig * ((q * r) * ((2.0 * num + q) * r))


def wide(tile, lanes):
    return jnp.concatenate([tile] * (lanes // tile.shape[1]), axis=1)


def grid_turn(outer, inner):
    n = outer * inner
    row = lax.broadcasted_iota(jnp.int32, (n, n), 0)
    col = lax.broadcasted_iota(jnp.int32, (n, n), 1)
    return ((row % outer) * inner + row // outer == col).astype(bf16)


def group_sum(values):
    s, c = values.shape
    row = lax.broadcasted_iota(jnp.int32, (128, 128), 0)
    col = lax.broadcasted_iota(jnp.int32, (128, 128), 1)
    ones = (row // GROUP == col // GROUP).astype(f32)
    tall = jnp.concatenate([values[:, i : i + 128] for i in range(0, c, 128)], axis=0)
    tot = lax.dot_general(tall, ones, (((1,), (0,)), ((), ())), precision=lax.Precision.HIGHEST, preferred_element_type=f32)
    return jnp.concatenate([tot[i * s : (i + 1) * s] for i in range(c // 128)], axis=1)


MESH = pl.DeviceIdType.MESH
PARTS = ((0, TAPS + 1), (TAPS + 1, TAPS), (2 * TAPS + 1, DOWN))
SMALL = 16


def step_kernel(
    n_dp, n_ch,
    inputs, cot, cond, lens_all, one_w, two_w, res_w, down_w, film_w, small_w,
    output, input_grad, gfin, gffin, gsfin,
    w_all, gw_all, x_raw, cot_raw, out_raw, ig_raw, small, stats, act, wf_all, film_out, film, gfilm, gfa, gwf,
    rcb, rxb, ryb, rzb, rfx, rfz, gsm, gsr,
    xpad, hpad, be, bo, cbuf, res, xh1, m1, dm1, xh2, dm2, gdn, gc2, gc1, gres,
    ag_send, ag_recv, st_send, st_recv, in_send, in_recv, fw_send, fw_recv, fo_send, fo_recv,
    rs_send, rs_recv, rz_send, rz_recv, out_send, out_recv, gf_send, gf_recv, rf_send, rf_recv, gs_send, gs_recv, loc,
):
    dp, ch = lax.axis_index("dp"), lax.axis_index("chan")
    hi, lo, yy, co = dp // 2, dp % 2, ch // 2, ch % 2
    n_hi = n_dp // 2
    dp_x = hi * 2 + 1 - lo
    ch_y = (1 - yy) * 2 + co
    ch_c = yy * 2 + 1 - co
    m, c = x_raw.shape
    h2 = m // 2
    rows, width = res_w.shape
    frp = film_w.shape[0]
    s = m // (inputs.shape[0] // lens_all.shape[0])
    frames = m // s
    half = frames // 2
    MC = 256 if m % 256 == 0 else m
    NB = 256

    def at(index, size):
        return pl.ds(pl.multiple_of(index * size, size), size)

    def remote(src, dst, ss, rs, device):
        return pltpu.make_async_remote_copy(
            src_ref=src, dst_ref=dst, send_sem=ss, recv_sem=rs, device_id=device, device_id_type=MESH
        )

    barrier = pltpu.get_barrier_semaphore()

    @pl.loop(1, n_dp)
    def _(i):
        pl.semaphore_signal(barrier, inc=1, device_id=((dp + i) % n_dp, ch), device_id_type=MESH)

    for i in range(1, n_ch):
        pl.semaphore_signal(barrier, inc=1, device_id=(dp, (ch + i) % n_ch), device_id_type=MESH)

    own_x = pltpu.make_async_copy(inputs.at[at(ch, m)], x_raw.at[:, at(ch, width)], loc.at[0])
    own_x.start()
    own_cot = pltpu.make_async_copy(cot.at[at(ch, h2)], cot_raw.at[:, at(ch, width)], loc.at[1])
    own_cot.start()
    my_rows, my_cols = at(dp, rows), at(ch, width)
    for k in range(TAPS):
        w_all[k, my_rows, my_cols] = one_w[:, k, :].astype(bf16)
    w_all[TAPS, my_rows, my_cols] = res_w[...].astype(bf16)
    for k in range(TAPS):
        w_all[TAPS + 1 + k, my_rows, my_cols] = two_w[:, k, :].astype(bf16)
    for k in range(DOWN):
        w_all[2 * TAPS + 1 + k, my_rows, my_cols] = down_w[:, k, :].astype(bf16)
    for i in range(2):
        wf_all[i, at(dp, frp), :] = film_w[:, i, :].astype(bf16)
    small[pl.ds(0, small_w.shape[0]), my_cols] = small_w[...]
    small[pl.ds(small_w.shape[0], SMALL - small_w.shape[0]), my_cols] = jnp.zeros((SMALL - small_w.shape[0], width), f32)
    values = cond[...]
    stats[dp, pl.ds(0, 1), :] = jnp.max(values, axis=0, keepdims=True)
    stats[dp, pl.ds(1, 1), :] = -jnp.min(values, axis=0, keepdims=True)
    stats[dp, pl.ds(2, 6), :] = jnp.zeros((6, values.shape[1]), f32)
    pad0 = jnp.zeros((2 * s, c), bf16)
    for ref in (xpad, hpad, gc2, gc1):
        ref[pl.ds(0, 2 * s), :] = pad0
        ref[pl.ds((frames + 2) * s, 2 * s), :] = pad0
    bo[pl.ds(0, s), :] = pad0[:s]
    gdn[pl.ds(half * s, s), :] = pad0[:s]
    pl.semaphore_wait(barrier, n_dp - 1 + n_ch - 1)

    def block(p, d, q):
        t0, nt = PARTS[p]
        return w_all.at[pl.ds(t0, nt), at(d, rows), at(q, width)]

    def pass_on(p, d, q, slot, device):
        return remote(block(p, d, q), block(p, d, q), ag_send.at[p, slot], ag_recv.at[p, d, q], device)

    def to_y(p, h):
        return pass_on(p, h * 2 + lo, ch, n_hi + h, (dp, ch_y))

    def to_x(p, h, v):
        return pass_on(p, h * 2 + lo, v * 2 + co, 2 * n_hi + 2 * h + v, (dp_x, ch))

    def to_c(p, h, l, v):
        return pass_on(p, h * 2 + l, v * 2 + co, 4 * n_hi + 4 * h + 2 * l + v, (dp, ch_c))

    def to_z(p, i):
        return pass_on(p, dp, ch, i, ((hi + i) % n_hi * 2 + lo, ch))

    def landed(p, d, q):
        pass_on(p, d, q, 0, (dp, ch)).wait_recv()

    def ag_own(p):
        @pl.loop(1, n_hi)
        def _(i):
            to_z(p, i).start()

        to_y(p, hi).start()
        to_x(p, hi, yy).start()
        to_c(p, hi, lo, yy).start()

    def ag_z(p):
        @pl.loop(1, n_hi)
        def _(i):
            h = (hi + i) % n_hi
            landed(p, h * 2 + lo, ch)
            to_y(p, h).start()
            to_x(p, h, yy).start()
            to_c(p, h, lo, yy).start()

    def ag_y(p):
        @pl.loop(0, n_hi)
        def _(i):
            h = (hi + i) % n_hi
            landed(p, h * 2 + lo, ch_y)
            to_x(p, h, 1 - yy).start()
            to_c(p, h, lo, 1 - yy).start()

    def ag_x(p):
        @pl.loop(0, n_hi)
        def _(i):
            h = (hi + i) % n_hi
            landed(p, h * 2 + 1 - lo, ch)
            to_c(p, h, 1 - lo, yy).start()

        @pl.loop(0, n_hi)
        def _(i):
            h = (hi + i) % n_hi
            landed(p, h * 2 + 1 - lo, ch_y)
            to_c(p, h, 1 - lo, 1 - yy).start()

    def ag_core(p):
        @pl.loop(0, n_dp)
        def _(d):
            for v in range(n_ch // 2):
                landed(p, d, v * 2 + 1 - co)

    def ag_done(p):
        @pl.loop(1, n_hi)
        def _(i):
            to_z(p, i).wait_send()

        @pl.loop(0, n_hi)
        def _(h):
            to_y(p, h).wait_send()
            for v in range(2):
                to_x(p, h, v).wait_send()
                for l in range(2):
                    to_c(p, h, l, v).wait_send()

    def swap_in(src, dst, n, k, i):
        q = (ch + i) % n_ch
        return remote(src.at[at(q, n)], dst.at[:, my_cols], in_send.at[k, i], in_recv.at[k, i], (dp, q))

    def swap_in_wait(src, dst, n, k):
        for i in range(1, n_ch):
            q = (ch + n_ch - i) % n_ch
            remote(src.at[at(q, n)], dst.at[:, at(q, width)], in_send.at[k, i], in_recv.at[k, i], (dp, q)).wait_recv()
        for i in range(1, n_ch):
            swap_in(src, dst, n, k, i).wait_send()

    def swap_out(src, dst, n, k, i):
        q = (ch + i) % n_ch
        return remote(src.at[:, at(q, width)], dst.at[at(ch, n)], out_send.at[k, i], out_recv.at[k, i], (dp, q))

    def swap_out_wait(src, dst, n, k):
        for i in range(1, n_ch):
            q = (ch + n_ch - i) % n_ch
            remote(src.at[:, at(q, width)], dst.at[at(q, n)], out_send.at[k, i], out_recv.at[k, i], (dp, q)).wait_recv()
        for i in range(1, n_ch):
            swap_out(src, dst, n, k, i).wait_send()

    def small_swap(i, q):
        return remote(small.at[:, at(q, width)], small.at[:, at(q, width)], in_send.at[2, i], in_recv.at[2, i], (dp, (ch + i) % n_ch))

    def bounds(i, d):
        return remote(stats.at[d], stats.at[d], st_send.at[i], st_recv.at[i], ((dp + i) % n_dp, ch))

    def film_block(d):
        return wf_all.at[:, at(d, frp), :]

    def film_pass(d, slot, device):
        return remote(film_block(d), film_block(d), fw_send.at[slot], fw_recv.at[d], device)

    def film_z(i):
        return film_pass(dp, i, ((hi + i) % n_hi * 2 + lo, ch))

    def film_x(h):
        return film_pass(h * 2 + lo, n_hi + h, (dp_x, ch))

    def film_swap(i, q):
        return remote(
            film_out.at[:, at(q, s), :], film.at[:, :, my_cols], fo_send.at[i], fo_recv.at[i], (dp, q)
        )

    @pl.loop(1, n_dp)
    def _(i):
        bounds(i, dp).start()

    ag_own(0)
    for i in range(1, n_ch):
        small_swap(i, ch).start()
        swap_in(inputs, x_raw, m, 0, i).start()

    @pl.loop(1, n_hi)
    def _(i):
        film_z(i).start()

    ag_z(0)
    film_x(hi).start()
    ag_y(0)

    @pl.loop(1, n_hi)
    def _(i):
        h = (hi + i) % n_hi
        film_pass(h * 2 + lo, 0, (dp, ch)).wait_recv()
        film_x(h).start()

    ag_own(1)
    ag_x(0)

    @pl.loop(1, n_dp)
    def _(i):
        bounds(i, (dp + n_dp - i) % n_dp).wait_recv()

    def widest(d, best):
        return jnp.maximum(best, stats[d])

    best = lax.fori_loop(1, n_dp, widest, stats[0])
    low = -best[1:2, :]
    span = jnp.maximum(best[0:1, :] - low, 1.0)
    CB = 64

    @pl.loop(0, cond.shape[0] // CB)
    def _(i):
        v = 2.0 * (cond[at(i, CB), :] - low) / span - 1.0
        act[at(i, CB), :] = mish_pair(v)[0].astype(bf16)

    ag_z(1)

    @pl.loop(0, n_hi)
    def _(h):
        film_pass(h * 2 + 1 - lo, 0, (dp, ch)).wait_recv()

    for i in range(2):
        film_out[i] = dot_nn(act[...], wf_all[i]) + small[pl.ds(6 + i, 1), my_cols]
    for i in range(1, n_ch):
        film_swap(i, (ch + i) % n_ch).start()
    for i in range(2):
        film[i, :, my_cols] = film_out[i, at(ch, s), :]

    lens_ref = lens_all.at[at(ch, s)]

    def mask(t):
        return wide((lens_ref[...] > t).astype(f32), c)

    count = wide(lens_ref[...].astype(f32), c) * GROUP
    own_x.wait()
    swap_in_wait(inputs, x_raw, m, 0)
    sb = 256 // frames
    turn = grid_turn(sb, frames)
    for b in range(s // sb):
        y = dot_nn(turn, x_raw[pl.ds(b * 256, 256), :])
        lens_b = lens_ref[pl.ds(b * sb, sb), :]
        for t in range(frames):
            keep = wide((lens_b > t).astype(f32), c)
            xpad[pl.ds((t + 2) * s + b * sb, sb), :] = (y[t * sb : (t + 1) * sb] * keep).astype(bf16)

    def conv_fwd(src, base, store):
        @pl.loop(0, c // NB)
        def _(n):
            cols = at(n, NB)
            for mi in range(m // MC):
                acc = dot_nn(src[pl.ds(mi * MC, MC), :], w_all[base, :, cols])
                for k in range(1, TAPS):
                    acc += dot_nn(src[pl.ds(mi * MC + k * s, MC), :], w_all[base + k, :, cols])
                store(pl.ds(mi * MC, MC), cols, acc)

    def conv_bwd(src, base, store):
        @pl.loop(0, c // NB)
        def _(n):
            cols = at(n, NB)
            for mi in range(m // MC):
                acc = dot_nt(src[pl.ds(mi * MC + (TAPS - 1) * s, MC), :], w_all[base, cols, :])
                for k in range(1, TAPS):
                    acc += dot_nt(src[pl.ds(mi * MC + (TAPS - 1 - k) * s, MC), :], w_all[base + k, cols, :])
                store(pl.ds(mi * MC, MC), cols, acc)

    def conv_grad(src, g, base):
        @pl.loop(0, TAPS)
        def _(k):
            shifted = pl.ds(pl.multiple_of((TAPS - 1 - k) * s, s), m)
            for n in range(c // NB):
                cols = pl.ds(n * NB, NB)
                gw_all[base + k, :, cols] = dot_tn(src[pl.ds(2 * s, m), :], g[shifted, cols]).astype(bf16)

    def norm_stats(bias):
        tot = jnp.zeros((s, c), f32)
        for t in range(frames):
            tot += (cbuf[pl.ds(t * s, s), :] + bias) * mask(t)
        mean = group_sum(tot) / count
        tot = jnp.zeros((s, c), f32)
        for t in range(frames):
            d = (cbuf[pl.ds(t * s, s), :] + bias - mean) * mask(t)
            tot += d * d
        return mean, lax.rsqrt(group_sum(tot) / count + eps_norm)

    def row(i):
        return small[pl.ds(i, 1), :]

    def keep_c(part, cols, acc):
        cbuf[part, cols] = acc

    ag_core(0)
    conv_fwd(xpad, 0, keep_c)
    ag_y(1)
    for n in range(c // NB):
        cols = pl.ds(n * NB, NB)
        for mi in range(m // MC):
            res[pl.ds(mi * MC, MC), cols] = dot_nn(xpad[pl.ds(2 * s + mi * MC, MC), :], w_all[TAPS, :, cols])
    ag_own(2)
    for i in range(1, n_ch):
        swap_in(cot, cot_raw, h2, 1, i).start()
    ag_x(1)
    for i in range(1, n_ch):
        small_swap(i, (ch + n_ch - i) % n_ch).wait_recv()
        q = (ch + n_ch - i) % n_ch
        remote(film_out.at[:, at(q, s), :], film.at[:, :, at(q, width)], fo_send.at[i], fo_recv.at[i], (dp, q)).wait_recv()
    bias = row(0)
    mean, rstd1 = norm_stats(bias)
    ag_z(2)
    for t in range(frames):
        part = pl.ds(t * s, s)
        xh = (cbuf[part, :] + bias - mean) * rstd1
        mi, dmi = mish_pair(xh * row(1) + row(2))
        xh1[part, :] = xh
        m1[part, :] = mi
        dm1[part, :] = dmi
        hpad[pl.ds((t + 2) * s, s), :] = ((film[0] * mi + film[1]) * mask(t)).astype(bf16)
    ag_y(2)
    ag_core(1)
    conv_fwd(hpad, TAPS + 1, keep_c)
    ag_x(2)
    bias = row(3)
    mean, rstd2 = norm_stats(bias)
    for t in range(frames):
        part = pl.ds(t * s, s)
        xh = (cbuf[part, :] + bias - mean) * rstd2
        mi, dmi = mish_pair(xh * row(4) + row(5))
        xh2[part, :] = xh
        dm2[part, :] = dmi
        val = ((mi + res[part, :] + row(8)) * mask(t)).astype(bf16)
        if t % 2 == 0:
            be[pl.ds(t // 2 * s, s), :] = val
        else:
            bo[pl.ds((t // 2 + 1) * s, s), :] = val
    own_cot.wait()
    swap_in_wait(cot, cot_raw, h2, 1)
    sh = 256 // half
    turn_h = grid_turn(sh, half)
    for b in range(s // sh):
        y = dot_nn(turn_h, cot_raw[pl.ds(b * 256, 256), :])
        lens_b = lens_ref[pl.ds(b * sh, sh), :]
        for j in range(half):
            keep = wide((lens_b > 2 * j).astype(f32), c)
            gdn[pl.ds(j * s + b * sh, sh), :] = (y[j * sh : (j + 1) * sh] * keep).astype(bf16)

    def rs_core(p, v):
        t0, nt = PARTS[p]
        return remote(
            gw_all.at[pl.ds(t0, nt), :, at(v * 2 + 1 - co, width)],
            rcb.at[pl.ds(t0, nt), :, pl.ds(v * width, width)],
            rs_send.at[p, v], rs_recv.at[p, v], (dp, ch_c),
        )

    def rs_x(p, h):
        t0, nt = PARTS[p]
        return remote(
            rcb.at[pl.ds(t0, nt), at(h * 2 + 1 - lo, rows), :],
            rxb.at[pl.ds(t0, nt), at(h, rows), :],
            rz_send.at[p, n_hi + h], rz_recv.at[p, n_hi + h], (dp_x, ch),
        )

    def rs_y(p):
        t0, nt = PARTS[p]
        return remote(
            rxb.at[pl.ds(t0, nt), :, at(1 - yy, width)], ryb.at[pl.ds(t0, nt)], rs_send.at[p, 2], rs_recv.at[p, 2], (dp, ch_y)
        )

    def rs_z(p, i):
        t0, nt = PARTS[p]
        h = (hi + i) % n_hi
        return remote(
            ryb.at[pl.ds(t0, nt), at(h, rows), :], rzb.at[i, pl.ds(t0, nt)], rz_send.at[p, i], rz_recv.at[p, i], (h * 2 + lo, ch)
        )

    def rs_start(p):
        for v in range(2):
            rs_core(p, v).start()

    def rs_after_core(p):
        t0, nt = PARTS[p]
        for v in range(2):
            rs_core(p, v).wait()

        @pl.loop(t0, t0 + nt)
        def _(k):
            for v in range(2):
                cols = pl.ds(v * width, width)
                rcb[k, :, cols] = (rcb[k, :, cols].astype(f32) + gw_all[k, :, at(v * 2 + co, width)].astype(f32)).astype(bf16)

        @pl.loop(0, n_hi)
        def _(h):
            rs_x(p, h).start()

    def rs_after_x(p):
        t0, nt = PARTS[p]

        @pl.loop(0, n_hi)
        def _(h):
            rs_x(p, h).wait()

        @pl.loop(t0, t0 + nt)
        def _(k):
            @pl.loop(0, n_hi)
            def _(h):
                part = at(h, rows)
                rxb[k, part, :] = (rxb[k, part, :].astype(f32) + rcb[k, at(h * 2 + lo, rows), :].astype(f32)).astype(bf16)

        rs_y(p).start()

    def rs_after_y(p):
        t0, nt = PARTS[p]
        rs_y(p).wait()

        @pl.loop(t0, t0 + nt)
        def _(k):
            ryb[k] = (ryb[k].astype(f32) + rxb[k, :, at(yy, width)].astype(f32)).astype(bf16)

        @pl.loop(1, n_hi)
        def _(i):
            rs_z(p, i).start()

    def rs_after_z(p):
        t0, nt = PARTS[p]

        @pl.loop(1, n_hi)
        def _(i):
            rs_z(p, i).wait()

        @pl.loop(t0, t0 + nt)
        def _(k):
            def more(i, tot):
                return tot + rzb[i, k].astype(f32)

            gfin[k] = lax.fori_loop(1, n_hi, more, ryb[k, at(hi, rows), :].astype(f32))

    ag_core(2)
    hm = half * s
    back_h = grid_turn(half, sh)
    dbase = 2 * TAPS + 1
    taps_in = (bo, be, bo)
    taps_at = (0, 0, s)
    for k in range(DOWN):
        for n in range(c // NB):
            cols = pl.ds(n * NB, NB)
            gw_all[dbase + k, :, cols] = dot_tn(taps_in[k][pl.ds(taps_at[k], hm), :], gdn[pl.ds(0, hm), cols]).astype(bf16)
    rs_start(2)
    for n in range(c // NB):
        cols = pl.ds(n * NB, NB)
        acc = dot_nn(bo[pl.ds(0, hm), :], w_all[dbase, :, cols])
        acc += dot_nn(be[...], w_all[dbase + 1, :, cols])
        acc += dot_nn(bo[pl.ds(s, hm), :], w_all[dbase + 2, :, cols])
        cbuf[pl.ds(0, hm), cols] = acc
    for b in range(s // sh):
        pieces = []
        lens_b = lens_ref[pl.ds(b * sh, sh), :]
        for j in range(half):
            keep = wide((lens_b > 2 * j).astype(f32), c)
            pieces.append(((cbuf[pl.ds(j * s + b * sh, sh), :] + row(9)) * keep).astype(bf16))
        out_raw[pl.ds(b * 256, 256), :] = dot_nn(back_h, jnp.concatenate(pieces, axis=0)).astype(bf16)
    rs_after_core(2)
    for i in range(1, n_ch):
        swap_out(out_raw, output, h2, 0, i).start()
    own_out = pltpu.make_async_copy(out_raw.at[:, my_cols], output.at[at(ch, h2)], loc.at[2])
    own_out.start()

    tot = jnp.zeros((s, c), f32)
    for j in range(half):
        tot += gdn[pl.ds(j * s, s), :].astype(f32)
    gs = [None] * SMALL
    gs[9] = jnp.sum(tot, axis=0, keepdims=True)
    for n in range(c // NB):
        cols = pl.ds(n * NB, NB)
        ge = dot_nt(gdn[pl.ds(0, hm), :], w_all[dbase + 1, cols, :])
        go = dot_nt(gdn[pl.ds(0, hm), :], w_all[dbase + 2, cols, :])
        go += dot_nt(gdn[pl.ds(s, hm), :], w_all[dbase, cols, :])
        for j in range(half):
            cbuf[pl.ds(2 * j * s, s), cols] = ge[j * s : (j + 1) * s]
            cbuf[pl.ds((2 * j + 1) * s, s), cols] = go[j * s : (j + 1) * s]

    def norm_back(xh, dm, gain, rstd, dst, scale):
        a1 = jnp.zeros((s, c), f32)
        a2 = jnp.zeros((s, c), f32)
        for t in range(frames):
            part = pl.ds(t * s, s)
            dy = cbuf[part, :] * mask(t) * dm[part, :]
            if scale is not None:
                dy = dy * scale
            dm[part, :] = dy
            a1 += dy
            a2 += dy * xh[part, :]
        g1 = group_sum(a1 * gain) / count
        g2 = group_sum(a2 * gain) / count
        tot = jnp.zeros((s, c), f32)
        for t in range(frames):
            part = pl.ds(t * s, s)
            dp_t = rstd * (dm[part, :] * gain - mask(t) * (g1 + xh[part, :] * g2))
            tot += dp_t
            dst[pl.ds((t + 2) * s, s), :] = dp_t.astype(bf16)
        return [jnp.sum(v, axis=0, keepdims=True) for v in (tot, a2, a1)]

    tot = jnp.zeros((s, c), f32)
    for t in range(frames):
        part = pl.ds(t * s, s)
        g = cbuf[part, :] * mask(t)
        tot += g
        gres[part, :] = g.astype(bf16)
    gs[8] = jnp.sum(tot, axis=0, keepdims=True)
    gs[3:6] = norm_back(xh2, dm2, row(4), rstd2, gc2, None)
    conv_grad(hpad, gc2, TAPS + 1)
    rs_start(1)
    rs_after_x(2)
    conv_bwd(gc2, TAPS + 1, keep_c)
    rs_after_core(1)
    rs_after_y(2)
    tot1 = jnp.zeros((s, c), f32)
    tot2 = jnp.zeros((s, c), f32)
    for t in range(frames):
        part = pl.ds(t * s, s)
        g = cbuf[part, :] * mask(t)
        tot1 += g * m1[part, :]
        tot2 += g
    gfilm[0] = tot1.astype(bf16)
    gfilm[1] = tot2.astype(bf16)
    gs[6] = jnp.sum(tot1, axis=0, keepdims=True)
    gs[7] = jnp.sum(tot2, axis=0, keepdims=True)

    def film_back(i):
        q = (ch + i) % n_ch
        return remote(gfilm.at[:, :, at(q, width)], gfa.at[:, at(ch, s), :], gf_send.at[i], gf_recv.at[i], (dp, q))

    for i in range(1, n_ch):
        film_back(i).start()
    gfa[:, at(ch, s), :] = gfilm[:, :, my_cols]
    gs[0:3] = norm_back(xh1, dm1, row(1), rstd1, gc1, film[0])
    conv_grad(xpad, gc1, 0)
    for n in range(c // NB):
        cols = pl.ds(n * NB, NB)
        gw_all[TAPS, :, cols] = dot_tn(xpad[pl.ds(2 * s, m), :], gres[:, cols]).astype(bf16)
    rs_start(0)
    zero = jnp.zeros((1, c), f32)
    for i in range(SMALL):
        gsm[pl.ds(i, 1), :] = gs[i] if gs[i] is not None else zero

    def small_pass(i, device):
        return remote(gsm, gsr.at[i], gs_send.at[i], gs_recv.at[i], device)

    small_pass(0, (dp, ch_c)).start()

    def keep_ig(part, cols, acc):
        cbuf[part, cols] = acc + dot_nt(gres[part, :], w_all[TAPS, cols, :])

    conv_bwd(gc1, 0, keep_ig)
    rs_after_x(1)
    rs_after_core(0)
    back = grid_turn(frames, sb)
    for b in range(s // sb):
        lens_b = lens_ref[pl.ds(b * sb, sb), :]
        pieces = [
            (cbuf[pl.ds(t * s + b * sb, sb), :] * wide((lens_b > t).astype(f32), c)).astype(bf16) for t in range(frames)
        ]
        ig_raw[pl.ds(b * 256, 256), :] = dot_nn(back, jnp.concatenate(pieces, axis=0)).astype(bf16)
    for i in range(1, n_ch):
        swap_out(ig_raw, input_grad, m, 1, i).start()
    own_ig = pltpu.make_async_copy(ig_raw.at[:, my_cols], input_grad.at[at(ch, m)], loc.at[3])
    own_ig.start()

    for i in range(1, n_ch):
        q = (ch + n_ch - i) % n_ch
        remote(gfilm.at[:, :, at(q, width)], gfa.at[:, at(q, s), :], gf_send.at[i], gf_recv.at[i], (dp, q)).wait_recv()
    for i in range(2):
        gwf[i] = dot_tn(act[...], gfa[i]).astype(bf16)

    def rf_x(h):
        return remote(gwf.at[:, at(h * 2 + 1 - lo, frp), :], rfx.at[:, at(h, frp), :], rf_send.at[n_hi + h], rf_recv.at[n_hi + h], (dp_x, ch))

    def rf_z(i):
        h = (hi + i) % n_hi
        return remote(rfx.at[:, at(h, frp), :], rfz.at[i], rf_send.at[i], rf_recv.at[i], (h * 2 + lo, ch))

    @pl.loop(0, n_hi)
    def _(h):
        rf_x(h).start()

    small_pass(0, (dp, ch_c)).wait()
    gsm[...] += gsr[0]
    small_pass(1, (dp_x, ch)).start()
    rs_after_z(2)
    rs_after_y(1)
    small_pass(1, (dp_x, ch)).wait()
    gsm[...] += gsr[1]
    small_pass(2, (dp, ch_y)).start()

    @pl.loop(0, n_hi)
    def _(h):
        rf_x(h).wait()

    for i in range(2):
        @pl.loop(0, n_hi)
        def _(h):
            part = at(h, frp)
            rfx[i, part, :] = (rfx[i, part, :].astype(f32) + gwf[i, at(h * 2 + lo, frp), :].astype(f32)).astype(bf16)

    @pl.loop(1, n_hi)
    def _(i):
        rf_z(i).start()

    small_pass(2, (dp, ch_y)).wait()
    gsm[...] += gsr[2]

    def small_z(i):
        return small_pass(2 + i, ((hi + i) % n_hi * 2 + lo, ch))

    @pl.loop(1, n_hi)
    def _(i):
        small_z(i).start()

    rs_after_z(1)

    @pl.loop(1, n_hi)
    def _(i):
        rf_z(i).wait()

    for v in range(2):
        def more(i, tot):
            return tot + rfz[i, v].astype(f32)

        gffin[v] = lax.fori_loop(1, n_hi, more, rfx[v, at(hi, frp), :].astype(f32))

    @pl.loop(1, n_hi)
    def _(i):
        small_z(i).wait()

    def more_small(i, tot):
        return tot + gsr[2 + i, :, my_cols]

    gsfin[...] = lax.fori_loop(1, n_hi, more_small, gsm[:, my_cols])
    rs_after_x(0)
    rs_after_y(0)
    rs_after_z(0)

    own_out.wait()
    own_ig.wait()
    swap_out_wait(out_raw, output, h2, 0)
    swap_out_wait(ig_raw, input_grad, m, 1)
    for p in range(3):
        ag_done(p)

    @pl.loop(1, n_dp)
    def _(i):
        bounds(i, dp).wait_send()

    @pl.loop(1, n_hi)
    def _(i):
        film_z(i).wait_send()

    @pl.loop(0, n_hi)
    def _(h):
        film_x(h).wait_send()

    for i in range(1, n_ch):
        small_swap(i, ch).wait_send()
        film_swap(i, (ch + i) % n_ch).wait_send()
        film_back(i).wait_send()


def block_step(n_dp, n_ch, inputs, cot, cond, lens_all, one_w, two_w, res_w, down_w, film_w, small_w):
    rows, width = res_w.shape
    c = rows * n_dp
    samples = lens_all.shape[0]
    s = samples // n_ch
    m = inputs.shape[0] // n_ch
    h = m // 2
    frp = film_w.shape[0]
    feats = cond.shape[1]
    n_hi = n_dp // 2
    taps = 2 * TAPS + 1 + DOWN
    V = pltpu.VMEM
    D = pltpu.SemaphoreType.DMA
    vm = pl.BlockSpec(memory_space=pltpu.VMEM)
    hbm = pl.BlockSpec(memory_space=pl.ANY)
    out = [
        jax.ShapeDtypeStruct((h * n_ch, width), bf16),
        jax.ShapeDtypeStruct((m * n_ch, width), bf16),
        jax.ShapeDtypeStruct((taps, rows, width), f32),
        jax.ShapeDtypeStruct((2, frp, width), f32),
        jax.ShapeDtypeStruct((SMALL, width), f32),
    ]
    pad = V((m + 4 * s, c), bf16)
    full = V((m, c), f32)
    scratch = [
        V((taps, c, c), bf16), V((taps, c, c), bf16), V((m, c), bf16), V((h, c), bf16), V((h, c), bf16), V((m, c), bf16),
        V((SMALL, c), f32), V((n_dp, 8, feats), f32), V((samples, feats), bf16), V((2, n_dp * frp, width), bf16),
        V((2, samples, width), f32), V((2, s, c), f32), V((2, s, c), bf16), V((2, samples, width), bf16), V((2, n_dp * frp, width), bf16),
        V((taps, c, 2 * width), bf16), V((taps, n_hi * rows, 2 * width), bf16), V((taps, n_hi * rows, width), bf16),
        V((n_hi, taps, rows, width), bf16), V((2, n_hi * frp, width), bf16), V((n_hi, 2, frp, width), bf16),
        V((SMALL, c), f32), V((2 + n_hi, SMALL, c), f32),
        pad, pad, V((h, c), bf16), V((h + s, c), bf16),
        full, full, full, full, full, full, full,
        V((h + s, c), bf16), pad, pad, V((m, c), bf16),
        D((3, 8 * n_hi)), D((3, n_dp, n_ch)), D((n_dp,)), D((n_dp,)), D((3, n_ch)), D((3, n_ch)),
        D((2 * n_hi,)), D((n_dp,)), D((n_ch,)), D((n_ch,)),
        D((3, 3)), D((3, 3)), D((3, 2 * n_hi)), D((3, 2 * n_hi)), D((2, n_ch)), D((2, n_ch)), D((n_ch,)), D((n_ch,)),
        D((2 * n_hi,)), D((2 * n_hi,)), D((2 + n_hi,)), D((2 + n_hi,)), D((4,)),
    ]
    return pl.pallas_call(
        partial(step_kernel, n_dp, n_ch),
        out_shape=out,
        in_specs=[hbm, hbm] + [vm] * 8,
        out_specs=[hbm, hbm, vm, vm, vm],
        scratch_shapes=scratch,
        compiler_params=pltpu.CompilerParams(vmem_limit_bytes=63 << 20, collective_id=0, has_side_effects=True),
        name="block_step",
    )(inputs, cot, cond, lens_all, one_w, two_w, res_w, down_w, film_w, small_w)


beta_one = 0.9
beta_two = 0.999
adam_eps = 1e-08
weight_decay = 0.01
rate_large = 0.05
rate_small = 0.3
adam_step = 10


def adam_update(weight, gradient, old_first, old_second, learn_rate, decay_term):
    first_new = beta_one * old_first + (1.0 - beta_one) * gradient
    second_new = beta_two * old_second + (1.0 - beta_two) * gradient * gradient
    step_size = (
        first_new
        / (1.0 - beta_one**adam_step)
        / (jnp.sqrt(second_new / (1.0 - beta_two**adam_step)) + adam_eps)
    )
    return (first_new, second_new, weight - learn_rate * (step_size + decay_term * weight))


def update_kernel(gw, gf, gs, *refs):
    ins, outs = refs[: len(refs) // 2], refs[len(refs) // 2 :]

    def put(i, index, grad, rate, decay):
        w, m, v = (ins[3 * i + j][index] for j in range(3))
        m, v, w = adam_update(w, grad, m, v, rate, decay)
        for j, value in enumerate((m, v, w)):
            outs[3 * i + j][index] = value

    everything = slice(None)
    for k in range(TAPS):
        put(0, (everything, k), gw[k], rate_large, weight_decay)
        put(1, (everything, k), gw[TAPS + 1 + k], rate_large, weight_decay)
    put(2, ..., gw[TAPS], rate_large, weight_decay)
    for k in range(DOWN):
        put(3, (everything, k), gw[2 * TAPS + 1 + k], rate_large, weight_decay)
    frows = ins[12].shape[0]
    for k in range(2):
        put(4, (everything, k), gf[k, pl.ds(0, frows), :], rate_large, weight_decay)
    put(5, ..., gs[pl.ds(0, ins[15].shape[0]), :], rate_small, 0.0)


def update(gw, gf, gs, *state):
    vm = pl.BlockSpec(memory_space=pltpu.VMEM)
    return pl.pallas_call(
        update_kernel,
        out_shape=[jax.ShapeDtypeStruct(a.shape, f32) for a in state],
        in_specs=[vm] * (3 + len(state)),
        out_specs=[vm] * len(state),
        compiler_params=pltpu.CompilerParams(vmem_limit_bytes=32 << 20),
        name="update",
    )(gw, gf, gs, *state)


def body(
    inputs, condition, lengths, cotangent,
    conv1_w, conv1_m, conv1_v, conv2_w, conv2_m, conv2_v, res_w, res_m, res_v,
    down_w, down_m, down_v, film_w, film_m, film_v, small_w, small_m, small_v,
):
    n_dp, n_ch = lax.axis_size("dp"), lax.axis_size("chan")
    lens_all = jnp.broadcast_to(lengths[:, None], (lengths.shape[0], 128))
    cond, film_rows = condition, film_w
    frows = film_w.shape[0]
    if frows % 16:
        short = -frows % 16
        film_rows = jnp.pad(film_w, ((0, short), (0, 0), (0, 0)))
        cond = jnp.pad(condition.reshape(-1, n_dp, frows), ((0, 0), (0, 0), (0, short))).reshape(condition.shape[0], -1)
    output, input_grad, gw, gf, gs = block_step(
        n_dp, n_ch, inputs, cotangent, cond, lens_all, conv1_w, conv2_w, res_w, down_w, film_rows, small_w
    )
    state = update(
        gw, gf, gs,
        conv1_w, conv1_m, conv1_v, conv2_w, conv2_m, conv2_v, res_w, res_m, res_v,
        down_w, down_m, down_v, film_w, film_m, film_v, small_w, small_m, small_v,
    )
    return (output, input_grad, *state)


def solution(mesh):
    in_specs = (
        P("dp", "chan"),
        P("dp", None),
        P("dp"),
        P("dp", "chan"),
        P("dp", None, "chan"),
        P("dp", None, "chan"),
        P("dp", None, "chan"),
        P("dp", None, "chan"),
        P("dp", None, "chan"),
        P("dp", None, "chan"),
        P("dp", "chan"),
        P("dp", "chan"),
        P("dp", "chan"),
        P("dp", None, "chan"),
        P("dp", None, "chan"),
        P("dp", None, "chan"),
        P("dp", None, "chan"),
        P("dp", None, "chan"),
        P("dp", None, "chan"),
        P(None, "chan"),
        P(None, "chan"),
        P(None, "chan"),
    )
    out_specs = (
        P("dp", "chan"),
        P("dp", "chan"),
        P("dp", None, "chan"),
        P("dp", None, "chan"),
        P("dp", None, "chan"),
        P("dp", None, "chan"),
        P("dp", None, "chan"),
        P("dp", None, "chan"),
        P("dp", "chan"),
        P("dp", "chan"),
        P("dp", "chan"),
        P("dp", None, "chan"),
        P("dp", None, "chan"),
        P("dp", None, "chan"),
        P("dp", None, "chan"),
        P("dp", None, "chan"),
        P("dp", None, "chan"),
        P(None, "chan"),
        P(None, "chan"),
        P(None, "chan"),
    )
    return jax.shard_map(body, mesh=mesh, in_specs=in_specs, out_specs=out_specs, check_vma=False)
```

```python
from functools import partial

import jax
import jax.numpy as jnp
from jax import lax
from jax.experimental import pallas as pl
from jax.experimental.pallas import tpu as pltpu
from jax.sharding import PartitionSpec as P

f32, bf16 = jnp.float32, jnp.bfloat16
GROUP = 64
TAPS = 5
DOWN = 3
eps_norm = 1e-05


def dot_nn(a, b):
    return lax.dot_general(a, b, (((1,), (0,)), ((), ())), preferred_element_type=f32)


def dot_nt(a, b):
    return lax.dot_general(a, b, (((1,), (1,)), ((), ())), preferred_element_type=f32)


def dot_tn(a, b):
    return lax.dot_general(a, b, (((0,), (0,)), ((), ())), preferred_element_type=f32)


def mish_pair(v):
    u = jnp.exp(-jnp.abs(v))
    pos = v >= 0
    num = jnp.where(pos, 1.0 + 2.0 * u, u * (u + 2.0))
    q = jnp.where(pos, 2.0 * u * u, 2.0)
    r = 1.0 / (num + q)
    w = num * r
    sig = jnp.where(pos, 1.0, u) / (1.0 + u)
    return v * w, w + v * sig * ((q * r) * ((2.0 * num + q) * r))


def wide(tile, lanes):
    return jnp.concatenate([tile] * (lanes // tile.shape[1]), axis=1)


def grid_turn(outer, inner):
    n = outer * inner
    row = lax.broadcasted_iota(jnp.int32, (n, n), 0)
    col = lax.broadcasted_iota(jnp.int32, (n, n), 1)
    return ((row % outer) * inner + row // outer == col).astype(bf16)


def group_sum(values):
    s, c = values.shape
    row = lax.broadcasted_iota(jnp.int32, (128, 128), 0)
    col = lax.broadcasted_iota(jnp.int32, (128, 128), 1)
    ones = (row // GROUP == col // GROUP).astype(f32)
    tall = jnp.concatenate([values[:, i : i + 128] for i in range(0, c, 128)], axis=0)
    tot = lax.dot_general(tall, ones, (((1,), (0,)), ((), ())), precision=lax.Precision.HIGHEST, preferred_element_type=f32)
    return jnp.concatenate([tot[i * s : (i + 1) * s] for i in range(c // 128)], axis=1)


MESH = pl.DeviceIdType.MESH
W_ONE, W_RES, W_TWO, W_DOWN = 0, TAPS, TAPS + 1, 2 * TAPS + 1
N_TAPS = W_DOWN + DOWN
PARTS = ((W_ONE, TAPS + 1), (W_TWO, TAPS), (W_DOWN, DOWN))
G_DOWN, G_RES, G_TWO_A, G_TWO_B, G_ONE_A, G_ONE_B, G_ONE_C = range(7)
SUMS = (
    (W_DOWN, DOWN, True), (W_RES, 1, False), (W_TWO, 3, False), (W_TWO + 3, 2, True),
    (W_ONE, 2, False), (W_ONE + 2, 2, False), (W_ONE + 4, 1, False),
)
SMALL = 16


def step_kernel(
    n_dp, n_ch,
    inputs, cot, cond_h, lens_h, one_w, two_w, res_w, down_w, film_h, small_h,
    output, input_grad, gfin_h, gffin_h, gsfin_h,
    w_all, gw_all, x_raw, cot_raw, out_raw, ig_raw, small, stats, act, wf_all, film_out, film, gfilm, gfa, gwf,
    gfin, gffin, gsfin, rcb, rxb, ryb, sidebuf, rzb, rfx, rfz, rfs, gsm, gsr, cond, lens_row, lens_all, wraw, film_w, small_w,
    xpad, hpad, be, bo, cbuf, res, xh1, m1, dm1, xh2, dm2, gdn, gc2, gc1, gres,
    ag_send, ag_recv, st_send, st_recv, in_send, in_recv, fw_send, fw_recv, fo_send, fo_recv,
    rs_send, rs_recv, rz_send, rz_recv, out_send, out_recv, gf_send, gf_recv, rf_send, rf_recv, gs_send, gs_recv, loc,
):
    dp, ch = lax.axis_index("dp"), lax.axis_index("chan")
    hi, lo, yy, co = dp // 2, dp % 2, ch // 2, ch % 2
    n_hi = n_dp // 2
    dp_x = hi * 2 + 1 - lo
    ch_y = (1 - yy) * 2 + co
    ch_c = yy * 2 + 1 - co
    m, c = x_raw.shape
    h2 = m // 2
    rows, width = res_w.shape
    frp = film_h.shape[0]
    s = lens_h.shape[1] // n_ch
    frames = m // s
    half = frames // 2
    MC = 256 if m % 256 == 0 else m
    NB = 256

    def at(index, size):
        return pl.ds(pl.multiple_of(index * size, size), size)

    def remote(src, dst, ss, rs, device):
        return pltpu.make_async_remote_copy(
            src_ref=src, dst_ref=dst, send_sem=ss, recv_sem=rs, device_id=device, device_id_type=MESH
        )

    barrier = pltpu.get_barrier_semaphore()

    @pl.loop(1, n_dp)
    def _(i):
        pl.semaphore_signal(barrier, inc=1, device_id=((dp + i) % n_dp, ch), device_id_type=MESH)

    for i in range(1, n_ch):
        pl.semaphore_signal(barrier, inc=1, device_id=(dp, (ch + i) % n_ch), device_id_type=MESH)

    def local(i, src, dst):
        copy = pltpu.make_async_copy(src, dst, loc.at[i])
        copy.start()
        return copy

    own_x = local(0, inputs.at[at(ch, m)], x_raw.at[:, at(ch, width)])
    own_cot = local(1, cot.at[at(ch, h2)], cot_raw.at[:, at(ch, width)])
    staged = [
        local(4, cond_h, cond), local(5, lens_h, lens_row), local(6, small_h, small_w),
        local(7, one_w, wraw.at[pl.ds(W_ONE, TAPS)]), local(8, two_w, wraw.at[pl.ds(W_TWO, TAPS)]),
        local(9, down_w, wraw.at[pl.ds(W_DOWN, DOWN)]), local(10, res_w, wraw.at[W_RES]), local(11, film_h, film_w),
    ]
    pad0 = jnp.zeros((2 * s, c), bf16)
    for ref in (xpad, hpad, gc2, gc1):
        ref[pl.ds(0, 2 * s), :] = pad0
        ref[pl.ds((frames + 2) * s, 2 * s), :] = pad0
    bo[pl.ds(0, s), :] = pad0[:s]
    gdn[pl.ds(half * s, s), :] = pad0[:s]
    for copy in staged:
        copy.wait()
    my_rows, my_cols = at(dp, rows), at(ch, width)

    @pl.loop(0, N_TAPS)
    def _(k):
        w_all[k, my_rows, my_cols] = wraw[k].astype(bf16)

    for i in range(2):
        wf_all[i, at(dp, frp), :] = film_w[:, i, :].astype(bf16)
    n_all = lens_all.shape[0]
    on_line = lax.broadcasted_iota(jnp.int32, (n_all, n_all), 0) == lax.broadcasted_iota(jnp.int32, (n_all, n_all), 1)
    across = jnp.sum(jnp.where(on_line, lens_row[...].astype(f32), 0.0), axis=1, keepdims=True)
    lens_all[...] = jnp.broadcast_to(across, lens_all.shape)
    small[pl.ds(0, small_w.shape[0]), my_cols] = small_w[...]
    small[pl.ds(small_w.shape[0], SMALL - small_w.shape[0]), my_cols] = jnp.zeros((SMALL - small_w.shape[0], width), f32)
    values = cond[...]
    feats = values.shape[1] // 128
    ends = (jnp.max(values, axis=0, keepdims=True), jnp.max(-values, axis=0, keepdims=True))
    for e in range(2):
        for i in range(feats):
            stats[0, pl.ds(e * feats + i, 1), :] = ends[e][:, i * 128 : (i + 1) * 128]
    if stats.shape[1] > 2 * feats:
        stats[0, pl.ds(2 * feats, stats.shape[1] - 2 * feats), :] = jnp.zeros((stats.shape[1] - 2 * feats, 128), f32)
    pl.semaphore_wait(barrier, n_dp - 1 + n_ch - 1)

    far, near = hi // 2, hi % 2
    if n_hi == 4:
        line = (far * 2 + 1 - near, (1 - far) * 2 + far, (1 - far) * 3)
    else:
        line = None

    def along(step, middle=None):
        if line is not None:
            for j, h in enumerate(line):
                step(h)
                if j == 1 and middle is not None:
                    middle()
        else:

            @pl.loop(1, n_hi)
            def _(i):
                step((hi + i) % n_hi)

            if middle is not None:
                middle()

    def block(p, d, q):
        t0, nt = PARTS[p]
        return w_all.at[pl.ds(t0, nt), at(d, rows), at(q, width)]

    def pass_on(p, d, q, slot, device):
        return remote(block(p, d, q), block(p, d, q), ag_send.at[p, slot], ag_recv.at[p, d, q], device)

    def to_y(p, h):
        return pass_on(p, h * 2 + lo, ch, n_hi + h, (dp, ch_y))

    def to_x(p, h, v):
        return pass_on(p, h * 2 + lo, v * 2 + co, 2 * n_hi + 2 * h + v, (dp_x, ch))

    def to_c(p, h, l, v):
        return pass_on(p, h * 2 + l, v * 2 + co, 4 * n_hi + 4 * h + 2 * l + v, (dp, ch_c))

    def to_z(p, h):
        return pass_on(p, dp, ch, h, (h * 2 + lo, ch))

    def landed(p, d, q):
        pass_on(p, d, q, 0, (dp, ch)).wait_recv()

    def ag_far(p):
        along(lambda h: to_z(p, h).start())

    def ag_own(p):
        to_y(p, hi).start()
        to_x(p, hi, yy).start()
        to_c(p, hi, lo, yy).start()

    def from_z(p, h):
        landed(p, h * 2 + lo, ch)
        to_y(p, h).start()
        to_x(p, h, yy).start()
        to_c(p, h, lo, yy).start()

    def from_y(p, h):
        landed(p, h * 2 + lo, ch_y)
        to_x(p, h, 1 - yy).start()
        to_c(p, h, lo, 1 - yy).start()

    def from_x(p, h, v):
        landed(p, h * 2 + 1 - lo, v * 2 + co)
        to_c(p, h, 1 - lo, v).start()

    def ag_z(p, middle=None):
        along(lambda h: from_z(p, h), middle)

    def ag_y(p):
        along(lambda h: from_y(p, h))

    def ag_x(p):
        for v in (yy, 1 - yy):
            from_x(p, hi, v)
            along(lambda h: from_x(p, h, v))

    def ag_core(p):
        @pl.loop(0, n_dp)
        def _(d):
            for v in range(n_ch // 2):
                landed(p, d, v * 2 + 1 - co)

    def ag_done(p):
        along(lambda h: to_z(p, h).wait_send())

        @pl.loop(0, n_hi)
        def _(h):
            to_y(p, h).wait_send()
            for v in range(2):
                to_x(p, h, v).wait_send()
                for l in range(2):
                    to_c(p, h, l, v).wait_send()

    def swap_in(src, dst, n, k, i):
        q = (ch + i) % n_ch
        return remote(src.at[at(q, n)], dst.at[:, my_cols], in_send.at[k, i], in_recv.at[k, i], (dp, q))

    def swap_in_wait(src, dst, n, k):
        for i in range(1, n_ch):
            q = (ch + n_ch - i) % n_ch
            remote(src.at[at(q, n)], dst.at[:, at(q, width)], in_send.at[k, i], in_recv.at[k, i], (dp, q)).wait_recv()
        for i in range(1, n_ch):
            swap_in(src, dst, n, k, i).wait_send()

    def swap_out(src, dst, n, k, i):
        q = (ch + i) % n_ch
        return remote(src.at[:, at(q, width)], dst.at[at(ch, n)], out_send.at[k, i], out_recv.at[k, i], (dp, q))

    def swap_out_wait(src, dst, n, k):
        for i in range(1, n_ch):
            q = (ch + n_ch - i) % n_ch
            remote(src.at[:, at(q, width)], dst.at[at(q, n)], out_send.at[k, i], out_recv.at[k, i], (dp, q)).wait_recv()
        for i in range(1, n_ch):
            swap_out(src, dst, n, k, i).wait_send()

    def small_swap(i, q):
        return remote(small.at[:, at(q, width)], small.at[:, at(q, width)], in_send.at[2, i], in_recv.at[2, i], (dp, (ch + i) % n_ch))

    def bounds_x():
        return remote(stats.at[0], stats.at[1], st_send.at[n_hi], st_recv.at[n_hi], (dp_x, ch))

    def bounds_z(h):
        return remote(stats.at[2], stats.at[3 + hi], st_send.at[h], st_recv.at[hi], (h * 2 + lo, ch))

    def bounds_in(h):
        return remote(stats.at[2], stats.at[3 + h], st_send.at[h], st_recv.at[h], (h * 2 + lo, ch))

    def film_block(d):
        return wf_all.at[:, at(d, frp), :]

    def film_pass(d, slot, device):
        return remote(film_block(d), film_block(d), fw_send.at[slot], fw_recv.at[d], device)

    def film_x():
        return film_pass(dp, 0, (dp_x, ch))

    def film_z(i, l):
        return film_pass(hi * 2 + l, 2 * i + l, ((hi + i) % n_hi * 2 + lo, ch))

    def film_swap(i, q):
        return remote(
            film_out.at[:, at(q, s), :], film.at[:, :, my_cols], fo_send.at[i], fo_recv.at[i], (dp, q)
        )

    bounds_x().start()
    film_x().start()
    ag_far(0)
    ag_own(0)
    ag_own(1)
    for i in range(1, n_ch):
        small_swap(i, ch).start()
    bounds_x().wait_recv()
    stats[2] = jnp.maximum(stats[0], stats[1])
    stats[3 + hi] = stats[2]
    along(lambda h: bounds_z(h).start())
    from_y(0, hi)
    ag_z(0, lambda: ag_far(1))
    for i in range(1, n_ch):
        swap_in(inputs, x_raw, m, 0, i).start()
    from_y(1, hi)
    ag_y(0)
    along(lambda h: bounds_in(h).wait_recv())
    best = stats[3]
    for h in range(1, n_hi):
        best = jnp.maximum(best, stats[3 + h])
    low = -jnp.concatenate([best[feats + i : feats + i + 1, :] for i in range(feats)], axis=1)
    span = jnp.concatenate([best[i : i + 1, :] for i in range(feats)], axis=1) - low
    slope = 2.0 / jnp.maximum(span, 1.0)
    CB = 64

    @pl.loop(0, cond.shape[0] // CB)
    def _(i):
        v = (cond[at(i, CB), :] - low) * slope - 1.0
        act[at(i, CB), :] = mish_pair(v)[0].astype(bf16)

    def film_on():
        film_pass(dp_x, 0, (dp, ch)).wait_recv()

        @pl.loop(1, n_hi)
        def _(i):
            for l in range(2):
                film_z(i, l).start()

    ag_z(1, film_on)
    ag_far(2)
    ag_x(0)

    lens_ref = lens_all.at[at(ch, s)]

    def mask(t):
        return wide((lens_ref[...] > t).astype(f32), c)

    count = wide(lens_ref[...].astype(f32), c) * GROUP
    own_x.wait()
    swap_in_wait(inputs, x_raw, m, 0)
    sb = 256 // frames
    turn = grid_turn(sb, frames)
    for b in range(s // sb):
        y = dot_nn(turn, x_raw[pl.ds(b * 256, 256), :])
        lens_b = lens_ref[pl.ds(b * sb, sb), :]
        for t in range(frames):
            keep = wide((lens_b > t).astype(f32), c)
            xpad[pl.ds((t + 2) * s + b * sb, sb), :] = (y[t * sb : (t + 1) * sb] * keep).astype(bf16)

    def conv_fwd(src, base, store):
        @pl.loop(0, c // NB)
        def _(n):
            cols = at(n, NB)
            for mi in range(m // MC):
                acc = dot_nn(src[pl.ds(mi * MC, MC), :], w_all[base, :, cols])
                for k in range(1, TAPS):
                    acc += dot_nn(src[pl.ds(mi * MC + k * s, MC), :], w_all[base + k, :, cols])
                store(pl.ds(mi * MC, MC), cols, acc)

    def conv_bwd(src, base, store):
        @pl.loop(0, c // NB)
        def _(n):
            cols = at(n, NB)
            for mi in range(m // MC):
                acc = dot_nt(src[pl.ds(mi * MC + (TAPS - 1) * s, MC), :], w_all[base, cols, :])
                for k in range(1, TAPS):
                    acc += dot_nt(src[pl.ds(mi * MC + (TAPS - 1 - k) * s, MC), :], w_all[base + k, cols, :])
                store(pl.ds(mi * MC, MC), cols, acc)

    def conv_grad(src, g, base, first, last):
        @pl.loop(first, last)
        def _(k):
            shifted = pl.ds(pl.multiple_of((TAPS - 1 - k) * s, s), m)
            for n in range(c // NB):
                cols = pl.ds(n * NB, NB)
                gw_all[base + k, :, cols] = dot_tn(src[pl.ds(2 * s, m), :], g[shifted, cols]).astype(bf16)

    def norm_stats(bias):
        tot = jnp.zeros((s, c), f32)
        for t in range(frames):
            tot += (cbuf[pl.ds(t * s, s), :] + bias) * mask(t)
        mean = group_sum(tot) / count
        tot = jnp.zeros((s, c), f32)
        for t in range(frames):
            d = (cbuf[pl.ds(t * s, s), :] + bias - mean) * mask(t)
            tot += d * d
        return mean, lax.rsqrt(group_sum(tot) / count + eps_norm)

    def row(i):
        return small[pl.ds(i, 1), :]

    def keep_c(part, cols, acc):
        cbuf[part, cols] = acc

    ag_core(0)
    ag_y(1)
    ag_own(2)
    conv_fwd(xpad, W_ONE, keep_c)
    for i in range(1, n_ch):
        small_swap(i, (ch + n_ch - i) % n_ch).wait_recv()
    bias = row(0)
    @pl.loop(1, n_hi)
    def _(i):
        for l in range(2):
            film_pass((hi + i) % n_hi * 2 + l, 0, (dp, ch)).wait_recv()

    for i in range(2):
        film_out[i] = dot_nn(act[...], wf_all[i]) + small[pl.ds(6 + i, 1), my_cols]
    for i in range(1, n_ch):
        film_swap(i, (ch + i) % n_ch).start()
    for i in range(2):
        film[i, :, my_cols] = film_out[i, at(ch, s), :]

    for n in range(c // NB):
        cols = pl.ds(n * NB, NB)
        for mi in range(m // MC):
            res[pl.ds(mi * MC, MC), cols] = dot_nn(xpad[pl.ds(2 * s + mi * MC, MC), :], w_all[W_RES, :, cols])
    mean, rstd1 = norm_stats(bias)
    ag_z(2)
    ag_x(1)
    for i in range(1, n_ch):
        swap_in(cot, cot_raw, h2, 1, i).start()
    for i in range(1, n_ch):
        q = (ch + n_ch - i) % n_ch
        remote(film_out.at[:, at(q, s), :], film.at[:, :, at(q, width)], fo_send.at[i], fo_recv.at[i], (dp, q)).wait_recv()
    for t in range(frames):
        part = pl.ds(t * s, s)
        xh = (cbuf[part, :] + bias - mean) * rstd1
        mi, dmi = mish_pair(xh * row(1) + row(2))
        xh1[part, :] = xh
        m1[part, :] = mi
        dm1[part, :] = dmi
        hpad[pl.ds((t + 2) * s, s), :] = ((film[0] * mi + film[1]) * mask(t)).astype(bf16)
    from_y(2, hi)
    ag_y(2)
    ag_core(1)
    conv_fwd(hpad, W_TWO, keep_c)
    bias = row(3)
    mean, rstd2 = norm_stats(bias)
    for t in range(frames):
        part = pl.ds(t * s, s)
        xh = (cbuf[part, :] + bias - mean) * rstd2
        mi, dmi = mish_pair(xh * row(4) + row(5))
        xh2[part, :] = xh
        dm2[part, :] = dmi
        val = ((mi + res[part, :] + row(8)) * mask(t)).astype(bf16)
        if t % 2 == 0:
            be[pl.ds(t // 2 * s, s), :] = val
        else:
            bo[pl.ds((t // 2 + 1) * s, s), :] = val
    sh = 256 // half
    turn_h = grid_turn(sh, half)
    hm = half * s
    back_h = grid_turn(half, sh)
    dbase = W_DOWN
    obuf = res.at[pl.ds(0, hm)]
    taps_in = (bo, be, bo)
    taps_at = (0, 0, s)
    ag_x(2)
    own_cot.wait()
    swap_in_wait(cot, cot_raw, h2, 1)
    for b in range(s // sh):
        y = dot_nn(turn_h, cot_raw[pl.ds(b * 256, 256), :])
        lens_b = lens_ref[pl.ds(b * sh, sh), :]
        for j in range(half):
            keep = wide((lens_b > 2 * j).astype(f32), c)
            gdn[pl.ds(j * s + b * sh, sh), :] = (y[j * sh : (j + 1) * sh] * keep).astype(bf16)

    results = []

    def side(p):
        return sum(nt for _, nt, y_first in SUMS[:p] if y_first)

    def rs_core(p, v):
        t0, nt, y_first = SUMS[p]
        return remote(
            gw_all.at[pl.ds(t0, nt), :, at(v * 2 + 1 - co, width)],
            rcb.at[pl.ds(t0, nt), :, pl.ds(v * width, width)],
            rs_send.at[p, v], rs_recv.at[p, v], (dp, ch_c),
        )

    def rs_x(p, h):
        t0, nt, y_first = SUMS[p]
        src = sidebuf if y_first else rcb
        dst = ryb if y_first else rxb
        t1 = side(p) if y_first else t0
        return remote(
            src.at[pl.ds(t1, nt), at(h * 2 + 1 - lo, rows), :],
            dst.at[pl.ds(t0, nt), at(h, rows), :],
            rz_send.at[p, n_hi + h], rz_recv.at[p, n_hi + h], (dp_x, ch),
        )

    def rs_y(p):
        t0, nt, y_first = SUMS[p]
        src = rcb if y_first else rxb
        dst = sidebuf.at[pl.ds(side(p), nt)] if y_first else ryb.at[pl.ds(t0, nt)]
        return remote(src.at[pl.ds(t0, nt), :, at(1 - yy, width)], dst, rs_send.at[p, 2], rs_recv.at[p, 2], (dp, ch_y))

    def rs_z(p, i):
        t0, nt, y_first = SUMS[p]
        h = (hi + i) % n_hi
        return remote(
            ryb.at[pl.ds(t0, nt), at(h, rows), :], rzb.at[i, pl.ds(t0, nt)], rz_send.at[p, i], rz_recv.at[p, i], (h * 2 + lo, ch)
        )

    def rs_start(p):
        for v in range(2):
            rs_core(p, v).start()

    def plus(a, b):
        return (a.astype(f32) + b.astype(f32)).astype(bf16)

    def rs_x_start(p):
        @pl.loop(0, n_hi)
        def _(h):
            rs_x(p, h).start()

    def rs_z_start(p):
        @pl.loop(1, n_hi)
        def _(i):
            rs_z(p, i).start()

    def rs_after_core(p):
        for v in range(2):
            rs_core(p, v).wait()

        @pl.loop(SUMS[p][0], SUMS[p][0] + SUMS[p][1])
        def _(k):
            for v in range(2):
                cols = pl.ds(v * width, width)
                rcb[k, :, cols] = plus(rcb[k, :, cols], gw_all[k, :, at(v * 2 + co, width)])

        if SUMS[p][2]:
            rs_y(p).start()
        else:
            rs_x_start(p)

    def rs_after_x(p):
        t0 = SUMS[p][0]

        @pl.loop(0, n_hi)
        def _(h):
            rs_x(p, h).wait()

        @pl.loop(SUMS[p][0], SUMS[p][0] + SUMS[p][1])
        def _(k):
            for h in range(n_hi):
                part = pl.ds(h * rows, rows)
                if SUMS[p][2]:
                    ryb[k, part, :] = plus(ryb[k, part, :], sidebuf[k - t0 + side(p), at(h * 2 + lo, rows), :])
                else:
                    rxb[k, part, :] = plus(rxb[k, part, :], rcb[k, at(h * 2 + lo, rows), :])

        if SUMS[p][2]:
            rs_z_start(p)
        else:
            rs_y(p).start()

    def rs_after_y(p):
        t0 = SUMS[p][0]

        rs_y(p).wait()

        @pl.loop(SUMS[p][0], SUMS[p][0] + SUMS[p][1])
        def _(k):
            if SUMS[p][2]:
                sidebuf[k - t0 + side(p)] = plus(sidebuf[k - t0 + side(p)], rcb[k, :, at(yy, width)])
            else:
                ryb[k] = plus(ryb[k], rxb[k, :, at(yy, width)])

        if SUMS[p][2]:
            rs_x_start(p)
        else:
            rs_z_start(p)

    def rs_after_z(p):
        t0, nt, y_first = SUMS[p]

        @pl.loop(1, n_hi)
        def _(i):
            rs_z(p, i).wait()

        @pl.loop(t0, t0 + nt)
        def _(k):
            def more(i, tot):
                return tot + rzb[i, k].astype(f32)

            gfin[k] = lax.fori_loop(1, n_hi, more, ryb[k, at(hi, rows), :].astype(f32))

        results.append(local(12 + p, gfin.at[pl.ds(t0, nt)], gfin_h.at[pl.ds(t0, nt)]))

    for k in range(DOWN):
        for n in range(c // NB):
            cols = pl.ds(n * NB, NB)
            gw_all[dbase + k, :, cols] = dot_tn(taps_in[k][pl.ds(taps_at[k], hm), :], gdn[pl.ds(0, hm), cols]).astype(bf16)
    rs_start(G_DOWN)
    ag_core(2)
    for n in range(c // NB):
        cols = pl.ds(n * NB, NB)
        acc = dot_nn(bo[pl.ds(0, hm), :], w_all[dbase, :, cols])
        acc += dot_nn(be[...], w_all[dbase + 1, :, cols])
        acc += dot_nn(bo[pl.ds(s, hm), :], w_all[dbase + 2, :, cols])
        obuf[:, cols] = acc
    for b in range(s // sh):
        pieces = []
        lens_b = lens_ref[pl.ds(b * sh, sh), :]
        for j in range(half):
            keep = wide((lens_b > 2 * j).astype(f32), c)
            pieces.append(((obuf[pl.ds(j * s + b * sh, sh), :] + row(9)) * keep).astype(bf16))
        out_raw[pl.ds(b * 256, 256), :] = dot_nn(back_h, jnp.concatenate(pieces, axis=0)).astype(bf16)
    for i in range(1, n_ch):
        swap_out(out_raw, output, h2, 0, i).start()
    own_out = local(2, out_raw.at[:, my_cols], output.at[at(ch, h2)])

    for n in range(c // NB):
        cols = pl.ds(n * NB, NB)
        ge = dot_nt(gdn[pl.ds(0, hm), :], w_all[dbase + 1, cols, :])
        go = dot_nt(gdn[pl.ds(0, hm), :], w_all[dbase + 2, cols, :])
        go += dot_nt(gdn[pl.ds(s, hm), :], w_all[dbase, cols, :])
        for j in range(half):
            cbuf[pl.ds(2 * j * s, s), cols] = ge[j * s : (j + 1) * s]
            cbuf[pl.ds((2 * j + 1) * s, s), cols] = go[j * s : (j + 1) * s]

    rs_after_core(G_DOWN)
    tot = jnp.zeros((s, c), f32)
    for j in range(half):
        tot += gdn[pl.ds(j * s, s), :].astype(f32)
    gs = [None] * SMALL
    gs[9] = jnp.sum(tot, axis=0, keepdims=True)
    tot = jnp.zeros((s, c), f32)
    for t in range(frames):
        part = pl.ds(t * s, s)
        g = cbuf[part, :] * mask(t)
        tot += g
        gres[part, :] = g.astype(bf16)
    gs[8] = jnp.sum(tot, axis=0, keepdims=True)
    for n in range(c // NB):
        cols = pl.ds(n * NB, NB)
        gw_all[W_RES, :, cols] = dot_tn(xpad[pl.ds(2 * s, m), :], gres[:, cols]).astype(bf16)
    rs_start(G_RES)

    def norm_back(xh, dm, gain, rstd, dst, scale):
        a1 = jnp.zeros((s, c), f32)
        a2 = jnp.zeros((s, c), f32)
        for t in range(frames):
            part = pl.ds(t * s, s)
            dy = cbuf[part, :] * mask(t) * dm[part, :]
            if scale is not None:
                dy = dy * scale
            dm[part, :] = dy
            a1 += dy
            a2 += dy * xh[part, :]
        g1 = group_sum(a1 * gain) / count
        g2 = group_sum(a2 * gain) / count
        tot = jnp.zeros((s, c), f32)
        for t in range(frames):
            part = pl.ds(t * s, s)
            dp_t = rstd * (dm[part, :] * gain - mask(t) * (g1 + xh[part, :] * g2))
            tot += dp_t
            dst[pl.ds((t + 2) * s, s), :] = dp_t.astype(bf16)
        return [jnp.sum(v, axis=0, keepdims=True) for v in (tot, a2, a1)]

    gs[3:6] = norm_back(xh2, dm2, row(4), rstd2, gc2, None)
    rs_after_core(G_RES)
    conv_bwd(gc2, W_TWO, keep_c)
    tot1 = jnp.zeros((s, c), f32)
    tot2 = jnp.zeros((s, c), f32)
    for t in range(frames):
        part = pl.ds(t * s, s)
        g = cbuf[part, :] * mask(t)
        tot1 += g * m1[part, :]
        tot2 += g
    gfilm[0] = tot1.astype(bf16)
    gfilm[1] = tot2.astype(bf16)
    gs[6] = jnp.sum(tot1, axis=0, keepdims=True)
    gs[7] = jnp.sum(tot2, axis=0, keepdims=True)

    def film_back(i):
        q = (ch + i) % n_ch
        return remote(gfilm.at[:, :, at(q, width)], gfa.at[:, at(ch, s), :], gf_send.at[i], gf_recv.at[i], (dp, q))

    for i in range(1, n_ch):
        film_back(i).start()
    gfa[:, at(ch, s), :] = gfilm[:, :, my_cols]
    conv_grad(hpad, gc2, W_TWO, 0, 3)
    rs_start(G_TWO_A)
    conv_grad(hpad, gc2, W_TWO, 3, TAPS)
    rs_start(G_TWO_B)
    rs_after_core(G_TWO_A)
    gs[0:3] = norm_back(xh1, dm1, row(1), rstd1, gc1, film[0])
    for i in range(1, n_ch):
        q = (ch + n_ch - i) % n_ch
        remote(gfilm.at[:, :, at(q, width)], gfa.at[:, at(q, s), :], gf_send.at[i], gf_recv.at[i], (dp, q)).wait_recv()
    for i in range(2):
        gwf[i] = dot_tn(act[...], gfa[i]).astype(bf16)

    def rf_z(i):
        h = (hi + i) % n_hi
        return remote(gwf.at[:, at(h, 2 * frp), :], rfz.at[i], rf_send.at[i], rf_recv.at[i], (h * 2 + lo, ch))

    def rf_x():
        return remote(rfs.at[:, at(1 - lo, frp), :], rfx, rf_send.at[0], rf_recv.at[0], (dp_x, ch))

    @pl.loop(1, n_hi)
    def _(i):
        rf_z(i).start()

    rs_after_core(G_TWO_B)
    rs_after_y(G_DOWN)
    rs_after_x(G_RES)
    zero = jnp.zeros((1, c), f32)
    for i in range(SMALL):
        gsm[pl.ds(i, 1), :] = gs[i] if gs[i] is not None else zero

    def small_pass(i, device):
        return remote(gsm, gsr.at[i], gs_send.at[i], gs_recv.at[i], device)

    small_pass(0, (dp, ch_c)).start()
    def keep_ig(part, cols, acc):
        cbuf[part, cols] = acc + dot_nt(gres[part, :], w_all[W_RES, cols, :])

    conv_bwd(gc1, W_ONE, keep_ig)
    back = grid_turn(frames, sb)
    for b in range(s // sb):
        lens_b = lens_ref[pl.ds(b * sb, sb), :]
        pieces = [
            (cbuf[pl.ds(t * s + b * sb, sb), :] * wide((lens_b > t).astype(f32), c)).astype(bf16) for t in range(frames)
        ]
        ig_raw[pl.ds(b * 256, 256), :] = dot_nn(back, jnp.concatenate(pieces, axis=0)).astype(bf16)
    rs_after_x(G_TWO_A)
    for i in range(1, n_ch):
        swap_out(ig_raw, input_grad, m, 1, i).start()
    own_ig = local(3, ig_raw.at[:, my_cols], input_grad.at[at(ch, m)])

    small_pass(0, (dp, ch_c)).wait()
    gsm[...] += gsr[0]
    small_pass(1, (dp_x, ch)).start()
    conv_grad(xpad, gc1, W_ONE, 0, 2)
    rs_start(G_ONE_A)
    rs_after_y(G_TWO_B)
    conv_grad(xpad, gc1, W_ONE, 2, 4)
    rs_start(G_ONE_B)
    rs_after_core(G_ONE_A)
    rs_after_x(G_DOWN)
    conv_grad(xpad, gc1, W_ONE, 4, 5)
    rs_start(G_ONE_C)
    rs_after_core(G_ONE_B)
    rs_after_y(G_RES)
    rs_after_core(G_ONE_C)
    small_pass(1, (dp_x, ch)).wait()
    gsm[...] += gsr[1]
    small_pass(2, (dp, ch_y)).start()
    rs_after_y(G_TWO_A)
    rs_after_x(G_TWO_B)
    @pl.loop(1, n_hi)
    def _(i):
        rf_z(i).wait()

    for v in range(2):
        def more(i, tot):
            return tot + rfz[i, v].astype(f32)

        rfs[v] = lax.fori_loop(1, n_hi, more, gwf[v, at(hi, 2 * frp), :].astype(f32)).astype(bf16)
    rf_x().start()
    for p in range(3):
        ag_done(p)
    bounds_x().wait_send()
    along(lambda h: bounds_z(h).wait_send())

    @pl.loop(1, n_hi)
    def _(i):
        for l in range(2):
            film_z(i, l).wait_send()

    film_x().wait_send()
    for i in range(1, n_ch):
        small_swap(i, ch).wait_send()
        film_swap(i, (ch + i) % n_ch).wait_send()
        film_back(i).wait_send()
    rs_after_z(G_RES)
    rs_after_z(G_DOWN)
    rs_after_x(G_ONE_A)
    rs_after_z(G_TWO_B)
    rs_after_x(G_ONE_B)
    small_pass(2, (dp, ch_y)).wait()
    gsm[...] += gsr[2]

    def small_z(i):
        return small_pass(2 + i, ((hi + i) % n_hi * 2 + lo, ch))

    @pl.loop(1, n_hi)
    def _(i):
        small_z(i).start()

    rs_after_y(G_ONE_A)
    rs_after_x(G_ONE_C)
    rs_after_z(G_TWO_A)
    rf_x().wait()
    for v in range(2):
        gffin[v] = rfs[v, at(lo, frp), :].astype(f32) + rfx[v].astype(f32)
    results.append(local(12 + len(SUMS), gffin, gffin_h))

    rs_after_y(G_ONE_B)
    rs_after_y(G_ONE_C)
    rs_after_z(G_ONE_A)
    @pl.loop(1, n_hi)
    def _(i):
        small_z(i).wait()

    def more_small(i, tot):
        return tot + gsr[2 + i, :, my_cols]

    gsfin[...] = lax.fori_loop(1, n_hi, more_small, gsm[:, my_cols])
    results.append(local(13 + len(SUMS), gsfin, gsfin_h))
    rs_after_z(G_ONE_B)
    rs_after_z(G_ONE_C)

    for copy in results:
        copy.wait()
    own_out.wait()
    own_ig.wait()
    swap_out_wait(out_raw, output, h2, 0)
    swap_out_wait(ig_raw, input_grad, m, 1)


def block_step(n_dp, n_ch, inputs, cot, cond, lens, one_w, two_w, res_w, down_w, film_w, small_w):
    rows, width = res_w.shape
    c = rows * n_dp
    samples = lens.shape[1]
    s = samples // n_ch
    m = inputs.shape[0] // n_ch
    h = m // 2
    frp = film_w.shape[0]
    feats = cond.shape[1]
    n_hi = n_dp // 2
    taps = N_TAPS
    V = pltpu.VMEM
    D = pltpu.SemaphoreType.DMA
    hbm = pl.BlockSpec(memory_space=pl.ANY)
    out = [
        jax.ShapeDtypeStruct((h * n_ch, width), bf16),
        jax.ShapeDtypeStruct((m * n_ch, width), bf16),
        jax.ShapeDtypeStruct((taps, rows, width), f32),
        jax.ShapeDtypeStruct((2, frp, width), f32),
        jax.ShapeDtypeStruct((SMALL, width), f32),
    ]
    pad = V((m + 4 * s, c), bf16)
    full = V((m, c), f32)
    scratch = [
        V((taps, c, c), bf16), V((taps, c, c), bf16), V((m, c), bf16), V((h, c), bf16), V((h, c), bf16), V((m, c), bf16),
        V((SMALL, c), f32), V((3 + n_hi, -(-feats // 512) * 8, 128), f32), V((samples, feats), bf16), V((2, n_dp * frp, width), bf16),
        V((2, samples, width), f32), V((2, s, c), f32), V((2, s, c), bf16), V((2, samples, width), bf16), V((2, n_dp * frp, width), bf16),
        *[V(o.shape, o.dtype) for o in out[2:]],
        V((taps, c, 2 * width), bf16), V((taps, n_hi * rows, 2 * width), bf16), V((taps, n_hi * rows, width), bf16), V((sum(nt for _, nt, y_first in SUMS if y_first), c, width), bf16),
        V((n_hi, taps, rows, width), bf16), V((2, frp, width), bf16), V((n_hi, 2, 2 * frp, width), bf16), V((2, 2 * frp, width), bf16),
        V((SMALL, c), f32), V((2 + n_hi, SMALL, c), f32),
        V((samples, feats), f32), V((1, samples), jnp.int32), V((samples, 128), f32), V((taps, rows, width), f32), V(film_w.shape, f32), V(small_w.shape, f32),
        pad, pad, V((h, c), bf16), V((h + s, c), bf16),
        full, full, full, full, full, full, full,
        V((h + s, c), bf16), pad, pad, V((m, c), bf16),
        D((3, 8 * n_hi)), D((3, n_dp, n_ch)), D((n_hi + 1,)), D((n_hi + 1,)), D((3, n_ch)), D((3, n_ch)),
        D((2 * n_hi,)), D((n_dp,)), D((n_ch,)), D((n_ch,)),
        D((len(SUMS), 3)), D((len(SUMS), 3)), D((len(SUMS), 2 * n_hi)), D((len(SUMS), 2 * n_hi)), D((2, n_ch)), D((2, n_ch)), D((n_ch,)), D((n_ch,)),
        D((n_hi,)), D((n_hi,)), D((2 + n_hi,)), D((2 + n_hi,)), D((14 + len(SUMS),)),
    ]
    return pl.pallas_call(
        partial(step_kernel, n_dp, n_ch),
        out_shape=out,
        in_specs=[hbm] * 10,
        out_specs=[hbm] * 5,
        scratch_shapes=scratch,
        compiler_params=pltpu.CompilerParams(vmem_limit_bytes=63 << 20, collective_id=0, has_side_effects=True),
        name="block_step",
    )(inputs, cot, cond, lens, one_w, two_w, res_w, down_w, film_w, small_w)


beta_one = 0.9
beta_two = 0.999
adam_eps = 1e-08
weight_decay = 0.01
rate_large = 0.05
rate_small = 0.3
adam_step = 10


def adam_update(weight, gradient, old_first, old_second, learn_rate, decay_term):
    first_new = beta_one * old_first + (1.0 - beta_one) * gradient
    second_new = beta_two * old_second + (1.0 - beta_two) * gradient * gradient
    step_size = (
        first_new
        / (1.0 - beta_one**adam_step)
        / (jnp.sqrt(second_new / (1.0 - beta_two**adam_step)) + adam_eps)
    )
    return (first_new, second_new, weight - learn_rate * (step_size + decay_term * weight))


def update_kernel(n, a_in, b_in, *refs):
    ins, a_out, b_out, refs = refs[:n], refs[n], refs[n + 1], refs[n + 2 :]
    outs, bufs, results, refs = refs[: n - 3], refs[n - 3 : 2 * n - 3], refs[2 * n - 3 : 3 * n - 6], refs[3 * n - 6 :]
    a_buf, b_buf, sem_in, sem_out, sem_ab = refs
    order = (2, 4, 5, 3, 1, 0)
    loads = [pltpu.make_async_copy(ins[i], bufs[i], sem_in.at[i]) for i in range(n)]
    stores = [pltpu.make_async_copy(results[i], outs[i], sem_out.at[i]) for i in range(n - 3)]
    gw, gf, gs = bufs[:3]
    big = [pltpu.make_async_copy(src, dst, sem_ab.at[i]) for i, (src, dst) in enumerate(((a_in, a_buf), (b_in, b_buf), (a_buf, a_out), (b_buf, b_out)))]
    for copy in loads[:3]:
        copy.start()
    for i in order:
        for j in range(3):
            loads[3 + 3 * i + j].start()
    big[0].start()
    big[1].start()

    def put(i, index, grad, rate, decay):
        w, m, v = (bufs[3 + 3 * i + j][index] for j in range(3))
        for j, value in enumerate(adam_update(w, grad, m, v, rate, decay)):
            results[3 * i + j][index] = value

    for copy in loads[:3]:
        copy.wait()
    frows = ins[3 + 12].shape[0]
    for i in order:
        for j in range(3):
            loads[3 + 3 * i + j].wait()
        if i in (0, 1, 3):
            base, taps = ((W_ONE, TAPS), (W_TWO, TAPS), None, (W_DOWN, DOWN))[i]
            for k in range(taps):
                put(i, k, gw[base + k], rate_large, weight_decay)
        elif i == 2:
            put(i, ..., gw[W_RES], rate_large, weight_decay)
        elif i == 4:
            for k in range(2):
                put(i, (slice(None), k), gf[k, pl.ds(0, frows), :], rate_large, weight_decay)
        else:
            put(i, ..., gs[pl.ds(0, ins[3 + 15].shape[0]), :], rate_small, 0.0)
        for j in range(3):
            stores[3 * i + j].start()
    for i in range(2):
        big[i].wait()
        big[2 + i].start()
    for copy in stores:
        copy.wait()
    big[2].wait()
    big[3].wait()


def update(output, input_grad, gw, gf, gs, *state):
    hbm = pl.BlockSpec(memory_space=pl.ANY)
    acts = (output, input_grad)
    arrays = (gw, gf, gs, *state)
    n = len(arrays)
    bufs = [pltpu.VMEM(a.shape, f32) for a in arrays]
    return pl.pallas_call(
        partial(update_kernel, n),
        out_shape=[jax.ShapeDtypeStruct(a.shape, a.dtype) for a in (*acts, *state)],
        in_specs=[hbm] * (n + 2),
        out_specs=[hbm] * (len(state) + 2),
        scratch_shapes=[
            *bufs, *bufs[3:], *[pltpu.VMEM(a.shape, a.dtype) for a in acts],
            pltpu.SemaphoreType.DMA((n,)), pltpu.SemaphoreType.DMA((n,)), pltpu.SemaphoreType.DMA((4,)),
        ],
        compiler_params=pltpu.CompilerParams(vmem_limit_bytes=60 << 20),
        name="update",
    )(*acts, *arrays)


def body(
    inputs, condition, lengths, cotangent,
    conv1_w, conv1_m, conv1_v, conv2_w, conv2_m, conv2_v, res_w, res_m, res_v,
    down_w, down_m, down_v, film_w, film_m, film_v, small_w, small_m, small_v,
):
    n_dp, n_ch = lax.axis_size("dp"), lax.axis_size("chan")
    lens = lengths.reshape(1, -1)

    def taps_first(*arrays):
        return tuple(jnp.transpose(a, (1, 0, 2)) for a in arrays)

    one, two, down = (
        taps_first(*state) for state in ((conv1_w, conv1_m, conv1_v), (conv2_w, conv2_m, conv2_v), (down_w, down_m, down_v))
    )
    cond, film_rows = condition, film_w
    frows = film_w.shape[0]
    if frows % 16:
        short = -frows % 16
        film_rows = jnp.pad(film_w, ((0, short), (0, 0), (0, 0)))
        cond = jnp.pad(condition.reshape(-1, n_dp, frows), ((0, 0), (0, 0), (0, short))).reshape(condition.shape[0], -1)
    output, input_grad, gw, gf, gs = block_step(
        n_dp, n_ch, inputs, cotangent, cond, lens, one[0], two[0], res_w, down[0], film_rows, small_w
    )
    output, input_grad, *state = update(
        output, input_grad, gw, gf, gs, *one, *two, res_w, res_m, res_v, *down, film_w, film_m, film_v, small_w, small_m, small_v
    )
    state = (*taps_first(*state[:6]), *state[6:9], *taps_first(*state[9:12]), *state[12:])
    return (output, input_grad, *state)


def solution(mesh):
    in_specs = (
        P("dp", "chan"),
        P("dp", None),
        P("dp"),
        P("dp", "chan"),
        P("dp", None, "chan"),
        P("dp", None, "chan"),
        P("dp", None, "chan"),
        P("dp", None, "chan"),
        P("dp", None, "chan"),
        P("dp", None, "chan"),
        P("dp", "chan"),
        P("dp", "chan"),
        P("dp", "chan"),
        P("dp", None, "chan"),
        P("dp", None, "chan"),
        P("dp", None, "chan"),
        P("dp", None, "chan"),
        P("dp", None, "chan"),
        P("dp", None, "chan"),
        P(None, "chan"),
        P(None, "chan"),
        P(None, "chan"),
    )
    out_specs = (
        P("dp", "chan"),
        P("dp", "chan"),
        P("dp", None, "chan"),
        P("dp", None, "chan"),
        P("dp", None, "chan"),
        P("dp", None, "chan"),
        P("dp", None, "chan"),
        P("dp", None, "chan"),
        P("dp", "chan"),
        P("dp", "chan"),
        P("dp", "chan"),
        P("dp", None, "chan"),
        P("dp", None, "chan"),
        P("dp", None, "chan"),
        P("dp", None, "chan"),
        P("dp", None, "chan"),
        P("dp", None, "chan"),
        P(None, "chan"),
        P(None, "chan"),
        P(None, "chan"),
    )
    return jax.shard_map(body, mesh=mesh, in_specs=in_specs, out_specs=out_specs, check_vma=False)
```

```python
from functools import partial

import jax
import jax.numpy as jnp
from jax import lax
from jax.experimental import pallas as pl
from jax.experimental.pallas import tpu as pltpu
from jax.sharding import PartitionSpec as P

f32, bf16 = jnp.float32, jnp.bfloat16
GROUP = 64
TAPS = 5
DOWN = 3
eps_norm = 1e-05


def dot_nn(a, b):
    return lax.dot_general(a, b, (((1,), (0,)), ((), ())), preferred_element_type=f32)


def dot_nt(a, b):
    return lax.dot_general(a, b, (((1,), (1,)), ((), ())), preferred_element_type=f32)


def dot_tn(a, b):
    return lax.dot_general(a, b, (((0,), (0,)), ((), ())), preferred_element_type=f32)


def mish_pair(v):
    u = jnp.exp(-jnp.abs(v))
    pos = v >= 0
    num = jnp.where(pos, 1.0 + 2.0 * u, u * (u + 2.0))
    q = jnp.where(pos, 2.0 * u * u, 2.0)
    r = 1.0 / (num + q)
    w = num * r
    sig = jnp.where(pos, 1.0, u) / (1.0 + u)
    return v * w, w + v * sig * ((q * r) * ((2.0 * num + q) * r))


def wide(tile, lanes):
    return jnp.concatenate([tile] * (lanes // tile.shape[1]), axis=1)


def grid_turn(outer, inner):
    n = outer * inner
    row = lax.broadcasted_iota(jnp.int32, (n, n), 0)
    col = lax.broadcasted_iota(jnp.int32, (n, n), 1)
    return ((row % outer) * inner + row // outer == col).astype(bf16)


def group_sum(values):
    s, c = values.shape
    row = lax.broadcasted_iota(jnp.int32, (128, 128), 0)
    col = lax.broadcasted_iota(jnp.int32, (128, 128), 1)
    ones = (row // GROUP == col // GROUP).astype(f32)
    tall = jnp.concatenate([values[:, i : i + 128] for i in range(0, c, 128)], axis=0)
    tot = lax.dot_general(tall, ones, (((1,), (0,)), ((), ())), precision=lax.Precision.HIGHEST, preferred_element_type=f32)
    return jnp.concatenate([tot[i * s : (i + 1) * s] for i in range(c // 128)], axis=1)


MESH = pl.DeviceIdType.MESH
W_ONE, W_RES, W_TWO, W_DOWN = 0, TAPS, TAPS + 1, 2 * TAPS + 1
N_TAPS = W_DOWN + DOWN
PARTS = ((W_ONE, TAPS + 1), (W_TWO, TAPS), (W_DOWN, DOWN))
GROUPS = ("DOWN", "RES", "TWO_A", "TWO_B", "ONE_A", "ONE_B", "ONE_C")
SUMS = (
    (W_DOWN, 3, True),
    (W_RES, 1, False),
    (W_TWO, 3, False),
    (W_TWO + 3, 2, True),
    (W_ONE, 2, False),
    (W_ONE + 2, 2, False),
    (W_ONE + 4, 1, False),
)
BACKWARD = (
    "gW_DOWN", "s_DOWN", "C2", "gblock", "gres", "gW_RES", "c_DOWN", "s_RES", "nb2", "gW_TWO_A", "c_RES",
    "s_TWO_A", "cb2", "filmg", "c_TWO_A", "nb1", "x_RES", "downf", "gW_ONE_A", "s_ONE_A", "y_RES", "gW_ONE_C",
    "fdot", "gW_TWO_B", "c_ONE_A", "small", "gW_ONE_B", "smy", "x_TWO_A", "s_ONE_C", "s_TWO_B", "cb1",
    "s_ONE_B", "c_ONE_C", "smx", "c_TWO_B", "c_ONE_B", "y_DOWN", "y_TWO_A", "x_ONE_A", "x_ONE_C", "y_ONE_A",
    "x_ONE_B", "y_TWO_B", "y_ONE_C", "ig", "x_DOWN", "z_ONE_C", "x_TWO_B", "z_DOWN", "y_ONE_B", "z_TWO_A",
    "fz", "smz", "z_ONE_A", "z_ONE_B", "z_RES", "fe", "z_TWO_B", "sme",
)
SMALL = 16


def step_kernel(
    n_dp, n_ch,
    inputs, cot, cond_h, lens_h, one_w, two_w, res_w, down_w, film_h, small_h,
    output, input_grad, gfin_h, gffin_h, gsfin_h,
    w_all, gw_all, x_raw, cot_raw, out_raw, ig_raw, small, stats, act, wf_all, film_out, film, gfilm, gfa, gwf,
    gfin, gffin, gsfin, rcb, rxb, ryb, sidebuf, rzb, rfx, rfz, rfs, gsm, gsr, cond, lens_row, lens_all, wraw, film_w, small_w,
    xpad, hpad, be, bo, cbuf, res, xh1, m1, dm1, xh2, dm2, gdn, gc2, gc1, gres,
    ag_send, ag_recv, st_send, st_recv, in_send, in_recv, fw_send, fw_recv, fo_send, fo_recv,
    rs_send, rs_recv, out_send, out_recv, gf_send, gf_recv, rf_send, rf_recv, gs_send, gs_recv, loc,
):
    dp, ch = lax.axis_index("dp"), lax.axis_index("chan")
    hi, lo, yy, co = dp // 2, dp % 2, ch // 2, ch % 2
    n_hi = n_dp // 2
    dp_x = hi * 2 + 1 - lo
    ch_y = (1 - yy) * 2 + co
    ch_c = yy * 2 + 1 - co
    m, c = x_raw.shape
    h2 = m // 2
    rows, width = res_w.shape
    frp = film_h.shape[0]
    s = lens_h.shape[1] // n_ch
    frames = m // s
    half = frames // 2
    MC = 256 if m % 256 == 0 else m
    NB = 256

    def at(index, size):
        return pl.ds(pl.multiple_of(index * size, size), size)

    def remote(src, dst, ss, rs, device):
        return pltpu.make_async_remote_copy(
            src_ref=src, dst_ref=dst, send_sem=ss, recv_sem=rs, device_id=device, device_id_type=MESH
        )

    barrier = pltpu.get_barrier_semaphore()

    @pl.loop(1, n_dp)
    def _(i):
        pl.semaphore_signal(barrier, inc=1, device_id=((dp + i) % n_dp, ch), device_id_type=MESH)

    for i in range(1, n_ch):
        pl.semaphore_signal(barrier, inc=1, device_id=(dp, (ch + i) % n_ch), device_id_type=MESH)

    def local(i, src, dst):
        copy = pltpu.make_async_copy(src, dst, loc.at[i])
        copy.start()
        return copy

    own_x = local(0, inputs.at[at(ch, m)], x_raw.at[:, at(ch, width)])
    own_cot = local(1, cot.at[at(ch, h2)], cot_raw.at[:, at(ch, width)])
    staged = [
        local(4, cond_h, cond), local(5, lens_h, lens_row), local(6, small_h, small_w),
        local(7, one_w, wraw.at[pl.ds(W_ONE, TAPS)]), local(8, two_w, wraw.at[pl.ds(W_TWO, TAPS)]),
        local(9, down_w, wraw.at[pl.ds(W_DOWN, DOWN)]), local(10, res_w, wraw.at[W_RES]), local(11, film_h, film_w),
    ]
    pad0 = jnp.zeros((2 * s, c), bf16)
    for ref in (xpad, hpad, gc2, gc1):
        ref[pl.ds(0, 2 * s), :] = pad0
        ref[pl.ds((frames + 2) * s, 2 * s), :] = pad0
    bo[pl.ds(0, s), :] = pad0[:s]
    gdn[pl.ds(half * s, s), :] = pad0[:s]
    for copy in staged:
        copy.wait()
    my_rows, my_cols = at(dp, rows), at(ch, width)

    @pl.loop(0, N_TAPS)
    def _(k):
        w_all[k, my_rows, my_cols] = wraw[k].astype(bf16)

    for i in range(2):
        wf_all[i, at(dp, frp), :] = film_w[:, i, :].astype(bf16)
    n_all = lens_all.shape[0]
    on_line = lax.broadcasted_iota(jnp.int32, (n_all, n_all), 0) == lax.broadcasted_iota(jnp.int32, (n_all, n_all), 1)
    across = jnp.sum(jnp.where(on_line, lens_row[...].astype(f32), 0.0), axis=1, keepdims=True)
    lens_all[...] = jnp.broadcast_to(across, lens_all.shape)
    small[pl.ds(0, small_w.shape[0]), my_cols] = small_w[...]
    small[pl.ds(small_w.shape[0], SMALL - small_w.shape[0]), my_cols] = jnp.zeros((SMALL - small_w.shape[0], width), f32)
    values = cond[...]
    feats = values.shape[1] // 128
    ends = (jnp.max(values, axis=0, keepdims=True), jnp.max(-values, axis=0, keepdims=True))
    for e in range(2):
        for i in range(feats):
            stats[0, pl.ds(e * feats + i, 1), :] = ends[e][:, i * 128 : (i + 1) * 128]
    if stats.shape[1] > 2 * feats:
        stats[0, pl.ds(2 * feats, stats.shape[1] - 2 * feats), :] = jnp.zeros((stats.shape[1] - 2 * feats, 128), f32)
    pl.semaphore_wait(barrier, n_dp - 1 + n_ch - 1)

    def arrived(ref, sem):
        remote(ref, ref, sem, sem, (dp, ch)).wait_recv()

    def gone(ref, sem):
        remote(ref, ref, sem, sem, (dp, ch)).wait_send()

    others = (n_ch - 1) * width

    far, near = hi // 2, hi % 2
    if n_hi == 4:
        line = (far * 2 + 1 - near, (1 - far) * 2 + far, (1 - far) * 3)
    else:
        line = None

    def along(step, middle=None):
        if line is not None:
            for j, h in enumerate(line):
                step(h)
                if j == 1 and middle is not None:
                    middle()
        else:

            @pl.loop(1, n_hi)
            def _(i):
                step((hi + i) % n_hi)

            if middle is not None:
                middle()

    def block(p, d, q):
        t0, nt = PARTS[p]
        return w_all.at[pl.ds(t0, nt), at(d, rows), at(q, width)]

    def pass_on(p, d, q, s_at, r_at, device):
        return remote(block(p, d, q), block(p, d, q), ag_send.at[p, s_at], ag_recv.at[p, r_at], device)

    def to_z(p, h):
        return pass_on(p, dp, ch, 0, hi, (h * 2 + lo, ch))

    def to_y(p, h):
        return pass_on(p, h * 2 + lo, ch, 1, n_hi + h, (dp, ch_y))

    def to_x(p, h, v):
        return pass_on(p, h * 2 + lo, v * 2 + co, 2, 2 * n_hi + v, (dp_x, ch))

    def to_c(p, h, l, v):
        return pass_on(p, h * 2 + l, v * 2 + co, 3, 2 * n_hi + 2, (dp, ch_c))

    def landed(p, n_rows, n_cols, at_sem):
        t0, nt = PARTS[p]
        arrived(w_all.at[pl.ds(t0, nt), pl.ds(0, n_rows), pl.ds(0, n_cols)], ag_recv.at[p, at_sem])

    def ag_far(p):
        along(lambda h: to_z(p, h).start())

    def ag_own(p):
        to_y(p, hi).start()
        to_x(p, hi, yy).start()
        to_c(p, hi, lo, yy).start()

    def from_z(p, h):
        landed(p, rows, width, h)
        to_y(p, h).start()
        to_x(p, h, yy).start()
        to_c(p, h, lo, yy).start()

    def from_y(p, h):
        landed(p, rows, width, n_hi + h)
        to_x(p, h, 1 - yy).start()
        to_c(p, h, lo, 1 - yy).start()

    def ag_z(p, middle=None):
        along(lambda h: from_z(p, h), middle)

    def ag_y(p):
        along(lambda h: from_y(p, h))

    def ag_x(p):
        for v in (yy, 1 - yy):
            landed(p, n_hi * rows, width, 2 * n_hi + v)

            @pl.loop(0, n_hi)
            def _(h):
                to_c(p, h, 1 - lo, v).start()

    def ag_core(p):
        landed(p, c, 2 * width, 2 * n_hi + 2)

    def ag_done(p):
        t0, nt = PARTS[p]
        for i, (n_rows, n_cols) in enumerate((((n_hi - 1) * rows, width), (n_hi * rows, width), (c, width), (c, 2 * width))):
            gone(w_all.at[pl.ds(t0, nt), pl.ds(0, n_rows), pl.ds(0, n_cols)], ag_send.at[p, i])

    def swap_in(src, dst, n, k, i):
        q = (ch + i) % n_ch
        return remote(src.at[at(q, n)], dst.at[:, my_cols], in_send.at[k], in_recv.at[k], (dp, q))

    def swap_in_wait(dst, k):
        arrived(dst.at[:, pl.ds(0, others)], in_recv.at[k])
        gone(dst.at[:, pl.ds(0, others)], in_send.at[k])

    def swap_out(src, dst, n, k, i):
        q = (ch + i) % n_ch
        return remote(src.at[:, at(q, width)], dst.at[at(ch, n)], out_send.at[k], out_recv.at[k], (dp, q))

    def swap_out_wait(src, dst, n, k):
        arrived(dst.at[pl.ds(0, (n_ch - 1) * n)], out_recv.at[k])
        gone(src.at[:, pl.ds(0, others)], out_send.at[k])

    def small_swap(i):
        return remote(small.at[:, my_cols], small.at[:, my_cols], in_send.at[2], in_recv.at[2], (dp, (ch + i) % n_ch))

    def bounds_x():
        return remote(stats.at[0], stats.at[1], st_send.at[0], st_recv.at[0], (dp_x, ch))

    def bounds_z(h):
        return remote(stats.at[2], stats.at[3 + hi], st_send.at[1], st_recv.at[1], (h * 2 + lo, ch))

    def film_block(d):
        return wf_all.at[:, at(d, frp), :]

    def film_pass(d, at_sem, device):
        return remote(film_block(d), film_block(d), fw_send.at[at_sem], fw_recv.at[at_sem], device)

    def film_x():
        return film_pass(dp, 0, (dp_x, ch))

    def film_z(i, l):
        return film_pass(hi * 2 + l, 1, ((hi + i) % n_hi * 2 + lo, ch))

    def film_swap(i, q):
        return remote(
            film_out.at[:, at(q, s), :], film.at[:, :, my_cols], fo_send.at[0], fo_recv.at[0], (dp, q)
        )

    bounds_x().start()
    film_x().start()
    ag_far(0)
    ag_own(0)
    ag_own(1)
    for i in range(1, n_ch):
        small_swap(i).start()
    bounds_x().wait_recv()
    stats[2] = jnp.maximum(stats[0], stats[1])
    stats[3 + hi] = stats[2]
    along(lambda h: bounds_z(h).start())
    from_y(0, hi)
    ag_z(0, lambda: ag_far(1))
    for i in range(1, n_ch):
        swap_in(inputs, x_raw, m, 0, i).start()
    from_y(1, hi)
    ag_y(0)
    arrived(stats.at[pl.ds(3, n_hi - 1)], st_recv.at[1])
    best = stats[3]
    for h in range(1, n_hi):
        best = jnp.maximum(best, stats[3 + h])
    low = -jnp.concatenate([best[feats + i : feats + i + 1, :] for i in range(feats)], axis=1)
    span = jnp.concatenate([best[i : i + 1, :] for i in range(feats)], axis=1) - low
    slope = 2.0 / jnp.maximum(span, 1.0)
    CB = 64

    @pl.loop(0, cond.shape[0] // CB)
    def _(i):
        v = (cond[at(i, CB), :] - low) * slope - 1.0
        act[at(i, CB), :] = mish_pair(v)[0].astype(bf16)

    def film_on():
        film_pass(dp_x, 0, (dp, ch)).wait_recv()

        @pl.loop(1, n_hi)
        def _(i):
            for l in range(2):
                film_z(i, l).start()

    ag_z(1, film_on)
    ag_far(2)
    ag_x(0)

    lens_ref = lens_all.at[at(ch, s)]

    def mask(t):
        return wide((lens_ref[...] > t).astype(f32), c)

    count = wide(lens_ref[...].astype(f32), c) * GROUP
    own_x.wait()
    swap_in_wait(x_raw, 0)
    sb = 256 // frames
    turn = grid_turn(sb, frames)
    for b in range(s // sb):
        y = dot_nn(turn, x_raw[pl.ds(b * 256, 256), :])
        lens_b = lens_ref[pl.ds(b * sb, sb), :]
        for t in range(frames):
            keep = wide((lens_b > t).astype(f32), c)
            xpad[pl.ds((t + 2) * s + b * sb, sb), :] = (y[t * sb : (t + 1) * sb] * keep).astype(bf16)

    def conv_fwd(src, base, store):
        @pl.loop(0, c // NB)
        def _(n):
            cols = at(n, NB)
            for mi in range(m // MC):
                acc = dot_nn(src[pl.ds(mi * MC, MC), :], w_all[base, :, cols])
                for k in range(1, TAPS):
                    acc += dot_nn(src[pl.ds(mi * MC + k * s, MC), :], w_all[base + k, :, cols])
                store(pl.ds(mi * MC, MC), cols, acc)

    def conv_bwd(src, base, store):
        @pl.loop(0, c // NB)
        def _(n):
            cols = at(n, NB)
            for mi in range(m // MC):
                acc = dot_nt(src[pl.ds(mi * MC + (TAPS - 1) * s, MC), :], w_all[base, cols, :])
                for k in range(1, TAPS):
                    acc += dot_nt(src[pl.ds(mi * MC + (TAPS - 1 - k) * s, MC), :], w_all[base + k, cols, :])
                store(pl.ds(mi * MC, MC), cols, acc)

    def conv_grad(src, g, base, first, last):
        @pl.loop(first, last)
        def _(k):
            shifted = pl.ds(pl.multiple_of((TAPS - 1 - k) * s, s), m)
            for n in range(c // NB):
                cols = pl.ds(n * NB, NB)
                gw_all[base + k, :, cols] = dot_tn(src[pl.ds(2 * s, m), :], g[shifted, cols]).astype(bf16)

    def norm_stats(bias):
        tot = jnp.zeros((s, c), f32)
        for t in range(frames):
            tot += (cbuf[pl.ds(t * s, s), :] + bias) * mask(t)
        mean = group_sum(tot) / count
        tot = jnp.zeros((s, c), f32)
        for t in range(frames):
            d = (cbuf[pl.ds(t * s, s), :] + bias - mean) * mask(t)
            tot += d * d
        return mean, lax.rsqrt(group_sum(tot) / count + eps_norm)

    def row(i):
        return small[pl.ds(i, 1), :]

    def keep_c(part, cols, acc):
        cbuf[part, cols] = acc

    ag_core(0)
    ag_y(1)
    ag_own(2)
    conv_fwd(xpad, W_ONE, keep_c)
    arrived(small.at[:, pl.ds(0, others)], in_recv.at[2])
    bias = row(0)
    arrived(wf_all.at[:, pl.ds(0, 2 * (n_hi - 1) * frp), :], fw_recv.at[1])

    for i in range(2):
        film_out[i] = dot_nn(act[...], wf_all[i]) + small[pl.ds(6 + i, 1), my_cols]
    for i in range(1, n_ch):
        film_swap(i, (ch + i) % n_ch).start()
    for i in range(2):
        film[i, :, my_cols] = film_out[i, at(ch, s), :]

    for n in range(c // NB):
        cols = pl.ds(n * NB, NB)
        for mi in range(m // MC):
            res[pl.ds(mi * MC, MC), cols] = dot_nn(xpad[pl.ds(2 * s + mi * MC, MC), :], w_all[W_RES, :, cols])
    mean, rstd1 = norm_stats(bias)
    ag_z(2)
    ag_x(1)
    for i in range(1, n_ch):
        swap_in(cot, cot_raw, h2, 1, i).start()
    arrived(film.at[:, :, pl.ds(0, others)], fo_recv.at[0])
    for t in range(frames):
        part = pl.ds(t * s, s)
        xh = (cbuf[part, :] + bias - mean) * rstd1
        mi, dmi = mish_pair(xh * row(1) + row(2))
        xh1[part, :] = xh
        m1[part, :] = mi
        dm1[part, :] = dmi
        hpad[pl.ds((t + 2) * s, s), :] = ((film[0] * mi + film[1]) * mask(t)).astype(bf16)
    from_y(2, hi)
    ag_y(2)
    ag_core(1)
    conv_fwd(hpad, W_TWO, keep_c)
    bias = row(3)
    mean, rstd2 = norm_stats(bias)
    for t in range(frames):
        part = pl.ds(t * s, s)
        xh = (cbuf[part, :] + bias - mean) * rstd2
        mi, dmi = mish_pair(xh * row(4) + row(5))
        xh2[part, :] = xh
        dm2[part, :] = dmi
        val = ((mi + res[part, :] + row(8)) * mask(t)).astype(bf16)
        if t % 2 == 0:
            be[pl.ds(t // 2 * s, s), :] = val
        else:
            bo[pl.ds((t // 2 + 1) * s, s), :] = val
    sh = 256 // half
    turn_h = grid_turn(sh, half)
    hm = half * s
    back_h = grid_turn(half, sh)
    dbase = W_DOWN
    obuf = res.at[pl.ds(0, hm)]
    taps_in = (bo, be, bo)
    taps_at = (0, 0, s)
    ag_x(2)
    own_cot.wait()
    swap_in_wait(cot_raw, 1)
    for b in range(s // sh):
        y = dot_nn(turn_h, cot_raw[pl.ds(b * 256, 256), :])
        lens_b = lens_ref[pl.ds(b * sh, sh), :]
        for j in range(half):
            keep = wide((lens_b > 2 * j).astype(f32), c)
            gdn[pl.ds(j * s + b * sh, sh), :] = (y[j * sh : (j + 1) * sh] * keep).astype(bf16)

    results = []

    def side(p):
        return sum(nt for _, nt, y_first in SUMS[:p] if y_first)

    def rs_core(p, v):
        t0, nt, y_first = SUMS[p]
        return remote(
            gw_all.at[pl.ds(t0, nt), :, at(v * 2 + 1 - co, width)],
            rcb.at[pl.ds(t0, nt), :, pl.ds(v * width, width)],
            rs_send.at[p, 0], rs_recv.at[p, 0], (dp, ch_c),
        )

    def rs_x(p, h):
        t0, nt, y_first = SUMS[p]
        src = sidebuf if y_first else rcb
        dst = ryb if y_first else rxb
        t1 = side(p) if y_first else t0
        return remote(
            src.at[pl.ds(t1, nt), at(h * 2 + 1 - lo, rows), :],
            dst.at[pl.ds(t0, nt), at(h, rows), :],
            rs_send.at[p, 1], rs_recv.at[p, 1], (dp_x, ch),
        )

    def rs_y(p):
        t0, nt, y_first = SUMS[p]
        src = rcb if y_first else rxb
        dst = sidebuf.at[pl.ds(side(p), nt)] if y_first else ryb.at[pl.ds(t0, nt)]
        return remote(src.at[pl.ds(t0, nt), :, at(1 - yy, width)], dst, rs_send.at[p, 2], rs_recv.at[p, 2], (dp, ch_y))

    def rs_z(p, i):
        t0, nt, y_first = SUMS[p]
        h = (hi + i) % n_hi
        return remote(
            ryb.at[pl.ds(t0, nt), at(h, rows), :], rzb.at[i, pl.ds(t0, nt)], rs_send.at[p, 3], rs_recv.at[p, 3], (h * 2 + lo, ch)
        )

    def rs_start(p):
        for v in range(2):
            rs_core(p, v).start()

    def plus(a, b):
        return (a.astype(f32) + b.astype(f32)).astype(bf16)

    def rs_x_start(p):
        @pl.loop(0, n_hi)
        def _(h):
            rs_x(p, h).start()

    def rs_z_start(p):
        @pl.loop(1, n_hi)
        def _(i):
            rs_z(p, i).start()

    def rs_after_core(p):
        both = rcb.at[pl.ds(SUMS[p][0], SUMS[p][1])]
        arrived(both, rs_recv.at[p, 0])
        gone(both, rs_send.at[p, 0])

        @pl.loop(SUMS[p][0], SUMS[p][0] + SUMS[p][1])
        def _(k):
            for v in range(2):
                cols = pl.ds(v * width, width)
                rcb[k, :, cols] = plus(rcb[k, :, cols], gw_all[k, :, at(v * 2 + co, width)])

        if SUMS[p][2]:
            rs_y(p).start()
        else:
            rs_x_start(p)

    def rs_after_x(p):
        t0 = SUMS[p][0]

        every = (ryb if SUMS[p][2] else rxb).at[pl.ds(t0, SUMS[p][1])]
        arrived(every, rs_recv.at[p, 1])
        gone(every, rs_send.at[p, 1])

        @pl.loop(SUMS[p][0], SUMS[p][0] + SUMS[p][1])
        def _(k):
            for h in range(n_hi):
                part = pl.ds(h * rows, rows)
                if SUMS[p][2]:
                    ryb[k, part, :] = plus(ryb[k, part, :], sidebuf[k - t0 + side(p), at(h * 2 + lo, rows), :])
                else:
                    rxb[k, part, :] = plus(rxb[k, part, :], rcb[k, at(h * 2 + lo, rows), :])

        if SUMS[p][2]:
            rs_z_start(p)
        else:
            rs_y(p).start()

    def rs_after_y(p):
        t0 = SUMS[p][0]

        rs_y(p).wait()

        @pl.loop(SUMS[p][0], SUMS[p][0] + SUMS[p][1])
        def _(k):
            if SUMS[p][2]:
                sidebuf[k - t0 + side(p)] = plus(sidebuf[k - t0 + side(p)], rcb[k, :, at(yy, width)])
            else:
                ryb[k] = plus(ryb[k], rxb[k, :, at(yy, width)])

        if SUMS[p][2]:
            rs_x_start(p)
        else:
            rs_z_start(p)

    def rs_after_z(p):
        t0, nt, y_first = SUMS[p]

        every = rzb.at[pl.ds(1, n_hi - 1), pl.ds(t0, nt)]
        arrived(every, rs_recv.at[p, 3])
        gone(every, rs_send.at[p, 3])

        @pl.loop(t0, t0 + nt)
        def _(k):
            def more(i, tot):
                return tot + rzb[i, k].astype(f32)

            gfin[k] = lax.fori_loop(1, n_hi, more, ryb[k, at(hi, rows), :].astype(f32))

        results.append(local(12 + p, gfin.at[pl.ds(t0, nt)], gfin_h.at[pl.ds(t0, nt)]))

    gs = [None] * SMALL

    def norm_back(xh, dm, gain, rstd, dst, scale):
        a1 = jnp.zeros((s, c), f32)
        a2 = jnp.zeros((s, c), f32)
        for t in range(frames):
            part = pl.ds(t * s, s)
            dy = cbuf[part, :] * mask(t) * dm[part, :]
            if scale is not None:
                dy = dy * scale
            dm[part, :] = dy
            a1 += dy
            a2 += dy * xh[part, :]
        g1 = group_sum(a1 * gain) / count
        g2 = group_sum(a2 * gain) / count
        tot = jnp.zeros((s, c), f32)
        for t in range(frames):
            part = pl.ds(t * s, s)
            dp_t = rstd * (dm[part, :] * gain - mask(t) * (g1 + xh[part, :] * g2))
            tot += dp_t
            dst[pl.ds((t + 2) * s, s), :] = dp_t.astype(bf16)
        return [jnp.sum(v, axis=0, keepdims=True) for v in (tot, a2, a1)]

    def film_back(i):
        q = (ch + i) % n_ch
        return remote(gfilm.at[:, :, at(q, width)], gfa.at[:, at(ch, s), :], gf_send.at[0], gf_recv.at[0], (dp, q))

    def small_c():
        return remote(gsm, gsr.at[0], gs_send.at[0], gs_recv.at[0], (dp, ch_c))

    def small_y():
        cols = at(ch_y, width)
        return remote(gsm.at[:, cols], gsr.at[1, :, cols], gs_send.at[1], gs_recv.at[1], (dp, ch_y))

    def small_x():
        return remote(gsm.at[:, my_cols], gsr.at[2, :, my_cols], gs_send.at[2], gs_recv.at[2], (dp_x, ch))

    def small_z(i):
        device = ((hi + i) % n_hi * 2 + lo, ch)
        return remote(gsm.at[:, my_cols], gsr.at[2 + i, :, my_cols], gs_send.at[3], gs_recv.at[3], device)

    def keep_ig(part, cols, acc):
        cbuf[part, cols] = acc + dot_nt(gres[part, :], w_all[W_RES, cols, :])

    def rf_z(i):
        h = (hi + i) % n_hi
        return remote(gwf.at[:, at(h, 2 * frp), :], rfz.at[i], rf_send.at[0], rf_recv.at[0], (h * 2 + lo, ch))

    def rf_x():
        return remote(rfs.at[:, at(1 - lo, frp), :], rfx, rf_send.at[1], rf_recv.at[1], (dp_x, ch))

    def gw_down():
        for k in range(DOWN):
            for n in range(c // NB):
                cols = pl.ds(n * NB, NB)
                gw_all[dbase + k, :, cols] = dot_tn(taps_in[k][pl.ds(taps_at[k], hm), :], gdn[pl.ds(0, hm), cols]).astype(bf16)

    def gw_res():
        for n in range(c // NB):
            cols = pl.ds(n * NB, NB)
            gw_all[W_RES, :, cols] = dot_tn(xpad[pl.ds(2 * s, m), :], gres[:, cols]).astype(bf16)

    def result_rows():
        for n in range(c // NB):
            cols = pl.ds(n * NB, NB)
            acc = dot_nn(bo[pl.ds(0, hm), :], w_all[dbase, :, cols])
            acc += dot_nn(be[...], w_all[dbase + 1, :, cols])
            acc += dot_nn(bo[pl.ds(s, hm), :], w_all[dbase + 2, :, cols])
            obuf[:, cols] = acc
        for b in range(s // sh):
            pieces = []
            lens_b = lens_ref[pl.ds(b * sh, sh), :]
            for j in range(half):
                keep = wide((lens_b > 2 * j).astype(f32), c)
                pieces.append(((obuf[pl.ds(j * s + b * sh, sh), :] + row(9)) * keep).astype(bf16))
            out_raw[pl.ds(b * 256, 256), :] = dot_nn(back_h, jnp.concatenate(pieces, axis=0)).astype(bf16)
        for i in range(1, n_ch):
            swap_out(out_raw, output, h2, 0, i).start()
        results.append(local(2, out_raw.at[:, my_cols], output.at[at(ch, h2)]))

    def into_block():
        for n in range(c // NB):
            cols = pl.ds(n * NB, NB)
            ge = dot_nt(gdn[pl.ds(0, hm), :], w_all[dbase + 1, cols, :])
            go = dot_nt(gdn[pl.ds(0, hm), :], w_all[dbase + 2, cols, :])
            go += dot_nt(gdn[pl.ds(s, hm), :], w_all[dbase, cols, :])
            for j in range(half):
                cbuf[pl.ds(2 * j * s, s), cols] = ge[j * s : (j + 1) * s]
                cbuf[pl.ds((2 * j + 1) * s, s), cols] = go[j * s : (j + 1) * s]

    def into_res():
        tot = jnp.zeros((s, c), f32)
        for j in range(half):
            tot += gdn[pl.ds(j * s, s), :].astype(f32)
        gs[9] = jnp.sum(tot, axis=0, keepdims=True)
        tot = jnp.zeros((s, c), f32)
        for t in range(frames):
            part = pl.ds(t * s, s)
            g = cbuf[part, :] * mask(t)
            tot += g
            gres[part, :] = g.astype(bf16)
        gs[8] = jnp.sum(tot, axis=0, keepdims=True)

    def norm_back_two():
        gs[3:6] = norm_back(xh2, dm2, row(4), rstd2, gc2, None)

    def norm_back_one():
        gs[0:3] = norm_back(xh1, dm1, row(1), rstd1, gc1, film[0])

    def film_rows():
        tot1 = jnp.zeros((s, c), f32)
        tot2 = jnp.zeros((s, c), f32)
        for t in range(frames):
            part = pl.ds(t * s, s)
            g = cbuf[part, :] * mask(t)
            tot1 += g * m1[part, :]
            tot2 += g
        gfilm[0] = tot1.astype(bf16)
        gfilm[1] = tot2.astype(bf16)
        gs[6] = jnp.sum(tot1, axis=0, keepdims=True)
        gs[7] = jnp.sum(tot2, axis=0, keepdims=True)

        for i in range(1, n_ch):
            film_back(i).start()
        gfa[:, at(ch, s), :] = gfilm[:, :, my_cols]

    def film_start():
        arrived(gfa.at[:, pl.ds(0, (n_ch - 1) * s), :], gf_recv.at[0])
        for i in range(2):
            gwf[i] = dot_tn(act[...], gfa[i]).astype(bf16)

        @pl.loop(1, n_hi)
        def _(i):
            rf_z(i).start()

    def film_hi():
        arrived(rfz.at[pl.ds(1, n_hi - 1)], rf_recv.at[0])
        gone(rfz.at[pl.ds(1, n_hi - 1)], rf_send.at[0])

        for v in range(2):
            def more(i, tot):
                return tot + rfz[i, v].astype(f32)

            rfs[v] = lax.fori_loop(1, n_hi, more, gwf[v, at(hi, 2 * frp), :].astype(f32)).astype(bf16)
        rf_x().start()

    def film_end():
        rf_x().wait()
        for v in range(2):
            gffin[v] = rfs[v, at(lo, frp), :].astype(f32) + rfx[v].astype(f32)
        results.append(local(12 + len(SUMS), gffin, gffin_h))

    def small_start():
        zero = jnp.zeros((1, c), f32)
        for i in range(SMALL):
            gsm[pl.ds(i, 1), :] = gs[i] if gs[i] is not None else zero

        small_c().start()

    def small_to_y():
        small_c().wait()
        gsm[...] += gsr[0]
        small_y().start()

    def small_to_x():
        small_y().wait()
        gsm[:, my_cols] += gsr[1, :, my_cols]
        small_x().start()

    def small_to_z():
        small_x().wait()
        gsm[:, my_cols] += gsr[2, :, my_cols]

        @pl.loop(1, n_hi)
        def _(i):
            small_z(i).start()

    def small_end():
        arrived(gsr.at[pl.ds(3, n_hi - 1), :, my_cols], gs_recv.at[3])
        gone(gsr.at[pl.ds(3, n_hi - 1), :, my_cols], gs_send.at[3])

        def more_small(i, tot):
            return tot + gsr[2 + i, :, my_cols]

        gsfin[...] = lax.fori_loop(1, n_hi, more_small, gsm[:, my_cols])
        results.append(local(13 + len(SUMS), gsfin, gsfin_h))

    def input_rows():
        back = grid_turn(frames, sb)
        for b in range(s // sb):
            lens_b = lens_ref[pl.ds(b * sb, sb), :]
            pieces = [
                (cbuf[pl.ds(t * s + b * sb, sb), :] * wide((lens_b > t).astype(f32), c)).astype(bf16) for t in range(frames)
            ]
            ig_raw[pl.ds(b * 256, 256), :] = dot_nn(back, jnp.concatenate(pieces, axis=0)).astype(bf16)
        for i in range(1, n_ch):
            swap_out(ig_raw, input_grad, m, 1, i).start()
        results.append(local(3, ig_raw.at[:, my_cols], input_grad.at[at(ch, m)]))

    def weight_grad(name):
        t0, nt, _ = SUMS[GROUPS.index(name)]
        src, g, first = (hpad, gc2, W_TWO) if name.startswith("TWO") else (xpad, gc1, W_ONE)
        conv_grad(src, g, first, t0 - first, t0 - first + nt)

    steps = dict(
        C2=lambda: ag_core(2), downf=result_rows, gW_DOWN=gw_down, gW_RES=gw_res, gblock=into_block, gres=into_res,
        nb2=norm_back_two, nb1=norm_back_one, filmg=film_rows, fdot=film_start, fz=film_hi, fe=film_end,
        small=small_start, smy=small_to_y, smx=small_to_x, smz=small_to_z, sme=small_end,
        cb2=lambda: conv_bwd(gc2, W_TWO, keep_c), cb1=lambda: conv_bwd(gc1, W_ONE, keep_ig), ig=input_rows,
    )
    sums = dict(s=rs_start, c=rs_after_core, x=rs_after_x, y=rs_after_y, z=rs_after_z)
    for name in BACKWARD:
        kind, _, group = name.partition("_")
        if name in steps:
            steps[name]()
        elif kind == "gW":
            weight_grad(group)
        else:
            sums[kind](GROUPS.index(group))
    for p in range(3):
        ag_done(p)
    bounds_x().wait_send()
    gone(stats.at[pl.ds(3, n_hi - 1)], st_send.at[1])

    gone(wf_all.at[:, pl.ds(0, 2 * (n_hi - 1) * frp), :], fw_send.at[1])

    film_x().wait_send()
    gone(small.at[:, pl.ds(0, others)], in_send.at[2])
    gone(film.at[:, :, pl.ds(0, others)], fo_send.at[0])
    gone(gfa.at[:, pl.ds(0, (n_ch - 1) * s), :], gf_send.at[0])

    for copy in results:
        copy.wait()
    swap_out_wait(out_raw, output, h2, 0)
    swap_out_wait(ig_raw, input_grad, m, 1)


def block_step(n_dp, n_ch, inputs, cot, cond, lens, one_w, two_w, res_w, down_w, film_w, small_w):
    rows, width = res_w.shape
    c = rows * n_dp
    samples = lens.shape[1]
    s = samples // n_ch
    m = inputs.shape[0] // n_ch
    h = m // 2
    frp = film_w.shape[0]
    feats = cond.shape[1]
    n_hi = n_dp // 2
    taps = N_TAPS
    V = pltpu.VMEM
    D = pltpu.SemaphoreType.DMA
    hbm = pl.BlockSpec(memory_space=pl.ANY)
    out = [
        jax.ShapeDtypeStruct((h * n_ch, width), bf16),
        jax.ShapeDtypeStruct((m * n_ch, width), bf16),
        jax.ShapeDtypeStruct((taps, rows, width), f32),
        jax.ShapeDtypeStruct((2, frp, width), f32),
        jax.ShapeDtypeStruct((SMALL, width), f32),
    ]
    pad = V((m + 4 * s, c), bf16)
    full = V((m, c), f32)
    scratch = [
        V((taps, c, c), bf16), V((taps, c, c), bf16), V((m, c), bf16), V((h, c), bf16), V((h, c), bf16), V((m, c), bf16),
        V((SMALL, c), f32), V((3 + n_hi, -(-feats // 512) * 8, 128), f32), V((samples, feats), bf16), V((2, n_dp * frp, width), bf16),
        V((2, samples, width), f32), V((2, s, c), f32), V((2, s, c), bf16), V((2, samples, width), bf16), V((2, n_dp * frp, width), bf16),
        *[V(o.shape, o.dtype) for o in out[2:]],
        V((taps, c, 2 * width), bf16), V((taps, n_hi * rows, 2 * width), bf16), V((taps, n_hi * rows, width), bf16), V((sum(nt for _, nt, y_first in SUMS if y_first), c, width), bf16),
        V((n_hi, taps, rows, width), bf16), V((2, frp, width), bf16), V((n_hi, 2, 2 * frp, width), bf16), V((2, 2 * frp, width), bf16),
        V((SMALL, c), f32), V((2 + n_hi, SMALL, c), f32),
        V((samples, feats), f32), V((1, samples), jnp.int32), V((samples, 128), f32), V((taps, rows, width), f32), V(film_w.shape, f32), V(small_w.shape, f32),
        pad, pad, V((h, c), bf16), V((h + s, c), bf16),
        full, full, full, full, full, full, full,
        V((h + s, c), bf16), pad, pad, V((m, c), bf16),
        D((3, 4)), D((3, 2 * n_hi + 3)), D((2,)), D((2,)), D((3,)), D((3,)), D((2,)), D((2,)), D((1,)), D((1,)),
        D((len(SUMS), 4)), D((len(SUMS), 4)), D((2,)), D((2,)), D((1,)), D((1,)), D((2,)), D((2,)), D((4,)), D((4,)),
        D((14 + len(SUMS),)),
    ]
    return pl.pallas_call(
        partial(step_kernel, n_dp, n_ch),
        out_shape=out,
        in_specs=[hbm] * 10,
        out_specs=[hbm] * 5,
        scratch_shapes=scratch,
        compiler_params=pltpu.CompilerParams(vmem_limit_bytes=63 << 20, collective_id=0, has_side_effects=True),
        name="block_step",
    )(inputs, cot, cond, lens, one_w, two_w, res_w, down_w, film_w, small_w)


beta_one = 0.9
beta_two = 0.999
adam_eps = 1e-08
weight_decay = 0.01
rate_large = 0.05
rate_small = 0.3
adam_step = 10


def adam_update(weight, gradient, old_first, old_second, learn_rate, decay_term):
    first_new = beta_one * old_first + (1.0 - beta_one) * gradient
    second_new = beta_two * old_second + (1.0 - beta_two) * gradient * gradient
    step_size = (
        first_new
        / (1.0 - beta_one**adam_step)
        / (jnp.sqrt(second_new / (1.0 - beta_two**adam_step)) + adam_eps)
    )
    return (first_new, second_new, weight - learn_rate * (step_size + decay_term * weight))


def update_kernel(n, a_in, b_in, *refs):
    ins, a_out, b_out, refs = refs[:n], refs[n], refs[n + 1], refs[n + 2 :]
    outs, bufs, results, refs = refs[: n - 3], refs[n - 3 : 2 * n - 3], refs[2 * n - 3 : 3 * n - 6], refs[3 * n - 6 :]
    a_buf, b_buf, sem_in, sem_out, sem_ab = refs
    order = (2, 4, 5, 3, 1, 0)
    loads = [pltpu.make_async_copy(ins[i], bufs[i], sem_in.at[i]) for i in range(n)]
    stores = [pltpu.make_async_copy(results[i], outs[i], sem_out.at[i]) for i in range(n - 3)]
    gw, gf, gs = bufs[:3]
    big = [pltpu.make_async_copy(src, dst, sem_ab.at[i]) for i, (src, dst) in enumerate(((a_in, a_buf), (b_in, b_buf), (a_buf, a_out), (b_buf, b_out)))]
    for copy in loads[:3]:
        copy.start()
    for i in order:
        for j in range(3):
            loads[3 + 3 * i + j].start()
    big[0].start()
    big[1].start()

    def put(i, index, grad, rate, decay):
        w, m, v = (bufs[3 + 3 * i + j][index] for j in range(3))
        for j, value in enumerate(adam_update(w, grad, m, v, rate, decay)):
            results[3 * i + j][index] = value

    for copy in loads[:3]:
        copy.wait()
    frows = ins[3 + 12].shape[0]
    for i in order:
        for j in range(3):
            loads[3 + 3 * i + j].wait()
        if i in (0, 1, 3):
            base, taps = ((W_ONE, TAPS), (W_TWO, TAPS), None, (W_DOWN, DOWN))[i]
            for k in range(taps):
                put(i, k, gw[base + k], rate_large, weight_decay)
        elif i == 2:
            put(i, ..., gw[W_RES], rate_large, weight_decay)
        elif i == 4:
            for k in range(2):
                put(i, (slice(None), k), gf[k, pl.ds(0, frows), :], rate_large, weight_decay)
        else:
            put(i, ..., gs[pl.ds(0, ins[3 + 15].shape[0]), :], rate_small, 0.0)
        for j in range(3):
            stores[3 * i + j].start()
    for i in range(2):
        big[i].wait()
        big[2 + i].start()
    for copy in stores:
        copy.wait()
    big[2].wait()
    big[3].wait()


def update(output, input_grad, gw, gf, gs, *state):
    hbm = pl.BlockSpec(memory_space=pl.ANY)
    acts = (output, input_grad)
    arrays = (gw, gf, gs, *state)
    n = len(arrays)
    bufs = [pltpu.VMEM(a.shape, f32) for a in arrays]
    return pl.pallas_call(
        partial(update_kernel, n),
        out_shape=[jax.ShapeDtypeStruct(a.shape, a.dtype) for a in (*acts, *state)],
        in_specs=[hbm] * (n + 2),
        out_specs=[hbm] * (len(state) + 2),
        scratch_shapes=[
            *bufs, *bufs[3:], *[pltpu.VMEM(a.shape, a.dtype) for a in acts],
            pltpu.SemaphoreType.DMA((n,)), pltpu.SemaphoreType.DMA((n,)), pltpu.SemaphoreType.DMA((4,)),
        ],
        compiler_params=pltpu.CompilerParams(vmem_limit_bytes=60 << 20),
        name="update",
    )(*acts, *arrays)


def body(
    inputs, condition, lengths, cotangent,
    conv1_w, conv1_m, conv1_v, conv2_w, conv2_m, conv2_v, res_w, res_m, res_v,
    down_w, down_m, down_v, film_w, film_m, film_v, small_w, small_m, small_v,
):
    n_dp, n_ch = lax.axis_size("dp"), lax.axis_size("chan")
    lens = lengths.reshape(1, -1)

    def taps_first(*arrays):
        return tuple(jnp.transpose(a, (1, 0, 2)) for a in arrays)

    one, two, down = (
        taps_first(*state) for state in ((conv1_w, conv1_m, conv1_v), (conv2_w, conv2_m, conv2_v), (down_w, down_m, down_v))
    )
    cond, film_rows = condition, film_w
    frows = film_w.shape[0]
    if frows % 16:
        short = -frows % 16
        film_rows = jnp.pad(film_w, ((0, short), (0, 0), (0, 0)))
        cond = jnp.pad(condition.reshape(-1, n_dp, frows), ((0, 0), (0, 0), (0, short))).reshape(condition.shape[0], -1)
    output, input_grad, gw, gf, gs = block_step(
        n_dp, n_ch, inputs, cotangent, cond, lens, one[0], two[0], res_w, down[0], film_rows, small_w
    )
    output, input_grad, *state = update(
        output, input_grad, gw, gf, gs, *one, *two, res_w, res_m, res_v, *down, film_w, film_m, film_v, small_w, small_m, small_v
    )
    state = (*taps_first(*state[:6]), *state[6:9], *taps_first(*state[9:12]), *state[12:])
    return (output, input_grad, *state)


def solution(mesh):
    in_specs = (
        P("dp", "chan"),
        P("dp", None),
        P("dp"),
        P("dp", "chan"),
        P("dp", None, "chan"),
        P("dp", None, "chan"),
        P("dp", None, "chan"),
        P("dp", None, "chan"),
        P("dp", None, "chan"),
        P("dp", None, "chan"),
        P("dp", "chan"),
        P("dp", "chan"),
        P("dp", "chan"),
        P("dp", None, "chan"),
        P("dp", None, "chan"),
        P("dp", None, "chan"),
        P("dp", None, "chan"),
        P("dp", None, "chan"),
        P("dp", None, "chan"),
        P(None, "chan"),
        P(None, "chan"),
        P(None, "chan"),
    )
    out_specs = (
        P("dp", "chan"),
        P("dp", "chan"),
        P("dp", None, "chan"),
        P("dp", None, "chan"),
        P("dp", None, "chan"),
        P("dp", None, "chan"),
        P("dp", None, "chan"),
        P("dp", None, "chan"),
        P("dp", "chan"),
        P("dp", "chan"),
        P("dp", "chan"),
        P("dp", None, "chan"),
        P("dp", None, "chan"),
        P("dp", None, "chan"),
        P("dp", None, "chan"),
        P("dp", None, "chan"),
        P("dp", None, "chan"),
        P(None, "chan"),
        P(None, "chan"),
        P(None, "chan"),
    )
    return jax.shard_map(body, mesh=mesh, in_specs=in_specs, out_specs=out_specs, check_vma=False)
```

```python
from functools import partial

import jax
import jax.numpy as jnp
from jax import lax
from jax.experimental import pallas as pl
from jax.experimental.pallas import tpu as pltpu
from jax.sharding import PartitionSpec as P

f32, bf16 = jnp.float32, jnp.bfloat16
GROUP = 64
TAPS = 5
DOWN = 3
eps_norm = 1e-05


def dot_nn(a, b):
    return lax.dot_general(a, b, (((1,), (0,)), ((), ())), preferred_element_type=f32)


def dot_nt(a, b):
    return lax.dot_general(a, b, (((1,), (1,)), ((), ())), preferred_element_type=f32)


def dot_tn(a, b):
    return lax.dot_general(a, b, (((0,), (0,)), ((), ())), preferred_element_type=f32)


def mish_pair(v):
    u = jnp.exp(-jnp.abs(v))
    pos = v >= 0
    num = jnp.where(pos, 1.0 + 2.0 * u, u * (u + 2.0))
    q = jnp.where(pos, 2.0 * u * u, 2.0)
    r = 1.0 / (num + q)
    w = num * r
    sig = jnp.where(pos, 1.0, u) / (1.0 + u)
    return v * w, w + v * sig * ((q * r) * ((2.0 * num + q) * r))


def wide(tile, lanes):
    return jnp.concatenate([tile] * (lanes // tile.shape[1]), axis=1)


def grid_turn(outer, inner):
    n = outer * inner
    row = lax.broadcasted_iota(jnp.int32, (n, n), 0)
    col = lax.broadcasted_iota(jnp.int32, (n, n), 1)
    return ((row % outer) * inner + row // outer == col).astype(bf16)


def group_sum(values):
    s, c = values.shape
    row = lax.broadcasted_iota(jnp.int32, (128, 128), 0)
    col = lax.broadcasted_iota(jnp.int32, (128, 128), 1)
    ones = (row // GROUP == col // GROUP).astype(f32)
    tall = jnp.concatenate([values[:, i : i + 128] for i in range(0, c, 128)], axis=0)
    tot = lax.dot_general(tall, ones, (((1,), (0,)), ((), ())), precision=lax.Precision.HIGHEST, preferred_element_type=f32)
    return jnp.concatenate([tot[i * s : (i + 1) * s] for i in range(c // 128)], axis=1)


MESH = pl.DeviceIdType.MESH
W_ONE, W_TWO, W_RES, W_DOWN = 0, TAPS, 2 * TAPS, 2 * TAPS + 1
N_TAPS = W_DOWN + DOWN
PARTS = ((W_ONE, TAPS), (W_TWO, TAPS + 1), (W_DOWN, DOWN))
GROUPS = ("DOWN", "RES", "TWO_A", "TWO_B", "TWO_C", "ONE_A", "ONE_B", "ONE_C")
SUMS = (
    (W_DOWN, 3, False),
    (W_RES, 1, True),
    (W_TWO, 1, True),
    (W_TWO + 1, 2, False),
    (W_TWO + 3, 2, False),
    (W_ONE, 1, True),
    (W_ONE + 1, 2, True),
    (W_ONE + 3, 2, False),
)
ORDER = (
    "far0", "own0", "own1", "far1", "fx0", "own2", "fz0_1", "bx", "fy1_0", "fz0_2", "bz", "fz0_3", "fy0_2",
    "inp", "fz1_2", "fy0_0", "filmon", "fy0_1", "far2", "fz1_3", "fz1_1", "fy0_3", "perm", "fy1_2", "fy1_3",
    "xa0", "xb0", "cond", "core0", "smallin", "fy1_1", "fy2_0", "xa1", "fdotf", "conv1", "fz2_2", "st1",
    "fz2_1", "fz2_3", "cot", "xb1", "app1", "core1", "fy2_2", "resd", "conv2", "fy2_1", "xa2", "st2", "fy2_3",
    "app2", "xb2", "gdnp", "gW_DOWN", "s_DOWN", "C2", "gblock", "downf", "c_DOWN", "gres", "nb2", "gW_RES",
    "s_RES", "gW_TWO_C", "s_TWO_C", "c_RES", "cb2", "filmg", "c_TWO_C", "nb1", "x_DOWN", "gW_ONE_A", "fdot",
    "s_ONE_A", "y_RES", "small", "gW_ONE_C", "s_ONE_C", "smy", "c_ONE_A", "gW_TWO_B", "x_TWO_C", "c_ONE_C",
    "gW_TWO_A", "s_TWO_A", "y_ONE_A", "s_TWO_B", "c_TWO_A", "gW_ONE_B", "s_ONE_B", "c_ONE_B", "y_TWO_C",
    "c_TWO_B", "cb1", "fz", "x_ONE_C", "y_TWO_A", "y_DOWN", "x_TWO_B", "x_RES", "x_ONE_A", "x_TWO_A", "smx",
    "y_ONE_C", "ig", "smz", "y_TWO_B", "y_ONE_B", "x_ONE_B", "z_TWO_C", "z_ONE_A", "z_ONE_C", "z_DOWN",
    "z_TWO_A", "z_TWO_B", "fe", "sme", "z_RES", "z_ONE_B",
)
SMALL = 16


def step_kernel(
    n_dp, n_ch,
    inputs, cot, cond_h, lens_h, one_w, two_w, res_w, down_w, film_h, small_h,
    output, input_grad, gfin_h, gffin_h, gsfin_h,
    w_all, gw_all, x_raw, cot_raw, out_raw, ig_raw, small, stats, act, wf_all, film_out, film, gfilm, gfa, gwf,
    gfin, gffin, gsfin, rcb, rxb, ryb, sidebuf, rzb, rfx, rfz, rfs, gsm, gsr, cond, lens_row, lens_all, wraw, film_w, small_w,
    xpad, hpad, be, bo, cbuf, res, xh1, m1, dm1, xh2, dm2, gdn, gc2, gc1, gres,
    ag_send, ag_recv, st_send, st_recv, in_send, in_recv, fw_send, fw_recv, fo_send, fo_recv,
    rs_send, rs_recv, out_send, out_recv, gf_send, gf_recv, rf_send, rf_recv, gs_send, gs_recv, loc,
):
    dp, ch = lax.axis_index("dp"), lax.axis_index("chan")
    hi, lo, yy, co = dp // 2, dp % 2, ch // 2, ch % 2
    n_hi = n_dp // 2
    dp_x = hi * 2 + 1 - lo
    ch_y = (1 - yy) * 2 + co
    ch_c = yy * 2 + 1 - co
    m, c = x_raw.shape
    h2 = m // 2
    rows, width = res_w.shape
    frp = film_h.shape[0]
    s = lens_h.shape[1] // n_ch
    frames = m // s
    half = frames // 2
    MC = 256 if m % 256 == 0 else m
    NB = 256

    def at(index, size):
        return pl.ds(pl.multiple_of(index * size, size), size)

    def remote(src, dst, ss, rs, device):
        return pltpu.make_async_remote_copy(
            src_ref=src, dst_ref=dst, send_sem=ss, recv_sem=rs, device_id=device, device_id_type=MESH
        )

    barrier = pltpu.get_barrier_semaphore()

    @pl.loop(1, n_dp)
    def _(i):
        pl.semaphore_signal(barrier, inc=1, device_id=((dp + i) % n_dp, ch), device_id_type=MESH)

    for i in range(1, n_ch):
        pl.semaphore_signal(barrier, inc=1, device_id=(dp, (ch + i) % n_ch), device_id_type=MESH)

    def local(i, src, dst):
        copy = pltpu.make_async_copy(src, dst, loc.at[i])
        copy.start()
        return copy

    own_x = local(0, inputs.at[at(ch, m)], x_raw.at[:, at(ch, width)])
    own_cot = local(1, cot.at[at(ch, h2)], cot_raw.at[:, at(ch, width)])
    staged = [
        local(4, cond_h, cond), local(5, lens_h, lens_row), local(6, small_h, small_w),
        local(7, one_w, wraw.at[pl.ds(W_ONE, TAPS)]), local(8, two_w, wraw.at[pl.ds(W_TWO, TAPS)]),
        local(9, down_w, wraw.at[pl.ds(W_DOWN, DOWN)]), local(10, res_w, wraw.at[W_RES]), local(11, film_h, film_w),
    ]
    pad0 = jnp.zeros((2 * s, c), bf16)
    for ref in (xpad, hpad, gc2, gc1):
        ref[pl.ds(0, 2 * s), :] = pad0
        ref[pl.ds((frames + 2) * s, 2 * s), :] = pad0
    bo[pl.ds(0, s), :] = pad0[:s]
    gdn[pl.ds(half * s, s), :] = pad0[:s]
    for copy in staged:
        copy.wait()
    my_rows, my_cols = at(dp, rows), at(ch, width)

    @pl.loop(0, N_TAPS)
    def _(k):
        w_all[k, my_rows, my_cols] = wraw[k].astype(bf16)

    for i in range(2):
        wf_all[i, at(dp, frp), :] = film_w[:, i, :].astype(bf16)
    n_all = lens_all.shape[0]
    on_line = lax.broadcasted_iota(jnp.int32, (n_all, n_all), 0) == lax.broadcasted_iota(jnp.int32, (n_all, n_all), 1)
    across = jnp.sum(jnp.where(on_line, lens_row[...].astype(f32), 0.0), axis=1, keepdims=True)
    lens_all[...] = jnp.broadcast_to(across, lens_all.shape)
    small[pl.ds(0, small_w.shape[0]), my_cols] = small_w[...]
    small[pl.ds(small_w.shape[0], SMALL - small_w.shape[0]), my_cols] = jnp.zeros((SMALL - small_w.shape[0], width), f32)
    values = cond[...]
    feats = values.shape[1] // 128
    ends = (jnp.max(values, axis=0, keepdims=True), jnp.max(-values, axis=0, keepdims=True))
    for e in range(2):
        for i in range(feats):
            stats[0, pl.ds(e * feats + i, 1), :] = ends[e][:, i * 128 : (i + 1) * 128]
    if stats.shape[1] > 2 * feats:
        stats[0, pl.ds(2 * feats, stats.shape[1] - 2 * feats), :] = jnp.zeros((stats.shape[1] - 2 * feats, 128), f32)
    pl.semaphore_wait(barrier, n_dp - 1 + n_ch - 1)

    def arrived(ref, sem):
        remote(ref, ref, sem, sem, (dp, ch)).wait_recv()

    def gone(ref, sem):
        remote(ref, ref, sem, sem, (dp, ch)).wait_send()

    others = (n_ch - 1) * width

    far, near = hi // 2, hi % 2
    if n_hi == 4:
        line = (far * 2 + 1 - near, (1 - far) * 2 + far, (1 - far) * 3)
    else:
        line = None

    def along(step):
        if line is not None:
            for h in line:
                step(h)
        else:

            @pl.loop(1, n_hi)
            def _(i):
                step((hi + i) % n_hi)

    def block(p, d, q):
        t0, nt = PARTS[p]
        return w_all.at[pl.ds(t0, nt), at(d, rows), at(q, width)]

    def pass_on(p, d, q, s_at, r_at, device):
        return remote(block(p, d, q), block(p, d, q), ag_send.at[p, s_at], ag_recv.at[p, r_at], device)

    def to_z(p, h):
        return pass_on(p, dp, ch, 0, hi, (h * 2 + lo, ch))

    def to_y(p, h):
        return pass_on(p, h * 2 + lo, ch, 1, n_hi + h, (dp, ch_y))

    def to_x(p, h, v):
        return pass_on(p, h * 2 + lo, v * 2 + co, 2, 2 * n_hi + v, (dp_x, ch))

    def to_c(p, h, l, v):
        return pass_on(p, h * 2 + l, v * 2 + co, 3, 2 * n_hi + 2, (dp, ch_c))

    def landed(p, n_rows, n_cols, at_sem):
        t0, nt = PARTS[p]
        arrived(w_all.at[pl.ds(t0, nt), pl.ds(0, n_rows), pl.ds(0, n_cols)], ag_recv.at[p, at_sem])

    def ag_far(p):
        along(lambda h: to_z(p, h).start())

    def ag_own(p):
        to_y(p, hi).start()
        to_x(p, hi, yy).start()
        to_c(p, hi, lo, yy).start()

    def from_z(p, h):
        landed(p, rows, width, h)
        to_y(p, h).start()
        to_x(p, h, yy).start()
        to_c(p, h, lo, yy).start()

    def from_y(p, h):
        landed(p, rows, width, n_hi + h)
        to_x(p, h, 1 - yy).start()
        to_c(p, h, lo, 1 - yy).start()

    passed = set()

    def from_one(step, kind, p, j):
        if line is not None:
            step(p, line[j - 1])
        elif (kind, p) not in passed:
            passed.add((kind, p))
            along(lambda h: step(p, h))

    def from_x(p, v):
        landed(p, n_hi * rows, width, 2 * n_hi + v)

        @pl.loop(0, n_hi)
        def _(h):
            to_c(p, h, 1 - lo, v).start()

    def ag_core(p):
        landed(p, c, 2 * width, 2 * n_hi + 2)

    def ag_done(p):
        t0, nt = PARTS[p]
        for i, (n_rows, n_cols) in enumerate((((n_hi - 1) * rows, width), (n_hi * rows, width), (c, width), (c, 2 * width))):
            gone(w_all.at[pl.ds(t0, nt), pl.ds(0, n_rows), pl.ds(0, n_cols)], ag_send.at[p, i])

    def swap_in(src, dst, n, k, i):
        q = (ch + i) % n_ch
        return remote(src.at[at(q, n)], dst.at[:, my_cols], in_send.at[k], in_recv.at[k], (dp, q))

    def swap_in_wait(dst, k):
        arrived(dst.at[:, pl.ds(0, others)], in_recv.at[k])
        gone(dst.at[:, pl.ds(0, others)], in_send.at[k])

    def swap_out(src, dst, n, k, i):
        q = (ch + i) % n_ch
        return remote(src.at[:, at(q, width)], dst.at[at(ch, n)], out_send.at[k], out_recv.at[k], (dp, q))

    def swap_out_wait(src, dst, n, k):
        arrived(dst.at[pl.ds(0, (n_ch - 1) * n)], out_recv.at[k])
        gone(src.at[:, pl.ds(0, others)], out_send.at[k])

    def small_swap(i):
        return remote(small.at[:, my_cols], small.at[:, my_cols], in_send.at[2], in_recv.at[2], (dp, (ch + i) % n_ch))

    def bounds_x():
        return remote(stats.at[0], stats.at[1], st_send.at[0], st_recv.at[0], (dp_x, ch))

    def bounds_z(h):
        return remote(stats.at[2], stats.at[3 + hi], st_send.at[1], st_recv.at[1], (h * 2 + lo, ch))

    def film_block(d):
        return wf_all.at[:, at(d, frp), :]

    def film_pass(d, at_sem, device):
        return remote(film_block(d), film_block(d), fw_send.at[at_sem], fw_recv.at[at_sem], device)

    def film_x():
        return film_pass(dp, 0, (dp_x, ch))

    def film_z(i, l):
        return film_pass(hi * 2 + l, 1, ((hi + i) % n_hi * 2 + lo, ch))

    def film_swap(i, q):
        return remote(
            film_out.at[:, at(q, s), :], film.at[:, :, my_cols], fo_send.at[0], fo_recv.at[0], (dp, q)
        )

    lens_ref = lens_all.at[at(ch, s)]

    def mask(t):
        return wide((lens_ref[...] > t).astype(f32), c)

    count = wide(lens_ref[...].astype(f32), c) * GROUP
    sb = 256 // frames
    turn = grid_turn(sb, frames)
    sh = 256 // half
    turn_h = grid_turn(sh, half)
    hm = half * s
    back_h = grid_turn(half, sh)
    dbase = W_DOWN
    obuf = res.at[pl.ds(0, hm)]
    taps_in = (bo, be, bo)
    taps_at = (0, 0, s)
    def conv_fwd(src, base, store):
        @pl.loop(0, c // NB)
        def _(n):
            cols = at(n, NB)
            for mi in range(m // MC):
                acc = dot_nn(src[pl.ds(mi * MC, MC), :], w_all[base, :, cols])
                for k in range(1, TAPS):
                    acc += dot_nn(src[pl.ds(mi * MC + k * s, MC), :], w_all[base + k, :, cols])
                store(pl.ds(mi * MC, MC), cols, acc)

    def conv_bwd(src, base, store):
        @pl.loop(0, c // NB)
        def _(n):
            cols = at(n, NB)
            for mi in range(m // MC):
                acc = dot_nt(src[pl.ds(mi * MC + (TAPS - 1) * s, MC), :], w_all[base, cols, :])
                for k in range(1, TAPS):
                    acc += dot_nt(src[pl.ds(mi * MC + (TAPS - 1 - k) * s, MC), :], w_all[base + k, cols, :])
                store(pl.ds(mi * MC, MC), cols, acc)

    def conv_grad(src, g, base, first, last):
        @pl.loop(first, last)
        def _(k):
            shifted = pl.ds(pl.multiple_of((TAPS - 1 - k) * s, s), m)
            for n in range(c // NB):
                cols = pl.ds(n * NB, NB)
                gw_all[base + k, :, cols] = dot_tn(src[pl.ds(2 * s, m), :], g[shifted, cols]).astype(bf16)

    def norm_stats(bias):
        tot = jnp.zeros((s, c), f32)
        for t in range(frames):
            tot += (cbuf[pl.ds(t * s, s), :] + bias) * mask(t)
        mean = group_sum(tot) / count
        tot = jnp.zeros((s, c), f32)
        for t in range(frames):
            d = (cbuf[pl.ds(t * s, s), :] + bias - mean) * mask(t)
            tot += d * d
        return mean, lax.rsqrt(group_sum(tot) / count + eps_norm)

    def row(i):
        return small[pl.ds(i, 1), :]

    def keep_c(part, cols, acc):
        cbuf[part, cols] = acc

    stats_of = {}

    def film_on():
        film_pass(dp_x, 0, (dp, ch)).wait_recv()

        @pl.loop(1, n_hi)
        def _(i):
            for l in range(2):
                film_z(i, l).start()

    def bounds_on():
        bounds_x().wait_recv()
        stats[2] = jnp.maximum(stats[0], stats[1])
        stats[3 + hi] = stats[2]
        along(lambda h: bounds_z(h).start())

    def small_on():
        for i in range(1, n_ch):
            small_swap(i).start()

    def inputs_on():
        for i in range(1, n_ch):
            swap_in(inputs, x_raw, m, 0, i).start()

    def cot_on():
        for i in range(1, n_ch):
            swap_in(cot, cot_raw, h2, 1, i).start()

    def condition_rows():
        arrived(stats.at[pl.ds(3, n_hi - 1)], st_recv.at[1])
        best = stats[3]
        for h in range(1, n_hi):
            best = jnp.maximum(best, stats[3 + h])
        low = -jnp.concatenate([best[feats + i : feats + i + 1, :] for i in range(feats)], axis=1)
        span = jnp.concatenate([best[i : i + 1, :] for i in range(feats)], axis=1) - low
        slope = 2.0 / jnp.maximum(span, 1.0)
        CB = 64

        @pl.loop(0, cond.shape[0] // CB)
        def _(i):
            v = (cond[at(i, CB), :] - low) * slope - 1.0
            act[at(i, CB), :] = mish_pair(v)[0].astype(bf16)

    def film_project():
        arrived(wf_all.at[:, pl.ds(0, 2 * (n_hi - 1) * frp), :], fw_recv.at[1])

        for i in range(2):
            film_out[i] = dot_nn(act[...], wf_all[i]) + small[pl.ds(6 + i, 1), my_cols]
        for i in range(1, n_ch):
            film_swap(i, (ch + i) % n_ch).start()
        for i in range(2):
            film[i, :, my_cols] = film_out[i, at(ch, s), :]

    def input_frames():
        own_x.wait()
        swap_in_wait(x_raw, 0)
        for b in range(s // sb):
            y = dot_nn(turn, x_raw[pl.ds(b * 256, 256), :])
            lens_b = lens_ref[pl.ds(b * sb, sb), :]
            for t in range(frames):
                keep = wide((lens_b > t).astype(f32), c)
                xpad[pl.ds((t + 2) * s + b * sb, sb), :] = (y[t * sb : (t + 1) * sb] * keep).astype(bf16)

    def residual():
        for n in range(c // NB):
            cols = pl.ds(n * NB, NB)
            for mi in range(m // MC):
                res[pl.ds(mi * MC, MC), cols] = dot_nn(xpad[pl.ds(2 * s + mi * MC, MC), :], w_all[W_RES, :, cols])

    def stats_one():
        arrived(small.at[:, pl.ds(0, others)], in_recv.at[2])
        stats_of[1] = norm_stats(row(0))

    def stats_two():
        stats_of[2] = norm_stats(row(3))

    def section_one():
        arrived(film.at[:, :, pl.ds(0, others)], fo_recv.at[0])
        mean, rstd1 = stats_of[1]
        bias = row(0)
        for t in range(frames):
            part = pl.ds(t * s, s)
            xh = (cbuf[part, :] + bias - mean) * rstd1
            mi, dmi = mish_pair(xh * row(1) + row(2))
            xh1[part, :] = xh
            m1[part, :] = mi
            dm1[part, :] = dmi
            hpad[pl.ds((t + 2) * s, s), :] = ((film[0] * mi + film[1]) * mask(t)).astype(bf16)

    def section_two():
        mean, rstd2 = stats_of[2]
        bias = row(3)
        for t in range(frames):
            part = pl.ds(t * s, s)
            xh = (cbuf[part, :] + bias - mean) * rstd2
            mi, dmi = mish_pair(xh * row(4) + row(5))
            xh2[part, :] = xh
            dm2[part, :] = dmi
            val = ((mi + res[part, :] + row(8)) * mask(t)).astype(bf16)
            if t % 2 == 0:
                be[pl.ds(t // 2 * s, s), :] = val
            else:
                bo[pl.ds((t // 2 + 1) * s, s), :] = val

    def cot_frames():
        own_cot.wait()
        swap_in_wait(cot_raw, 1)
        for b in range(s // sh):
            y = dot_nn(turn_h, cot_raw[pl.ds(b * 256, 256), :])
            lens_b = lens_ref[pl.ds(b * sh, sh), :]
            for j in range(half):
                keep = wide((lens_b > 2 * j).astype(f32), c)
                gdn[pl.ds(j * s + b * sh, sh), :] = (y[j * sh : (j + 1) * sh] * keep).astype(bf16)

    results = []

    def side(p):
        return sum(nt for _, nt, y_first in SUMS[:p] if y_first)

    def rs_core(p, v):
        t0, nt, y_first = SUMS[p]
        return remote(
            gw_all.at[pl.ds(t0, nt), :, at(v * 2 + 1 - co, width)],
            rcb.at[pl.ds(t0, nt), :, pl.ds(v * width, width)],
            rs_send.at[p, 0], rs_recv.at[p, 0], (dp, ch_c),
        )

    def rs_x(p, h):
        t0, nt, y_first = SUMS[p]
        src = sidebuf if y_first else rcb
        dst = ryb if y_first else rxb
        t1 = side(p) if y_first else t0
        return remote(
            src.at[pl.ds(t1, nt), at(h * 2 + 1 - lo, rows), :],
            dst.at[pl.ds(t0, nt), at(h, rows), :],
            rs_send.at[p, 1], rs_recv.at[p, 1], (dp_x, ch),
        )

    def rs_y(p):
        t0, nt, y_first = SUMS[p]
        src = rcb if y_first else rxb
        dst = sidebuf.at[pl.ds(side(p), nt)] if y_first else ryb.at[pl.ds(t0, nt)]
        return remote(src.at[pl.ds(t0, nt), :, at(1 - yy, width)], dst, rs_send.at[p, 2], rs_recv.at[p, 2], (dp, ch_y))

    def rs_z(p, i):
        t0, nt, y_first = SUMS[p]
        h = (hi + i) % n_hi
        return remote(
            ryb.at[pl.ds(t0, nt), at(h, rows), :], rzb.at[i, pl.ds(t0, nt)], rs_send.at[p, 3], rs_recv.at[p, 3], (h * 2 + lo, ch)
        )

    def rs_start(p):
        for v in range(2):
            rs_core(p, v).start()

    def plus(a, b):
        return (a.astype(f32) + b.astype(f32)).astype(bf16)

    def rs_x_start(p):
        @pl.loop(0, n_hi)
        def _(h):
            rs_x(p, h).start()

    def rs_z_start(p):
        @pl.loop(1, n_hi)
        def _(i):
            rs_z(p, i).start()

    def rs_after_core(p):
        both = rcb.at[pl.ds(SUMS[p][0], SUMS[p][1])]
        arrived(both, rs_recv.at[p, 0])
        gone(both, rs_send.at[p, 0])

        @pl.loop(SUMS[p][0], SUMS[p][0] + SUMS[p][1])
        def _(k):
            for v in range(2):
                cols = pl.ds(v * width, width)
                rcb[k, :, cols] = plus(rcb[k, :, cols], gw_all[k, :, at(v * 2 + co, width)])

        if SUMS[p][2]:
            rs_y(p).start()
        else:
            rs_x_start(p)

    def rs_after_x(p):
        t0 = SUMS[p][0]

        every = (ryb if SUMS[p][2] else rxb).at[pl.ds(t0, SUMS[p][1])]
        arrived(every, rs_recv.at[p, 1])
        gone(every, rs_send.at[p, 1])

        @pl.loop(SUMS[p][0], SUMS[p][0] + SUMS[p][1])
        def _(k):
            for h in range(n_hi):
                part = pl.ds(h * rows, rows)
                if SUMS[p][2]:
                    ryb[k, part, :] = plus(ryb[k, part, :], sidebuf[k - t0 + side(p), at(h * 2 + lo, rows), :])
                else:
                    rxb[k, part, :] = plus(rxb[k, part, :], rcb[k, at(h * 2 + lo, rows), :])

        if SUMS[p][2]:
            rs_z_start(p)
        else:
            rs_y(p).start()

    def rs_after_y(p):
        t0 = SUMS[p][0]

        rs_y(p).wait()

        @pl.loop(SUMS[p][0], SUMS[p][0] + SUMS[p][1])
        def _(k):
            if SUMS[p][2]:
                sidebuf[k - t0 + side(p)] = plus(sidebuf[k - t0 + side(p)], rcb[k, :, at(yy, width)])
            else:
                ryb[k] = plus(ryb[k], rxb[k, :, at(yy, width)])

        if SUMS[p][2]:
            rs_x_start(p)
        else:
            rs_z_start(p)

    def rs_after_z(p):
        t0, nt, y_first = SUMS[p]

        every = rzb.at[pl.ds(1, n_hi - 1), pl.ds(t0, nt)]
        arrived(every, rs_recv.at[p, 3])
        gone(every, rs_send.at[p, 3])

        @pl.loop(t0, t0 + nt)
        def _(k):
            def more(i, tot):
                return tot + rzb[i, k].astype(f32)

            gfin[k] = lax.fori_loop(1, n_hi, more, ryb[k, at(hi, rows), :].astype(f32))

        results.append(local(12 + p, gfin.at[pl.ds(t0, nt)], gfin_h.at[pl.ds(t0, nt)]))

    gs = [None] * SMALL

    def norm_back(xh, dm, gain, rstd, dst, scale):
        a1 = jnp.zeros((s, c), f32)
        a2 = jnp.zeros((s, c), f32)
        for t in range(frames):
            part = pl.ds(t * s, s)
            dy = cbuf[part, :] * mask(t) * dm[part, :]
            if scale is not None:
                dy = dy * scale
            dm[part, :] = dy
            a1 += dy
            a2 += dy * xh[part, :]
        g1 = group_sum(a1 * gain) / count
        g2 = group_sum(a2 * gain) / count
        tot = jnp.zeros((s, c), f32)
        for t in range(frames):
            part = pl.ds(t * s, s)
            dp_t = rstd * (dm[part, :] * gain - mask(t) * (g1 + xh[part, :] * g2))
            tot += dp_t
            dst[pl.ds((t + 2) * s, s), :] = dp_t.astype(bf16)
        return [jnp.sum(v, axis=0, keepdims=True) for v in (tot, a2, a1)]

    def film_back(i):
        q = (ch + i) % n_ch
        return remote(gfilm.at[:, :, at(q, width)], gfa.at[:, at(ch, s), :], gf_send.at[0], gf_recv.at[0], (dp, q))

    def small_c():
        return remote(gsm, gsr.at[0], gs_send.at[0], gs_recv.at[0], (dp, ch_c))

    def small_y():
        cols = at(ch_y, width)
        return remote(gsm.at[:, cols], gsr.at[1, :, cols], gs_send.at[1], gs_recv.at[1], (dp, ch_y))

    def small_x():
        return remote(gsm.at[:, my_cols], gsr.at[2, :, my_cols], gs_send.at[2], gs_recv.at[2], (dp_x, ch))

    def small_z(i):
        device = ((hi + i) % n_hi * 2 + lo, ch)
        return remote(gsm.at[:, my_cols], gsr.at[2 + i, :, my_cols], gs_send.at[3], gs_recv.at[3], device)

    def keep_ig(part, cols, acc):
        cbuf[part, cols] = acc + dot_nt(gres[part, :], w_all[W_RES, cols, :])

    def rf_z(i):
        h = (hi + i) % n_hi
        return remote(gwf.at[:, at(h, 2 * frp), :], rfz.at[i], rf_send.at[0], rf_recv.at[0], (h * 2 + lo, ch))

    def rf_x():
        return remote(rfs.at[:, at(1 - lo, frp), :], rfx, rf_send.at[1], rf_recv.at[1], (dp_x, ch))

    def gw_down():
        for k in range(DOWN):
            for n in range(c // NB):
                cols = pl.ds(n * NB, NB)
                gw_all[dbase + k, :, cols] = dot_tn(taps_in[k][pl.ds(taps_at[k], hm), :], gdn[pl.ds(0, hm), cols]).astype(bf16)

    def gw_res():
        for n in range(c // NB):
            cols = pl.ds(n * NB, NB)
            gw_all[W_RES, :, cols] = dot_tn(xpad[pl.ds(2 * s, m), :], gres[:, cols]).astype(bf16)

    def result_rows():
        for n in range(c // NB):
            cols = pl.ds(n * NB, NB)
            acc = dot_nn(bo[pl.ds(0, hm), :], w_all[dbase, :, cols])
            acc += dot_nn(be[...], w_all[dbase + 1, :, cols])
            acc += dot_nn(bo[pl.ds(s, hm), :], w_all[dbase + 2, :, cols])
            obuf[:, cols] = acc
        for b in range(s // sh):
            pieces = []
            lens_b = lens_ref[pl.ds(b * sh, sh), :]
            for j in range(half):
                keep = wide((lens_b > 2 * j).astype(f32), c)
                pieces.append(((obuf[pl.ds(j * s + b * sh, sh), :] + row(9)) * keep).astype(bf16))
            out_raw[pl.ds(b * 256, 256), :] = dot_nn(back_h, jnp.concatenate(pieces, axis=0)).astype(bf16)
        for i in range(1, n_ch):
            swap_out(out_raw, output, h2, 0, i).start()
        results.append(local(2, out_raw.at[:, my_cols], output.at[at(ch, h2)]))

    def into_block():
        for n in range(c // NB):
            cols = pl.ds(n * NB, NB)
            ge = dot_nt(gdn[pl.ds(0, hm), :], w_all[dbase + 1, cols, :])
            go = dot_nt(gdn[pl.ds(0, hm), :], w_all[dbase + 2, cols, :])
            go += dot_nt(gdn[pl.ds(s, hm), :], w_all[dbase, cols, :])
            for j in range(half):
                cbuf[pl.ds(2 * j * s, s), cols] = ge[j * s : (j + 1) * s]
                cbuf[pl.ds((2 * j + 1) * s, s), cols] = go[j * s : (j + 1) * s]

    def into_res():
        tot = jnp.zeros((s, c), f32)
        for j in range(half):
            tot += gdn[pl.ds(j * s, s), :].astype(f32)
        gs[9] = jnp.sum(tot, axis=0, keepdims=True)
        tot = jnp.zeros((s, c), f32)
        for t in range(frames):
            part = pl.ds(t * s, s)
            g = cbuf[part, :] * mask(t)
            tot += g
            gres[part, :] = g.astype(bf16)
        gs[8] = jnp.sum(tot, axis=0, keepdims=True)

    def norm_back_two():
        gs[3:6] = norm_back(xh2, dm2, row(4), stats_of[2][1], gc2, None)

    def norm_back_one():
        gs[0:3] = norm_back(xh1, dm1, row(1), stats_of[1][1], gc1, film[0])

    def film_rows():
        tot1 = jnp.zeros((s, c), f32)
        tot2 = jnp.zeros((s, c), f32)
        for t in range(frames):
            part = pl.ds(t * s, s)
            g = cbuf[part, :] * mask(t)
            tot1 += g * m1[part, :]
            tot2 += g
        gfilm[0] = tot1.astype(bf16)
        gfilm[1] = tot2.astype(bf16)
        gs[6] = jnp.sum(tot1, axis=0, keepdims=True)
        gs[7] = jnp.sum(tot2, axis=0, keepdims=True)

        for i in range(1, n_ch):
            film_back(i).start()
        gfa[:, at(ch, s), :] = gfilm[:, :, my_cols]

    def film_start():
        arrived(gfa.at[:, pl.ds(0, (n_ch - 1) * s), :], gf_recv.at[0])
        for i in range(2):
            gwf[i] = dot_tn(act[...], gfa[i]).astype(bf16)

        @pl.loop(1, n_hi)
        def _(i):
            rf_z(i).start()

    def film_hi():
        arrived(rfz.at[pl.ds(1, n_hi - 1)], rf_recv.at[0])
        gone(rfz.at[pl.ds(1, n_hi - 1)], rf_send.at[0])

        for v in range(2):
            def more(i, tot):
                return tot + rfz[i, v].astype(f32)

            rfs[v] = lax.fori_loop(1, n_hi, more, gwf[v, at(hi, 2 * frp), :].astype(f32)).astype(bf16)
        rf_x().start()

    def film_end():
        rf_x().wait()
        for v in range(2):
            gffin[v] = rfs[v, at(lo, frp), :].astype(f32) + rfx[v].astype(f32)
        results.append(local(12 + len(SUMS), gffin, gffin_h))

    def small_start():
        zero = jnp.zeros((1, c), f32)
        for i in range(SMALL):
            gsm[pl.ds(i, 1), :] = gs[i] if gs[i] is not None else zero

        small_c().start()

    def small_to_y():
        small_c().wait()
        gsm[...] += gsr[0]
        small_y().start()

    def small_to_x():
        small_y().wait()
        gsm[:, my_cols] += gsr[1, :, my_cols]
        small_x().start()

    def small_to_z():
        small_x().wait()
        gsm[:, my_cols] += gsr[2, :, my_cols]

        @pl.loop(1, n_hi)
        def _(i):
            small_z(i).start()

    def small_end():
        arrived(gsr.at[pl.ds(3, n_hi - 1), :, my_cols], gs_recv.at[3])
        gone(gsr.at[pl.ds(3, n_hi - 1), :, my_cols], gs_send.at[3])

        def more_small(i, tot):
            return tot + gsr[2 + i, :, my_cols]

        gsfin[...] = lax.fori_loop(1, n_hi, more_small, gsm[:, my_cols])
        results.append(local(13 + len(SUMS), gsfin, gsfin_h))

    def input_rows():
        back = grid_turn(frames, sb)
        for b in range(s // sb):
            lens_b = lens_ref[pl.ds(b * sb, sb), :]
            pieces = [
                (cbuf[pl.ds(t * s + b * sb, sb), :] * wide((lens_b > t).astype(f32), c)).astype(bf16) for t in range(frames)
            ]
            ig_raw[pl.ds(b * 256, 256), :] = dot_nn(back, jnp.concatenate(pieces, axis=0)).astype(bf16)
        for i in range(1, n_ch):
            swap_out(ig_raw, input_grad, m, 1, i).start()
        results.append(local(3, ig_raw.at[:, my_cols], input_grad.at[at(ch, m)]))

    def weight_grad(name):
        t0, nt, _ = SUMS[GROUPS.index(name)]
        src, g, first = (hpad, gc2, W_TWO) if name.startswith("TWO") else (xpad, gc1, W_ONE)
        conv_grad(src, g, first, t0 - first, t0 - first + nt)

    steps = dict(
        bx=lambda: bounds_x().start(), fx0=lambda: film_x().start(), smallin=small_on, bz=bounds_on, filmon=film_on,
        inp=inputs_on, cot=cot_on, cond=condition_rows, fdotf=film_project, perm=input_frames, resd=residual,
        conv1=lambda: conv_fwd(xpad, W_ONE, keep_c), conv2=lambda: conv_fwd(hpad, W_TWO, keep_c),
        st1=stats_one, st2=stats_two, app1=section_one, app2=section_two, gdnp=cot_frames,
        C2=lambda: ag_core(2), downf=result_rows, gW_DOWN=gw_down, gW_RES=gw_res, gblock=into_block, gres=into_res,
        nb2=norm_back_two, nb1=norm_back_one, filmg=film_rows, fdot=film_start, fz=film_hi, fe=film_end,
        small=small_start, smy=small_to_y, smx=small_to_x, smz=small_to_z, sme=small_end,
        cb2=lambda: conv_bwd(gc2, W_TWO, keep_c), cb1=lambda: conv_bwd(gc1, W_ONE, keep_ig), ig=input_rows,
    )
    for p in range(3):
        steps.update({f"far{p}": partial(ag_far, p), f"own{p}": partial(ag_own, p), f"core{p}": partial(ag_core, p)})
        steps.update({f"xa{p}": partial(from_x, p, yy), f"xb{p}": partial(from_x, p, 1 - yy), f"fy{p}_0": partial(from_y, p, hi)})
        for j in range(1, 4):
            steps[f"fz{p}_{j}"] = partial(from_one, from_z, "z", p, j)
            steps[f"fy{p}_{j}"] = partial(from_one, from_y, "y", p, j)
    sums = dict(s=rs_start, c=rs_after_core, x=rs_after_x, y=rs_after_y, z=rs_after_z)
    for name in ORDER:
        kind, _, group = name.partition("_")
        if name in steps:
            steps[name]()
        elif kind == "gW":
            weight_grad(group)
        else:
            sums[kind](GROUPS.index(group))
    for p in range(3):
        ag_done(p)
    bounds_x().wait_send()
    gone(stats.at[pl.ds(3, n_hi - 1)], st_send.at[1])

    gone(wf_all.at[:, pl.ds(0, 2 * (n_hi - 1) * frp), :], fw_send.at[1])

    film_x().wait_send()
    gone(small.at[:, pl.ds(0, others)], in_send.at[2])
    gone(film.at[:, :, pl.ds(0, others)], fo_send.at[0])
    gone(gfa.at[:, pl.ds(0, (n_ch - 1) * s), :], gf_send.at[0])

    for copy in results:
        copy.wait()
    swap_out_wait(out_raw, output, h2, 0)
    swap_out_wait(ig_raw, input_grad, m, 1)


def block_step(n_dp, n_ch, inputs, cot, cond, lens, one_w, two_w, res_w, down_w, film_w, small_w):
    rows, width = res_w.shape
    c = rows * n_dp
    samples = lens.shape[1]
    s = samples // n_ch
    m = inputs.shape[0] // n_ch
    h = m // 2
    frp = film_w.shape[0]
    feats = cond.shape[1]
    n_hi = n_dp // 2
    taps = N_TAPS
    V = pltpu.VMEM
    D = pltpu.SemaphoreType.DMA
    hbm = pl.BlockSpec(memory_space=pl.ANY)
    out = [
        jax.ShapeDtypeStruct((h * n_ch, width), bf16),
        jax.ShapeDtypeStruct((m * n_ch, width), bf16),
        jax.ShapeDtypeStruct((taps, rows, width), f32),
        jax.ShapeDtypeStruct((2, frp, width), f32),
        jax.ShapeDtypeStruct((SMALL, width), f32),
    ]
    pad = V((m + 4 * s, c), bf16)
    full = V((m, c), f32)
    scratch = [
        V((taps, c, c), bf16), V((taps, c, c), bf16), V((m, c), bf16), V((h, c), bf16), V((h, c), bf16), V((m, c), bf16),
        V((SMALL, c), f32), V((3 + n_hi, -(-feats // 512) * 8, 128), f32), V((samples, feats), bf16), V((2, n_dp * frp, width), bf16),
        V((2, samples, width), f32), V((2, s, c), f32), V((2, s, c), bf16), V((2, samples, width), bf16), V((2, n_dp * frp, width), bf16),
        *[V(o.shape, o.dtype) for o in out[2:]],
        V((taps, c, 2 * width), bf16), V((taps, n_hi * rows, 2 * width), bf16), V((taps, n_hi * rows, width), bf16), V((sum(nt for _, nt, y_first in SUMS if y_first), c, width), bf16),
        V((n_hi, taps, rows, width), bf16), V((2, frp, width), bf16), V((n_hi, 2, 2 * frp, width), bf16), V((2, 2 * frp, width), bf16),
        V((SMALL, c), f32), V((2 + n_hi, SMALL, c), f32),
        V((samples, feats), f32), V((1, samples), jnp.int32), V((samples, 128), f32), V((taps, rows, width), f32), V(film_w.shape, f32), V(small_w.shape, f32),
        pad, pad, V((h, c), bf16), V((h + s, c), bf16),
        full, full, full, full, full, full, full,
        V((h + s, c), bf16), pad, pad, V((m, c), bf16),
        D((3, 4)), D((3, 2 * n_hi + 3)), D((2,)), D((2,)), D((3,)), D((3,)), D((2,)), D((2,)), D((1,)), D((1,)),
        D((len(SUMS), 4)), D((len(SUMS), 4)), D((2,)), D((2,)), D((1,)), D((1,)), D((2,)), D((2,)), D((4,)), D((4,)),
        D((14 + len(SUMS),)),
    ]
    return pl.pallas_call(
        partial(step_kernel, n_dp, n_ch),
        out_shape=out,
        in_specs=[hbm] * 10,
        out_specs=[hbm] * 5,
        scratch_shapes=scratch,
        compiler_params=pltpu.CompilerParams(vmem_limit_bytes=63 << 20, collective_id=0, has_side_effects=True),
        name="block_step",
    )(inputs, cot, cond, lens, one_w, two_w, res_w, down_w, film_w, small_w)


beta_one = 0.9
beta_two = 0.999
adam_eps = 1e-08
weight_decay = 0.01
rate_large = 0.05
rate_small = 0.3
adam_step = 10


def adam_update(weight, gradient, old_first, old_second, learn_rate, decay_term):
    first_new = beta_one * old_first + (1.0 - beta_one) * gradient
    second_new = beta_two * old_second + (1.0 - beta_two) * gradient * gradient
    step_size = (
        first_new
        / (1.0 - beta_one**adam_step)
        / (jnp.sqrt(second_new / (1.0 - beta_two**adam_step)) + adam_eps)
    )
    return (first_new, second_new, weight - learn_rate * (step_size + decay_term * weight))


def update_kernel(n, a_in, b_in, *refs):
    ins, a_out, b_out, refs = refs[:n], refs[n], refs[n + 1], refs[n + 2 :]
    outs, bufs, results, refs = refs[: n - 3], refs[n - 3 : 2 * n - 3], refs[2 * n - 3 : 3 * n - 6], refs[3 * n - 6 :]
    a_buf, b_buf, sem_in, sem_out, sem_ab = refs
    order = (2, 4, 5, 3, 1, 0)
    loads = [pltpu.make_async_copy(ins[i], bufs[i], sem_in.at[i]) for i in range(n)]
    stores = [pltpu.make_async_copy(results[i], outs[i], sem_out.at[i]) for i in range(n - 3)]
    gw, gf, gs = bufs[:3]
    big = [pltpu.make_async_copy(src, dst, sem_ab.at[i]) for i, (src, dst) in enumerate(((a_in, a_buf), (b_in, b_buf), (a_buf, a_out), (b_buf, b_out)))]
    for copy in loads[:3]:
        copy.start()
    for i in order:
        for j in range(3):
            loads[3 + 3 * i + j].start()
    big[0].start()
    big[1].start()

    def put(i, index, grad, rate, decay):
        w, m, v = (bufs[3 + 3 * i + j][index] for j in range(3))
        for j, value in enumerate(adam_update(w, grad, m, v, rate, decay)):
            results[3 * i + j][index] = value

    for copy in loads[:3]:
        copy.wait()
    frows = ins[3 + 12].shape[0]
    for i in order:
        for j in range(3):
            loads[3 + 3 * i + j].wait()
        if i in (0, 1, 3):
            base, taps = ((W_ONE, TAPS), (W_TWO, TAPS), None, (W_DOWN, DOWN))[i]
            for k in range(taps):
                put(i, k, gw[base + k], rate_large, weight_decay)
        elif i == 2:
            put(i, ..., gw[W_RES], rate_large, weight_decay)
        elif i == 4:
            for k in range(2):
                put(i, (slice(None), k), gf[k, pl.ds(0, frows), :], rate_large, weight_decay)
        else:
            put(i, ..., gs[pl.ds(0, ins[3 + 15].shape[0]), :], rate_small, 0.0)
        for j in range(3):
            stores[3 * i + j].start()
    for i in range(2):
        big[i].wait()
        big[2 + i].start()
    for copy in stores:
        copy.wait()
    big[2].wait()
    big[3].wait()


def update(output, input_grad, gw, gf, gs, *state):
    hbm = pl.BlockSpec(memory_space=pl.ANY)
    acts = (output, input_grad)
    arrays = (gw, gf, gs, *state)
    n = len(arrays)
    bufs = [pltpu.VMEM(a.shape, f32) for a in arrays]
    return pl.pallas_call(
        partial(update_kernel, n),
        out_shape=[jax.ShapeDtypeStruct(a.shape, a.dtype) for a in (*acts, *state)],
        in_specs=[hbm] * (n + 2),
        out_specs=[hbm] * (len(state) + 2),
        scratch_shapes=[
            *bufs, *bufs[3:], *[pltpu.VMEM(a.shape, a.dtype) for a in acts],
            pltpu.SemaphoreType.DMA((n,)), pltpu.SemaphoreType.DMA((n,)), pltpu.SemaphoreType.DMA((4,)),
        ],
        compiler_params=pltpu.CompilerParams(vmem_limit_bytes=60 << 20),
        name="update",
    )(*acts, *arrays)


def body(
    inputs, condition, lengths, cotangent,
    conv1_w, conv1_m, conv1_v, conv2_w, conv2_m, conv2_v, res_w, res_m, res_v,
    down_w, down_m, down_v, film_w, film_m, film_v, small_w, small_m, small_v,
):
    n_dp, n_ch = lax.axis_size("dp"), lax.axis_size("chan")
    lens = lengths.reshape(1, -1)

    def taps_first(*arrays):
        return tuple(jnp.transpose(a, (1, 0, 2)) for a in arrays)

    one, two, down = (
        taps_first(*state) for state in ((conv1_w, conv1_m, conv1_v), (conv2_w, conv2_m, conv2_v), (down_w, down_m, down_v))
    )
    cond, film_rows = condition, film_w
    frows = film_w.shape[0]
    if frows % 16:
        short = -frows % 16
        film_rows = jnp.pad(film_w, ((0, short), (0, 0), (0, 0)))
        cond = jnp.pad(condition.reshape(-1, n_dp, frows), ((0, 0), (0, 0), (0, short))).reshape(condition.shape[0], -1)
    output, input_grad, gw, gf, gs = block_step(
        n_dp, n_ch, inputs, cotangent, cond, lens, one[0], two[0], res_w, down[0], film_rows, small_w
    )
    output, input_grad, *state = update(
        output, input_grad, gw, gf, gs, *one, *two, res_w, res_m, res_v, *down, film_w, film_m, film_v, small_w, small_m, small_v
    )
    state = (*taps_first(*state[:6]), *state[6:9], *taps_first(*state[9:12]), *state[12:])
    return (output, input_grad, *state)


def solution(mesh):
    in_specs = (
        P("dp", "chan"),
        P("dp", None),
        P("dp"),
        P("dp", "chan"),
        P("dp", None, "chan"),
        P("dp", None, "chan"),
        P("dp", None, "chan"),
        P("dp", None, "chan"),
        P("dp", None, "chan"),
        P("dp", None, "chan"),
        P("dp", "chan"),
        P("dp", "chan"),
        P("dp", "chan"),
        P("dp", None, "chan"),
        P("dp", None, "chan"),
        P("dp", None, "chan"),
        P("dp", None, "chan"),
        P("dp", None, "chan"),
        P("dp", None, "chan"),
        P(None, "chan"),
        P(None, "chan"),
        P(None, "chan"),
    )
    out_specs = (
        P("dp", "chan"),
        P("dp", "chan"),
        P("dp", None, "chan"),
        P("dp", None, "chan"),
        P("dp", None, "chan"),
        P("dp", None, "chan"),
        P("dp", None, "chan"),
        P("dp", None, "chan"),
        P("dp", "chan"),
        P("dp", "chan"),
        P("dp", "chan"),
        P("dp", None, "chan"),
        P("dp", None, "chan"),
        P("dp", None, "chan"),
        P("dp", None, "chan"),
        P("dp", None, "chan"),
        P("dp", None, "chan"),
        P(None, "chan"),
        P(None, "chan"),
        P(None, "chan"),
    )
    return jax.shard_map(body, mesh=mesh, in_specs=in_specs, out_specs=out_specs, check_vma=False)
```
